128 devices in a mesh: ka: 16 (over y, z), row: 8 (over x, core).
Axes of the slice: x: 4, y: 4, z: 4, core: 2. Of those that a mesh axis runs over, the one named last changes fastest.
Arguments:
- base_k: float32 [128, 3], P('ka'), may hold values from 0 to 1
- counts: int32 [128], P('ka'), may hold values from 1 to 4, 320 in all
- block_order: int32 [128], P(('ka', 'row')), may hold values from 0 to 127, each once
- lattice: int32 [4096, 3], P('row'), may hold values from -8 to 7, as said below
- real_space: bfloat16 [4096, 3, 128, 2, 128], P('row', None, 'ka'), may hold values from -0.09375 to 0.09375
- eigvecs: bfloat16 [512, 128, 2, 128], P(('ka', 'row')), may hold values from -0.5 to 0.5
- occupied: int32 [512, 128], P(('ka', 'row')), may hold values 0 or 1
Outputs:
- curvature: float32 [512], P(('ka', 'row'))
The draws below stay inside these ranges and needn't reach their ends.
Inputs may be any that keep to these rules, and one draw needn't show every extreme that they name: The counts sum to 320, and some block has count 4. `block_order`: each block stands at exactly one position. `lattice`: all 4096 R-vectors are distinct.
All inputs are finite; a program needn't handle non-finite values. No bound on the sum of `occupied` on one device may be relied on, other than what follows from the above.
Results may differ from the reference program's by a relative error of at most 0.012.
The reference program's roundings to bfloat16 on the way count: a program that leaves them out, or rounds other values in their place, can miss the bound.
Values sent between devices are 32-bit elements; how exact they have to be, the bound alone decides.
No kernel may reach another device: no remote copies, remote signals or barrier semaphores. Data moves between devices by JAX's collectives and lax.ppermute only.
A program may use at most 128 MiB of HBM per device.

```python
import math
import jax
import jax.numpy as jnp
import numpy as np
from jax import lax

NW = 128
NR = 4096
SUB = 4
NBLK = 128
K_TOTAL = 512


def draw_lattice(key, part):
    first_key = jax.random.fold_in(key, 7001)
    second_key = jax.random.fold_in(key, 7002)
    inner = jax.random.permutation(first_key, 4094) + 1
    picked = jnp.concatenate([jnp.array([0, 4095], dtype=jnp.int32), inner[:NR - 2].astype(jnp.int32)])
    picked = jax.random.permutation(second_key, picked)
    coord_x = picked // 256 - 8
    coord_y = picked // 16 % 16 - 8
    coord_z = picked % 16 - 8
    return jnp.stack([coord_x, coord_y, coord_z], axis=1).astype(jnp.int32)


def set_ends(entries, own_key, least, top_value):
    longest = entries.shape.index(max(entries.shape))
    spots = []
    for shift in (0, 1):
        where = [jax.random.randint(jax.random.fold_in(own_key, axis), (), 0, length) for axis, length in enumerate(entries.shape)]
        where[longest] = (where[longest] + shift) % entries.shape[longest]
        spots.append(tuple(where))
    return entries.at[spots[0]].set(least).at[spots[1]].set(top_value)


def levels(stream_key, shape, shards, low, high):
    loudness = 1.0
    for axis_at, parts in shards:
        heights = jax.random.uniform(jax.random.fold_in(jax.random.fold_in(stream_key, 6), axis_at), (parts,), jnp.float32, low / len(shards), high / len(shards))
        loudness = loudness * jnp.repeat(jnp.exp(heights), shape[axis_at] // parts).reshape((-1,) + (1,) * (len(shape) - 1 - axis_at))
    return loudness


def split_up(count, total, most, lean):
    portions = [(1 << 20) // math.isqrt(grade ** lean) + 1 for grade in range(2, count + 1)]
    surplus, given = total - most - (count - 1), [1] * (count - 1)
    while surplus > 0:
        free = [i for i in range(count - 1) if given[i] < most]
        pool, remaining = sum([portions[i] for i in free]), surplus
        for i in free:
            more = min(most - given[i], max(1, remaining * portions[i] // pool), surplus)
            given[i] = given[i] + more
            surplus = surplus - more
    return np.array([most] + given)


def uneven(stream_key, number_of, total, reach, skew):
    if number_of == 2:
        one = jax.random.randint(stream_key, (), max(1, total - reach), min(reach, total - 1) + 1)
        return jnp.stack([one, total - one])
    tallies = jnp.asarray(split_up(number_of, total, reach, skew), jnp.int32)
    twos = (number_of - 1) // 2
    donor, taker = tallies[1:1 + 2 * twos:2], tallies[2:2 + 2 * twos:2]
    slack = jnp.minimum(donor - 1, reach - taker)
    passed = jax.random.randint(jax.random.fold_in(stream_key, 1), (twos,), 0, 1 << 20) % (slack + 1)
    tallies = tallies.at[1:1 + 2 * twos:2].set(donor - passed).at[2:2 + 2 * twos:2].set(taker + passed)
    return tallies[jax.random.permutation(jax.random.fold_in(stream_key, 2), number_of)]


def bell_draw(own_key, extent, deviation, most, split=(), kind=jnp.bfloat16):
    values = jax.random.normal(own_key, extent, jnp.float32) * deviation
    if len(split) > 0:
        values = levels(own_key, extent, split, -0.22, 0.18) * values
    return jnp.clip(values, min=-most, max=most).astype(kind)


def setup_inputs(seed: int = 0) -> dict:
    key_list = jax.random.split(jax.random.key(seed), 8)
    base_k = jnp.clip(1.0 * jax.random.uniform(key_list[0], (NBLK, 3), jnp.float32) ** levels(key_list[0], (NBLK, 3), ((0, 16),), -0.2, 0.2), 0.0, 1.0)
    counts = uneven(key_list[1], NBLK, 5 * NBLK // 2, SUB, 2).astype(jnp.int32)
    block_order = jax.random.permutation(key_list[2], NBLK).astype(jnp.int32)
    lattice = draw_lattice(jax.random.fold_in(key_list[7], 71), 0)
    real_space = bell_draw(key_list[4], (NR, 3, NW, 2, NW), NR ** -0.5, 0.09375, ((0, 8), (2, 16)))
    eigvecs = bell_draw(key_list[5], (K_TOTAL, NW, 2, NW), NW ** -0.5, 0.5, ((0, 128),))
    occupied = set_ends((jax.random.randint(key_list[6], (K_TOTAL, NW), 0, 2) < 1).astype(jnp.int32), jax.random.fold_in(key_list[6], 1), 0, 1)
    return dict(base_k=base_k, counts=counts, block_order=block_order, lattice=lattice, real_space=real_space, eigvecs=eigvecs, occupied=occupied)


broadening = 1.0
refine_step = (0.05, 0.03, 0.02)


def slot_points(base_points, block_counts):
    count_float = block_counts.astype(jnp.float32)
    sub_index = jnp.arange(SUB, dtype=jnp.float32)
    fraction = (sub_index[None, :] + 0.5) / count_float[:, None] - 0.5
    refine = jnp.array(refine_step, dtype=jnp.float32)
    kpoints = base_points[:, None, :] + fraction[:, :, None] * refine[None, None, :]
    alive = jnp.arange(SUB, dtype=jnp.int32)[None, :] < block_counts[:, None]
    weight = jnp.where(alive, 1.0 / count_float[:, None], 0.0).astype(jnp.float32)
    block_total = base_points.shape[0]
    return kpoints.reshape(block_total * SUB, 3), weight.reshape(block_total * SUB)


def make_phases(kpoints, lattice):
    coords = lattice.astype(jnp.float32)
    angles = (2.0 * math.pi) * (kpoints[:, 0:1] * coords[None, :, 0] + kpoints[:, 1:2] * coords[None, :, 1] + kpoints[:, 2:3] * coords[None, :, 2])
    cosines = jnp.cos(angles)
    sines = jnp.sin(angles)
    coord_x = coords[None, :, 0]
    coord_y = coords[None, :, 1]
    return jnp.stack([cosines, sines, -coord_x * sines, coord_x * cosines, -coord_y * sines, coord_y * cosines]).astype(jnp.bfloat16)


def combine(first_part, second_part):
    real_part = first_part[..., 0, :] - second_part[..., 1, :]
    imag_part = second_part[..., 0, :] + first_part[..., 1, :]
    return jnp.stack([real_part, imag_part], axis=-2)


def fourier(kpoints, lattice, real_space):
    phase_rows = make_phases(kpoints, lattice)
    row_count = kpoints.shape[0]
    r_count = real_space.shape[0]
    slab_rows = real_space.shape[2]
    width = real_space.shape[4]
    matrix_h = real_space[:, 0].reshape(r_count, slab_rows * 2 * width)
    matrix_a = real_space[:, 1:3].reshape(r_count, 2 * slab_rows * 2 * width)
    product_h = jnp.dot(phase_rows.reshape(6 * row_count, r_count), matrix_h, preferred_element_type=jnp.float32).reshape(6, row_count, slab_rows, 2, width)
    product_a = jnp.dot(phase_rows[0:2].reshape(2 * row_count, r_count), matrix_a, preferred_element_type=jnp.float32).reshape(2, row_count, 2, slab_rows, 2, width)
    pieces = [combine(product_h[0], product_h[1]), combine(product_h[2], product_h[3]), combine(product_h[4], product_h[5]), combine(product_a[0, :, 0], product_a[1, :, 0]), combine(product_a[0, :, 1], product_a[1, :, 1])]
    return jnp.stack(pieces, axis=1)


def curvature(k_field, vectors, occupied, weight):
    best = lax.Precision.HIGHEST
    matrices = k_field.astype(jnp.float32)
    vectors_f = vectors.astype(jnp.float32)
    mat_real = matrices[:, :, :, 0, :]
    mat_imag = matrices[:, :, :, 1, :]
    vec_real = vectors_f[:, :, 0, :]
    vec_imag = vectors_f[:, :, 1, :]
    turned_real = jnp.einsum('ncij,njb->ncib', mat_real, vec_real, precision=best) - jnp.einsum('ncij,njb->ncib', mat_imag, vec_imag, precision=best)
    turned_imag = jnp.einsum('ncij,njb->ncib', mat_real, vec_imag, precision=best) + jnp.einsum('ncij,njb->ncib', mat_imag, vec_real, precision=best)
    energy = jnp.sum(vec_real * turned_real[:, 0] + vec_imag * turned_imag[:, 0], axis=1)
    bar_real = jnp.einsum('nia,ncib->ncab', vec_real, turned_real[:, 1:], precision=best) + jnp.einsum('nia,ncib->ncab', vec_imag, turned_imag[:, 1:], precision=best)
    bar_imag = jnp.einsum('nia,ncib->ncab', vec_real, turned_imag[:, 1:], precision=best) - jnp.einsum('nia,ncib->ncab', vec_imag, turned_real[:, 1:], precision=best)
    spacing = energy[:, None, :] - energy[:, :, None]
    smoothed = spacing / (spacing * spacing + broadening)
    xcov_real = bar_real[:, 2] + smoothed * bar_real[:, 0]
    xcov_imag = bar_imag[:, 2] + smoothed * bar_imag[:, 0]
    ycov_real = bar_real[:, 3] + smoothed * bar_real[:, 1]
    ycov_imag = bar_imag[:, 3] + smoothed * bar_imag[:, 1]
    product_im = xcov_real * jnp.swapaxes(ycov_imag, 1, 2) + xcov_imag * jnp.swapaxes(ycov_real, 1, 2)
    filled = occupied.astype(jnp.float32)
    pairing = filled[:, :, None] * (1.0 - filled[:, None, :])
    berry_sum = (-2.0 / NW) * jnp.sum(pairing * product_im, axis=(1, 2))
    return weight * berry_sum


def reference(base_k, counts, block_order, lattice, real_space, eigvecs, occupied):
    kpoints, weight = slot_points(base_k[block_order], counts[block_order])
    block_size = 64
    slot_count = kpoints.shape[0]
    groups = slot_count // block_size

    def per_block(operands):
        block_points, block_vectors, block_occupied, block_weight = operands
        k_field = fourier(block_points, lattice, real_space)
        return curvature(k_field, block_vectors, block_occupied, block_weight)

    results = lax.map(per_block, (kpoints.reshape(groups, block_size, 3), eigvecs.reshape(groups, block_size, NW, 2, NW), occupied.reshape(groups, block_size, NW), weight.reshape(groups, block_size)))
    return results.reshape(slot_count)
```

```python
import math

import jax
import jax.numpy as jnp
from jax import lax
from jax.experimental import pallas as pl
from jax.experimental.pallas import tpu as pltpu
from jax.sharding import Mesh
from jax.sharding import PartitionSpec as P

SUB = 4
KA = ("ka_0", "ka_1")
KA_ROW = ("ka_0", "ka_1", "row_0", "row_1")
ROW = ("row_0", "row_1")
PLANE = ("ka_0", "ka_1", "row_1")
INTERPRET = False

broadening = 1.0
refine_step = (0.05, 0.03, 0.02)

f32 = jnp.float32
bf16 = jnp.bfloat16
VMEM = pl.BlockSpec(memory_space=pltpu.VMEM)
SMEM = pl.BlockSpec(memory_space=pltpu.SMEM)
NX = 4
OWNERS = 32
BLOCKS = 128


def params(**more):
    return pltpu.CompilerParams(vmem_limit_bytes=56 << 20, **more)


def iota(shape, dim):
    return lax.broadcasted_iota(jnp.int32, shape, dim)


def place_of(position):
    plane = (position % 8) // 2
    owner = (position // 8) * 2 + position % 2
    return plane, owner


def index_kernel(place_ref, table_ref, points_ref, slots_ref, weight_ref):
    my_plane = place_ref[0]
    table = table_ref[...]
    turned = table.T
    square = (BLOCKS, BLOCKS)
    order_down = table[:, 4:5].astype(jnp.int32)
    order_along = turned[4:5, :].astype(jnp.int32)
    here_down = order_down == iota(square, 1)
    here_along = iota(square, 0) == order_along

    def along(column):
        return jnp.sum(jnp.where(here_along, table[:, column : column + 1], 0.0), axis=0, keepdims=True)

    base = [along(axis) for axis in range(3)]
    count = along(3)
    count_down = jnp.sum(jnp.where(here_down, turned[3:4, :], 0.0), axis=1, keepdims=True)

    plane_down, owner_down = place_of(iota(square, 0))
    plane_along, owner_along = place_of(iota(square, 1))
    mates = plane_down == plane_along
    ahead = mates & (owner_down < owner_along)
    plane_row, owner_row = place_of(iota((1, BLOCKS), 1))
    away = (plane_row - my_plane + NX) % NX

    rows = OWNERS * NX
    entry = iota((3 * rows, BLOCKS), 0)
    dense_entry = iota((rows, BLOCKS), 0)
    lane = iota((4 * rows, BLOCKS), 1)
    gathered = [jnp.zeros((3 * rows, BLOCKS), f32) for _ in range(3)]
    dense = []
    before = jnp.zeros((1, BLOCKS), f32)
    slots_ref[...] = jnp.zeros((8, BLOCKS), jnp.int32)
    weight_ref[...] = jnp.zeros((8, BLOCKS), f32)
    for s in range(SUB):
        fraction = (s + 0.5) / count - 0.5
        points = [base[axis] + fraction * refine_step[axis] for axis in range(3)]
        alive = count > s
        weight_ref[s : s + 1, :] = jnp.where(alive, 1.0 / count, 0.0)
        if s == 0:
            match = dense_entry == away * OWNERS + owner_row
            for axis in range(3):
                dense.append(jnp.where(match, points[axis], 0.0))
            continue
        live_down = count_down > s
        rank = before + jnp.sum(jnp.where(ahead & live_down, 1.0, 0.0), axis=0, keepdims=True)
        before = before + jnp.sum(jnp.where(mates & live_down, 1.0, 0.0), axis=0, keepdims=True)
        rank = rank.astype(jnp.int32)
        target = (rank // OWNERS) * rows + away * OWNERS + rank % OWNERS
        match = entry == jnp.where(alive, target, -1)
        for axis in range(3):
            gathered[axis] = gathered[axis] + jnp.where(match, points[axis], 0.0)
        slots_ref[s : s + 1, :] = jnp.where(alive, rank, 0)
    most = jnp.max(before, axis=1, keepdims=True)
    slots_ref[0:1, :] = jnp.broadcast_to(most, (1, BLOCKS)).astype(jnp.int32)
    points = jnp.zeros((4 * rows, BLOCKS), f32)
    for axis in range(3):
        column = jnp.concatenate([gathered[axis], dense[axis]], axis=0)
        points = jnp.where(lane == axis, jnp.sum(column, axis=1, keepdims=True), points)
    points_ref[...] = points


def find_points(table, plane):
    rows = OWNERS * NX
    return pl.pallas_call(
        index_kernel,
        out_shape=(
            jax.ShapeDtypeStruct((4 * rows, BLOCKS), f32),
            jax.ShapeDtypeStruct((8, BLOCKS), jnp.int32),
            jax.ShapeDtypeStruct((8, BLOCKS), f32),
        ),
        in_specs=[SMEM, VMEM],
        out_specs=(VMEM, VMEM, VMEM),
        compiler_params=params(),
        interpret=INTERPRET,
        name="find_points",
    )(plane, table)


def split_kernel(core_ref, space_ref, own_ref, send_ref, wide_ref):
    core = core_ref[0]
    depth, rows, width = space_ref.shape
    half = rows // 12
    wide_ref[...] = space_ref[...].astype(f32).reshape(depth * rows, width)
    for matrix in range(3):
        for part in range(2):
            for r in range(half):
                lanes = slice(r * width, (r + 1) * width)
                own_at = matrix * (rows // 3) + 2 * (half * core + r) + part
                send_at = matrix * (rows // 3) + 2 * (half * (1 - core) + r) + part
                own = wide_ref[pl.ds(own_at, depth, stride=rows), :]
                own_ref[matrix, part, :, lanes] = own.astype(bf16)
                send_ref[matrix, part, :, lanes] = wide_ref[pl.ds(send_at, depth, stride=rows), :]


def split_rows(space, core):
    depth, rows, width = space.shape
    block = min(depth, 128)
    lanes = rows // 12 * width
    shape = (3, 2, depth, lanes)
    spec = pl.BlockSpec((3, 2, block, lanes), lambda i: (0, 0, i, 0))
    return pl.pallas_call(
        split_kernel,
        grid=(depth // block,),
        out_shape=(jax.ShapeDtypeStruct(shape, bf16), jax.ShapeDtypeStruct(shape, f32)),
        in_specs=[SMEM, pl.BlockSpec((block, rows, width), lambda i: (i, 0, 0))],
        out_specs=(spec, spec),
        scratch_shapes=[pltpu.VMEM((block * rows, width), f32)],
        compiler_params=params(),
        interpret=INTERPRET,
        name="split_rows",
    )(core, space)


def narrow_kernel(wide_ref, narrow_ref):
    narrow_ref[...] = wide_ref[...].astype(bf16)


def narrow(wide):
    matrices, depth, lanes = wide.shape
    spec = pl.BlockSpec((1, depth, lanes), lambda i: (i, 0, 0))
    return pl.pallas_call(
        narrow_kernel,
        grid=(matrices,),
        out_shape=jax.ShapeDtypeStruct(wide.shape, bf16),
        in_specs=[spec],
        out_specs=spec,
        compiler_params=params(),
        interpret=INTERPRET,
        name="narrow",
    )(wide)


def turn(points, coords):
    turns = points[:, 0:1] * coords[0:1, :] + points[:, 1:2] * coords[1:2, :] + points[:, 2:3] * coords[2:3, :]
    rest = turns - jnp.floor(turns + 0.5)
    quarter = jnp.floor(4.0 * rest + 0.5)
    angle = (rest - 0.25 * quarter) * (2.0 * math.pi)
    square = angle * angle
    sine = angle * (1.0 + square * (-1.0 / 6 + square * (1.0 / 120 + square * (-1.0 / 5040 + square * (1.0 / 362880)))))
    cosine = 1.0 + square * (-0.5 + square * (1.0 / 24 + square * (-1.0 / 720 + square * (1.0 / 40320 - square / 3628800))))
    odd = jnp.abs(quarter) == 1.0
    first = jnp.where(odd, sine, cosine)
    second = jnp.where(odd, cosine, sine)
    cos_sign = jnp.where((quarter == 1.0) | (jnp.abs(quarter) == 2.0), -1.0, 1.0)
    sin_sign = jnp.where((quarter == -1.0) | (jnp.abs(quarter) == 2.0), -1.0, 1.0)
    return first * cos_sign, second * sin_sign


def fourier_kernel(points_ref, coords_ref, own_ref, other_ref, keep_ref, right_ref, near_ref, far_ref, left_ref, phase_ref):
    step = pl.program_id(0)
    count = points_ref.shape[0]
    depth = coords_ref.shape[1] // 2
    owners = count // NX

    @pl.when(step == 0)
    def _():
        points = points_ref[...]
        for source in range(2):
            coords = coords_ref[:, source * depth : (source + 1) * depth]
            cosine, sine = turn(points, coords)
            at_real = slice(source * 2 * depth, source * 2 * depth + depth)
            at_imag = slice(source * 2 * depth + depth, source * 2 * depth + 2 * depth)
            pairs = [(cosine, sine)]
            for axis in range(2):
                coord = coords[axis : axis + 1, :]
                pairs.append((-coord * sine, coord * cosine))
            for kind, (real, imag) in enumerate(pairs):
                phase_ref[(2 * kind) * count : (2 * kind + 1) * count, at_real] = real.astype(bf16)
                phase_ref[(2 * kind) * count : (2 * kind + 1) * count, at_imag] = (-imag).astype(bf16)
                phase_ref[(2 * kind + 1) * count : (2 * kind + 2) * count, at_real] = imag.astype(bf16)
                phase_ref[(2 * kind + 1) * count : (2 * kind + 2) * count, at_imag] = real.astype(bf16)

    def store(product, kinds, first_kind, first_row):
        width = product.shape[1] // 2
        for kind in range(kinds):
            for half in range(2):
                block = product[kind * count : (kind + 1) * count, half * width : (half + 1) * width]
                at = (first_kind + kind) * 4 + first_row + half
                start = 0
                for ref in (keep_ref, right_ref, near_ref, far_ref, left_ref):
                    size = ref.shape[0] // 40
                    ref[pl.ds(at, size, stride=40), :] = block[start : start + size]
                    start += size

    def product(kinds):
        rows = slice(0, kinds * count)
        return jnp.dot(phase_ref[rows, : 2 * depth], own_ref[0], preferred_element_type=f32) + jnp.dot(
            phase_ref[rows, 2 * depth :], other_ref[0], preferred_element_type=f32
        )

    @pl.when(step < 2)
    def _():
        store(product(6), 6, 0, 2 * step)

    @pl.when(step >= 2)
    def _():
        store(product(2), 2, 6 + 2 * (step // 2 - 1), 2 * (step % 2))


def fourier(points, coords, own, other):
    count = points.shape[0]
    depth2 = own.shape[1]
    width = own.shape[2] // 4
    owners = count // NX
    spec = pl.BlockSpec((1, depth2, 2 * width), lambda j: (j // 2, 0, j % 2))
    sizes = (owners, owners, owners // 2, owners // 2, owners)
    shapes = tuple(jax.ShapeDtypeStruct((size * 40, width), f32) for size in sizes)
    outs = pl.pallas_call(
        fourier_kernel,
        grid=(6,),
        out_shape=shapes,
        in_specs=[
            pl.BlockSpec(points.shape, lambda j: (0, 0)),
            pl.BlockSpec(coords.shape, lambda j: (0, 0)),
            spec,
            spec,
        ],
        out_specs=tuple(pl.BlockSpec(shape.shape, lambda j: (0, 0)) for shape in shapes),
        scratch_shapes=[pltpu.VMEM((6 * count, 2 * depth2), bf16)],
        compiler_params=params(),
        interpret=INTERPRET,
        name="fourier",
    )(points, coords, own, other)
    return tuple(out.reshape(-1, 40, width) for out in outs)


def to_right(value):
    return lax.ppermute(value, "row_0", [(i, (i + 1) % NX) for i in range(NX)])


def to_left(value):
    return lax.ppermute(value, "row_0", [(i, (i - 1) % NX) for i in range(NX)])


def first_hop(parts):
    keep, right, near, far, left = parts
    return to_right(near), to_left(far)


def second_hop(parts, arrived):
    keep, right, near, far, left = parts
    half = near.shape[0]
    right = jnp.concatenate([right[:half] + arrived[0], right[half:]], axis=0)
    left = jnp.concatenate([left[:half], left[half:] + arrived[1]], axis=0)
    return keep, to_right(right), to_left(left)


def place_kernel(units, place_ref, slots_ref, *refs):
    ins, outs = refs[:-1], refs[-1]
    plane = place_ref[0]
    tables = [ins[i] for i in range(len(ins))]

    def body(owner, carry):
        position = (owner // 2) * 8 + 2 * plane + owner % 2
        for u, s in enumerate(units):
            at = slots_ref[s, position]
            outs[owner, u] = tables[0][at]
        return carry

    lax.fori_loop(0, OWNERS, body, 0)


def place_slots(units, plane, slots, table):
    width = table.shape[-1]
    return pl.pallas_call(
        lambda *refs: place_kernel(units, *refs),
        out_shape=jax.ShapeDtypeStruct((OWNERS, len(units), 40, width), f32),
        in_specs=[SMEM, SMEM, VMEM],
        out_specs=VMEM,
        compiler_params=params(),
        interpret=INTERPRET,
        name="place_slots",
    )(plane, slots, table)


def to_owners(value):
    return lax.all_to_all(value, PLANE, split_axis=0, concat_axis=0, tiled=True)


def two_terms(value):
    high = value.astype(bf16)
    return high, (value - high.astype(f32)).astype(bf16)


def curvature_kernel(units, weight_ref, field_ref, turn_ref, back_ref, occupied_ref, out_ref):
    sources = field_ref.shape[0] // (len(units) * 40)
    width = field_ref.shape[1]
    lane = iota((1, BLOCKS), 1)
    total = jnp.zeros((1, BLOCKS), f32)
    for u, s in enumerate(units):
        stride = len(units) * 40

        def plane_of(kind):
            return jnp.concatenate(
                [field_ref[pl.ds(u * 40 + kind * 4 + r, sources, stride=stride), :] for r in range(4)], axis=0
            )

        matrices = jnp.concatenate(
            [jnp.concatenate([plane_of(2 * c), plane_of(2 * c + 1)], axis=1) for c in range(5)], axis=0
        )
        high, low = two_terms(matrices)
        vectors = turn_ref[s]
        rotated = jnp.dot(high, vectors, preferred_element_type=f32) + jnp.dot(
            low, vectors, preferred_element_type=f32
        )
        n = width
        back = back_ref[s]
        adjoint = back[:n, :].astype(f32)
        vec_real = adjoint[:, :n].T
        vec_imag = adjoint[:, n:].T
        energy = jnp.sum(vec_real * rotated[:n, :n] + vec_imag * rotated[:n, n:], axis=0, keepdims=True)
        stacked = jnp.concatenate(
            [
                jnp.concatenate([rotated[(c + 1) * n : (c + 2) * n, :n] for c in range(4)], axis=1),
                jnp.concatenate([rotated[(c + 1) * n : (c + 2) * n, n:] for c in range(4)], axis=1),
            ],
            axis=0,
        )
        high, low = two_terms(stacked)
        bar = jnp.dot(back, high, preferred_element_type=f32) + jnp.dot(back, low, preferred_element_type=f32)
        bar_real, bar_imag = bar[:n], bar[n:]
        across = jnp.broadcast_to(energy, (n, n))
        spacing = across - across.T
        smoothed = spacing / (spacing * spacing + broadening)

        def pick(value, c):
            return value[:, c * n : (c + 1) * n]

        xcov_real = pick(bar_real, 2) + smoothed * pick(bar_real, 0)
        xcov_imag = pick(bar_imag, 2) + smoothed * pick(bar_imag, 0)
        ycov_real = pick(bar_real, 3) + smoothed * pick(bar_real, 1)
        ycov_imag = pick(bar_imag, 3) + smoothed * pick(bar_imag, 1)
        filled = occupied_ref[s : s + 1, :].astype(f32)
        filled_down = jnp.broadcast_to(filled, (n, n)).T
        pairing = filled_down * (1.0 - filled)
        product = pairing * (xcov_real * ycov_imag.T + xcov_imag * ycov_real.T)
        berry = jnp.sum(jnp.sum(product, axis=0, keepdims=True), axis=1, keepdims=True) * (-2.0 / n)
        weight = weight_ref[s]
        total = jnp.where((lane == s) & (weight > 0.0), weight * berry, total)
    out_ref[...] = total


def curvature(units, weight, arrived, vectors, adjoint, occupied):
    width = arrived.shape[-1]
    return pl.pallas_call(
        lambda *refs: curvature_kernel(units, *refs),
        out_shape=jax.ShapeDtypeStruct((1, BLOCKS), f32),
        in_specs=[SMEM, VMEM, VMEM, VMEM, VMEM],
        out_specs=VMEM,
        compiler_params=params(),
        interpret=INTERPRET,
        name="curvature",
    )(weight, arrived.reshape(-1, width), vectors, adjoint, occupied)


def vector_matrices(eigvecs):
    slots, width = eigvecs.shape[0], eigvecs.shape[1]
    real, imag = eigvecs[:, :, 0, :], eigvecs[:, :, 1, :]
    turning = jnp.concatenate(
        [jnp.concatenate([real, imag], axis=2), jnp.concatenate([-imag, real], axis=2)], axis=1
    )

    def adjoint(value):
        return value.reshape(slots, OWNERS, width // OWNERS, width).transpose(0, 3, 2, 1).reshape(slots, width, width)

    real, imag = adjoint(real), adjoint(imag)
    back = jnp.concatenate(
        [jnp.concatenate([real, imag], axis=2), jnp.concatenate([-imag, real], axis=2)], axis=1
    )
    return turning, back


def on_device(base_k, counts, block_order, lattice, real_space, eigvecs, occupied):
    plane, core = lax.axis_index("row_0"), lax.axis_index("row_1")
    row = plane * 2 + core
    plane_ref = plane.reshape(1).astype(jnp.int32)
    core_ref = core.reshape(1).astype(jnp.int32)
    depth, _, slab, _, width = real_space.shape

    own_base = lax.dynamic_slice_in_dim(base_k, row, 1, 0)
    own_count = lax.dynamic_slice_in_dim(counts, row, 1, 0).astype(f32)[:, None]
    mine = jnp.concatenate([own_base, own_count, block_order.astype(f32)[:, None]], axis=1)
    mine = jnp.pad(mine, ((0, 0), (0, BLOCKS - 5)))
    line = lax.all_to_all(jnp.broadcast_to(mine[None], (8, 1, BLOCKS)), ROW, 0, 0, tiled=True)

    own, send = split_rows(real_space.reshape(depth, 6 * slab, width), core_ref)
    swap = [(0, 1), (1, 0)]
    other = lax.ppermute(send, "row_1", swap)
    own_coords = jnp.pad(lattice.T.astype(f32), ((0, 5), (0, 0)))
    coords = jnp.concatenate([own_coords, lax.ppermute(own_coords, "row_1", swap)], axis=1)

    lines = jnp.broadcast_to(line.reshape(1, 8, BLOCKS), (16, 8, BLOCKS))
    table = lax.all_to_all(lines, KA, 0, 0, tiled=True).reshape(BLOCKS, BLOCKS)
    points, slots, weights = find_points(table, plane_ref)
    position = (lax.axis_index(KA) * 8 + row).astype(jnp.int32)
    weight = lax.dynamic_slice(weights, (jnp.int32(0), position), (SUB, 1)).reshape(SUB)

    own = own.reshape(3, 2 * depth, -1)
    other = narrow(other.reshape(3, 2 * depth, -1))
    rows = OWNERS * NX

    def chunk(i):
        return fourier(points[i * rows : (i + 1) * rows], coords, own, other)

    turning, back = vector_matrices(eigvecs)

    parts0 = chunk(0)
    hop0 = first_hop(parts0)
    parts1 = chunk(1)
    hop1 = first_hop(parts1)
    sum0 = sum(second_hop(parts0, hop0))
    parts3 = chunk(3)
    hop3 = first_hop(parts3)
    sum1 = sum(second_hop(parts1, hop1))
    sum3 = sum(second_hop(parts3, hop3))

    def further(_):
        parts = chunk(2)
        return sum(second_hop(parts, first_hop(parts)))

    extra = lax.cond(slots[0, 0] > 2 * OWNERS, further, lambda _: jnp.zeros(sum0.shape, f32), 0)

    unit1 = to_owners(place_slots((1,), plane_ref, slots, sum0))
    unit23 = to_owners(place_slots((2, 3), plane_ref, slots, jnp.concatenate([sum0, sum1, extra], axis=0)))
    unit0 = to_owners(sum3)
    curve = (
        curvature((1,), weight, unit1, turning, back, occupied)
        + curvature((2, 3), weight, unit23, turning, back, occupied)
        + curvature((0,), weight, unit0, turning, back, occupied)
    )
    return curve[0, :SUB]


def solution(mesh):
    finer = Mesh(mesh.devices.reshape(4, 4, 4, 2), ("ka_0", "ka_1", "row_0", "row_1"))
    placed = (
        P(KA, None),
        P(KA),
        P(KA_ROW),
        P(ROW, None),
        P(ROW, None, KA, None, None),
        P(KA_ROW, None, None, None),
        P(KA_ROW, None),
    )
    return jax.shard_map(
        on_device, mesh=finer, in_specs=placed, out_specs=P(KA_ROW), check_vma=False
    )
```

```python
import math

import jax
import jax.numpy as jnp
from jax import lax
from jax.experimental import pallas as pl
from jax.experimental.pallas import tpu as pltpu
from jax.sharding import Mesh
from jax.sharding import PartitionSpec as P

SUB = 4
KA = ("ka_0", "ka_1")
KA_ROW = ("ka_0", "ka_1", "row_0", "row_1")
ROW = ("row_0", "row_1")
PLANE = ("ka_0", "ka_1", "row_1")
INTERPRET = False

broadening = 1.0
refine_step = (0.05, 0.03, 0.02)

f32 = jnp.float32
bf16 = jnp.bfloat16
VMEM = pl.BlockSpec(memory_space=pltpu.VMEM)
SMEM = pl.BlockSpec(memory_space=pltpu.SMEM)
NX = 4
OWNERS = 32
BLOCKS = 128


def params(**more):
    return pltpu.CompilerParams(vmem_limit_bytes=56 << 20, **more)


ANY = pl.BlockSpec(memory_space=pl.ANY)


def cost(microseconds):
    return pl.CostEstimate(flops=int(microseconds * 2.5e8), bytes_accessed=0, transcendentals=0)


def iota(shape, dim):
    return lax.broadcasted_iota(jnp.int32, shape, dim)


def place_of(position):
    plane = (position % 8) // 2
    owner = (position // 8) * 2 + position % 2
    return plane, owner


def index_kernel(place_ref, table_ref, points_ref, slots_ref, weight_ref):
    my_plane = place_ref[0]
    table = table_ref[...]
    turned = table.T
    square = (BLOCKS, BLOCKS)
    order_down = table[:, 4:5].astype(jnp.int32)
    order_along = turned[4:5, :].astype(jnp.int32)
    here_down = order_down == iota(square, 1)
    here_along = iota(square, 0) == order_along

    def along(column):
        return jnp.sum(jnp.where(here_along, table[:, column : column + 1], 0.0), axis=0, keepdims=True)

    base = [along(axis) for axis in range(3)]
    count = along(3)
    count_down = jnp.sum(jnp.where(here_down, turned[3:4, :], 0.0), axis=1, keepdims=True)

    plane_down, owner_down = place_of(iota(square, 0))
    plane_along, owner_along = place_of(iota(square, 1))
    mates = plane_down == plane_along
    ahead = mates & (owner_down < owner_along)
    plane_row, owner_row = place_of(iota((1, BLOCKS), 1))
    away = (plane_row - my_plane + NX) % NX
    seat = jnp.where(away == 1, 0, jnp.where(away == 3, 1, 2))

    def row_of(chunk, within):
        half = within // (OWNERS // 2)
        opposite = jnp.where(chunk == 0, within, OWNERS // 2 * (1 + chunk + half) + within)
        apart = 3 * OWNERS * (1 + chunk) + seat * OWNERS + within
        spare = 12 * OWNERS + jnp.where(away == 2, 0, 1 + seat) * OWNERS + within
        return jnp.where(chunk == 3, spare, jnp.where(away == 2, opposite, apart))

    rows = 4 * OWNERS * NX
    entry = iota((rows, BLOCKS), 0)
    lane = iota((rows, BLOCKS), 1)
    gathered = [jnp.zeros((rows, BLOCKS), f32) for _ in range(3)]
    before = jnp.zeros((1, BLOCKS), f32)
    slots_ref[...] = jnp.zeros((8, BLOCKS), jnp.int32)
    weight_ref[...] = jnp.zeros((8, BLOCKS), f32)
    for s in range(SUB):
        fraction = (s + 0.5) / count - 0.5
        points = [base[axis] + fraction * refine_step[axis] for axis in range(3)]
        alive = count > s
        weight_ref[s : s + 1, :] = jnp.where(alive, 1.0 / count, 0.0)
        if s == 0:
            chunk, within = jnp.full((1, BLOCKS), 2, jnp.int32), owner_row
        else:
            live_down = count_down > s
            rank = before + jnp.sum(jnp.where(ahead & live_down, 1.0, 0.0), axis=0, keepdims=True)
            before = before + jnp.sum(jnp.where(mates & live_down, 1.0, 0.0), axis=0, keepdims=True)
            rank = jnp.where(alive, rank, 0.0).astype(jnp.int32)
            slots_ref[s : s + 1, :] = rank
            chunk, within = rank // OWNERS, rank % OWNERS
            chunk = jnp.where(chunk == 2, 3, chunk)
        match = entry == jnp.where(alive, row_of(chunk, within), -1)
        for axis in range(3):
            gathered[axis] = gathered[axis] + jnp.where(match, points[axis], 0.0)
    most = jnp.max(before, axis=1, keepdims=True)
    slots_ref[0:1, :] = jnp.broadcast_to(most, (1, BLOCKS)).astype(jnp.int32)
    points = jnp.zeros((rows, BLOCKS), f32)
    for axis in range(3):
        points = jnp.where(lane == axis, jnp.sum(gathered[axis], axis=1, keepdims=True), points)
    points_ref[...] = points


def find_points(table, plane):
    rows = OWNERS * NX
    return pl.pallas_call(
        index_kernel,
        out_shape=(
            jax.ShapeDtypeStruct((4 * rows, BLOCKS), f32),
            jax.ShapeDtypeStruct((8, BLOCKS), jnp.int32),
            jax.ShapeDtypeStruct((8, BLOCKS), f32),
        ),
        in_specs=[SMEM, VMEM],
        out_specs=(VMEM, VMEM, VMEM),
        compiler_params=params(),
        cost_estimate=cost(2),
        interpret=INTERPRET,
        name="find_points",
    )(plane, table)


def split_kernel(core_ref, space_ref, own_ref, send_ref, wide_ref):
    core = core_ref[0]
    depth, rows, width = space_ref.shape
    half = rows // 12
    pitch = wide_ref.shape[0] // depth
    for first in range(0, depth, 8):
        wide = space_ref[first : first + 8].astype(f32)
        for r in range(8):
            wide_ref[(first + r) * pitch : (first + r) * pitch + rows, :] = wide[r]
    for matrix in range(3):
        for part in range(2):
            for r in range(half):
                lanes = slice(r * width, (r + 1) * width)
                own_at = matrix * (rows // 3) + 2 * (half * core + r) + part
                send_at = matrix * (rows // 3) + 2 * (half * (1 - core) + r) + part
                own = wide_ref[pl.ds(own_at, depth, stride=pitch), :]
                own_ref[matrix, part, :, lanes] = own.astype(bf16)
                send_ref[matrix, part, :, lanes] = wide_ref[pl.ds(send_at, depth, stride=pitch), :]


def split_rows(space, core):
    depth, rows, width = space.shape
    block = min(depth, 128)
    lanes = rows // 12 * width
    shape = (3, 2, depth, lanes)
    spec = pl.BlockSpec((3, 2, block, lanes), lambda i: (0, 0, i, 0))
    return pl.pallas_call(
        split_kernel,
        grid=(depth // block,),
        out_shape=(jax.ShapeDtypeStruct(shape, bf16), jax.ShapeDtypeStruct(shape, f32)),
        in_specs=[SMEM, pl.BlockSpec((block, rows, width), lambda i: (i, 0, 0))],
        out_specs=(spec, spec),
        scratch_shapes=[pltpu.VMEM((block * (rows + 8), width), f32)],
        compiler_params=params(),
        cost_estimate=cost(8),
        interpret=INTERPRET,
        name="split_rows",
    )(core, space)


def turn(points, coords):
    turns = points[:, 0:1] * coords[0:1, :] + points[:, 1:2] * coords[1:2, :] + points[:, 2:3] * coords[2:3, :]
    rest = turns - jnp.floor(turns + 0.5)
    quarter = jnp.floor(4.0 * rest + 0.5)
    angle = (rest - 0.25 * quarter) * (2.0 * math.pi)
    square = angle * angle
    sine = angle * (1.0 + square * (-1.0 / 6 + square * (1.0 / 120 + square * (-1.0 / 5040 + square * (1.0 / 362880)))))
    cosine = 1.0 + square * (-0.5 + square * (1.0 / 24 + square * (-1.0 / 720 + square * (1.0 / 40320 - square / 3628800))))
    odd = jnp.abs(quarter) == 1.0
    first = jnp.where(odd, sine, cosine)
    second = jnp.where(odd, cosine, sine)
    cos_sign = jnp.where((quarter == 1.0) | (jnp.abs(quarter) == 2.0), -1.0, 1.0)
    sin_sign = jnp.where((quarter == -1.0) | (jnp.abs(quarter) == 2.0), -1.0, 1.0)
    return first * cos_sign, second * sin_sign


def fourier_kernel(low, high, narrowing, waits, points_ref, coords_ref, own_ref, other_ref, *refs):
    out_refs, phase_ref = refs[waits:-1], refs[-1]
    step = pl.program_id(0)
    count = high - low
    depth = coords_ref.shape[1] // 2
    tile = 16

    @pl.when(step == 0)
    def _():
        def rows_of(i, carry):
            first = pl.multiple_of(i * tile, tile)
            points = points_ref[pl.ds(low + first, tile), :]
            for source in range(2):
                coords = coords_ref[:, source * depth : (source + 1) * depth]
                cosine, sine = turn(points, coords)
                at_real = slice(source * 2 * depth, source * 2 * depth + depth)
                at_imag = slice(source * 2 * depth + depth, source * 2 * depth + 2 * depth)
                pairs = [(cosine, sine)]
                for axis in range(2):
                    coord = coords[axis : axis + 1, :]
                    pairs.append((-coord * sine, coord * cosine))
                for kind, (real, imag) in enumerate(pairs):
                    real_rows = pl.ds(2 * kind * count + first, tile)
                    imag_rows = pl.ds((2 * kind + 1) * count + first, tile)
                    phase_ref[real_rows, at_real] = real.astype(bf16)
                    phase_ref[real_rows, at_imag] = (-imag).astype(bf16)
                    phase_ref[imag_rows, at_real] = imag.astype(bf16)
                    phase_ref[imag_rows, at_imag] = real.astype(bf16)
            return carry

        lax.fori_loop(0, count // tile, rows_of, 0)

    if narrowing:
        other_value = other_ref[0].astype(bf16)
        out_refs[-1][0] = other_value
    else:
        other_value = other_ref[0]

    def store(product, kinds, first_kind, first_row):
        width = product.shape[1] // 2
        for kind in range(kinds):
            for half in range(2):
                block = product[kind * count : (kind + 1) * count, half * width : (half + 1) * width]
                at = (first_kind + kind) * 4 + first_row + half
                start = 0
                for ref in out_refs[: len(out_refs) - narrowing]:
                    size = ref.shape[0] // 40
                    ref[pl.ds(at, size, stride=40), :] = block[start : start + size]
                    start += size

    def product(kinds):
        rows = slice(0, kinds * count)
        return jnp.dot(phase_ref[rows, : 2 * depth], own_ref[0], preferred_element_type=f32) + jnp.dot(
            phase_ref[rows, 2 * depth :], other_value, preferred_element_type=f32
        )

    @pl.when(step < 2)
    def _():
        store(product(6), 6, 0, 2 * step)

    @pl.when(step >= 2)
    def _():
        store(product(2), 2, 6 + 2 * (step // 2 - 1), 2 * (step % 2))


def fourier(points, low, high, sizes, coords, own, other, microseconds, after=(), narrowing=False):
    depth2 = own.shape[1]
    width = own.shape[2] // 4
    spec = pl.BlockSpec((1, depth2, 2 * width), lambda j: (j // 2, 0, j % 2))
    shapes = [jax.ShapeDtypeStruct((size * 40, width), f32) for size in sizes]
    specs = [pl.BlockSpec(shape.shape, lambda j: (0, 0)) for shape in shapes]
    if narrowing:
        shapes.append(jax.ShapeDtypeStruct(own.shape, bf16))
        specs.append(spec)
    outs = pl.pallas_call(
        lambda *refs: fourier_kernel(low, high, int(narrowing), len(after), *refs),
        grid=(6,),
        out_shape=tuple(shapes),
        in_specs=[
            pl.BlockSpec(points.shape, lambda j: (0, 0)),
            pl.BlockSpec(coords.shape, lambda j: (0, 0)),
            spec,
            spec,
        ]
        + [ANY] * len(after),
        out_specs=tuple(specs),
        scratch_shapes=[pltpu.VMEM((6 * (high - low), 2 * depth2), bf16)],
        compiler_params=params(),
        cost_estimate=cost(microseconds),
        interpret=INTERPRET,
        name="fourier",
    )(points, coords, own, other, *after)
    return tuple(out.reshape(-1, 40, width) for out in outs[: len(sizes)]) + tuple(outs[len(sizes) :])


def to_right(value):
    return lax.ppermute(value, "row_0", [(i, (i + 1) % NX) for i in range(NX)])


def to_left(value):
    return lax.ppermute(value, "row_0", [(i, (i - 1) % NX) for i in range(NX)])


def first_hop(near, far):
    return to_right(near), to_left(far)


def add_kernel(chunks, waits, near_ref, far_ref, *refs):
    ins, outs = refs[: 2 * chunks], refs[2 * chunks + waits :]
    size = near_ref.shape[0] // chunks
    for c in range(chunks):
        rows = slice(c * size, (c + 1) * size)
        outs[2 * c][...] = ins[2 * c][...] + near_ref[rows]
        outs[2 * c + 1][...] = ins[2 * c + 1][...] + far_ref[rows]


def add_arrived(near, far, sides, after=()):
    chunks = len(sides) // 2
    count, rows, width = near.shape
    size = count // chunks
    whole = pl.BlockSpec(near.shape, lambda i: (0, 0, 0))
    lower = pl.BlockSpec((size, rows, width), lambda i: (0, 0, 0))
    upper = pl.BlockSpec((size, rows, width), lambda i: (1, 0, 0))
    return pl.pallas_call(
        lambda *refs: add_kernel(chunks, len(after), *refs),
        grid=(1,),
        out_shape=tuple(jax.ShapeDtypeStruct(side.shape, f32) for side in sides),
        in_specs=[whole, whole] + [lower, upper] * chunks + [ANY] * len(after),
        out_specs=(lower, upper) * chunks,
        input_output_aliases={2 + i: i for i in range(2 * chunks)},
        compiler_params=params(),
        cost_estimate=cost(1.5 * chunks),
        interpret=INTERPRET,
        name="add_arrived",
    )(near, far, *sides, *after)


def second_hop(right, left):
    right = to_right(right)
    left = to_left(left)
    return right, left


def place_kernel(units, tables, waits, place_ref, slots_ref, *refs):
    ins = refs[: tables + 3]
    outs = refs[tables + 3 + waits :]
    out_ref, table_ref = outs[0], outs[1]
    plane = place_ref[0]
    size = ins[0].shape[0]
    for i in range(tables):
        table_ref[i * size : (i + 1) * size] = ins[i][...]
    keep, right, left = ins[tables:]
    if tables == 2:
        table_ref[2 * size : 3 * size] = ins[1][...]
    at = min(tables, 1) * size
    table_ref[at : at + size] = keep[...] + right[...] + left[...]

    def body(owner, carry):
        position = (owner // 2) * 8 + 2 * plane + owner % 2
        for u, s in enumerate(units):
            out_ref[owner, u] = table_ref[slots_ref[s, position]]
        return carry

    lax.fori_loop(0, OWNERS, body, 0)


def place_slots(units, plane, slots, tables, parts, keep_table, after=()):
    size, rows, width = parts[0].shape
    count = len(tables) + 1
    table = jax.ShapeDtypeStruct((count * size, rows, width), f32)
    out = jax.ShapeDtypeStruct((OWNERS, len(units), rows, width), f32)
    return pl.pallas_call(
        lambda *refs: place_kernel(units, len(tables), len(after), *refs),
        out_shape=(out, table) if keep_table else (out,),
        in_specs=[SMEM, SMEM] + [VMEM] * (len(tables) + 3) + [ANY] * len(after),
        out_specs=(VMEM, VMEM) if keep_table else (VMEM,),
        scratch_shapes=[] if keep_table else [pltpu.VMEM(table.shape, f32)],
        compiler_params=params(),
        cost_estimate=cost(3),
        interpret=INTERPRET,
        name="place_slots",
    )(plane, slots, *tables, *parts, *after)


def to_owners(value):
    return lax.all_to_all(value, PLANE, split_axis=0, concat_axis=0, tiled=True)


def two_terms(value):
    high = value.astype(bf16)
    return high, (value - high.astype(f32)).astype(bf16)


def curvature_kernel(first, units, weight_ref, field_ref, turn_ref, back_ref, occupied_ref, *refs):
    out_ref = refs[-1]
    unit = pl.program_id(0)
    sources = field_ref.shape[0] // (units * 40)
    n = field_ref.shape[1]
    stride = units * 40

    def plane_of(kind):
        return jnp.concatenate(
            [field_ref[pl.ds(unit * 40 + kind * 4 + r, sources, stride=stride), :] for r in range(4)], axis=0
        )

    matrices = jnp.concatenate(
        [jnp.concatenate([plane_of(2 * c), plane_of(2 * c + 1)], axis=1) for c in range(5)], axis=0
    )
    high, low = two_terms(matrices)
    vectors = turn_ref[0]
    rotated = jnp.dot(high, vectors, preferred_element_type=f32) + jnp.dot(low, vectors, preferred_element_type=f32)
    stacked = jnp.concatenate(
        [
            jnp.concatenate([rotated[c * n : (c + 1) * n, :n] for c in range(5)], axis=1),
            jnp.concatenate([rotated[c * n : (c + 1) * n, n:] for c in range(5)], axis=1),
        ],
        axis=0,
    )
    back = back_ref[0]
    high, low = two_terms(stacked)
    bar = jnp.dot(back, high, preferred_element_type=f32) + jnp.dot(back, low, preferred_element_type=f32)
    bar_real, bar_imag = bar[:n], bar[n:]
    diagonal = jnp.where(iota((n, n), 0) == iota((n, n), 1), bar_real[:, :n], 0.0)
    spacing = jnp.sum(diagonal, axis=0, keepdims=True) - jnp.sum(diagonal, axis=1, keepdims=True)
    smoothed = spacing / (spacing * spacing + broadening)

    def pick(value, c):
        return value[:, (c + 1) * n : (c + 2) * n]

    xcov_real = pick(bar_real, 2) + smoothed * pick(bar_real, 0)
    xcov_imag = pick(bar_imag, 2) + smoothed * pick(bar_imag, 0)
    ycov_real = pick(bar_real, 3) + smoothed * pick(bar_real, 1)
    ycov_imag = pick(bar_imag, 3) + smoothed * pick(bar_imag, 1)
    s = first + unit
    filled = occupied_ref[pl.ds(s, 1), :].astype(f32)
    filled_down = jnp.broadcast_to(filled, (n, n)).T
    pairing = filled_down * (1.0 - filled)
    product = pairing * (xcov_real * ycov_imag.T + xcov_imag * ycov_real.T)
    berry = jnp.sum(jnp.sum(product, axis=0, keepdims=True), axis=1, keepdims=True) * (-2.0 / n)
    weight = weight_ref[s]
    lane = iota((1, BLOCKS), 1)
    result = jnp.where((lane == s) & (weight > 0.0), weight * berry, 0.0)
    before = jnp.where(unit == 0, 0.0, out_ref[...])
    out_ref[...] = result + before


def curvature(first, units, weight, arrived, vectors, adjoint, occupied, after=()):
    width = arrived.shape[-1]
    flat = arrived.reshape(-1, width)
    matrix = pl.BlockSpec((1, 2 * width, 2 * width), lambda u: (first + u, 0, 0))
    return pl.pallas_call(
        lambda *refs: curvature_kernel(first, units, *refs),
        grid=(units,),
        out_shape=jax.ShapeDtypeStruct((1, BLOCKS), f32),
        in_specs=[
            SMEM,
            pl.BlockSpec(flat.shape, lambda u: (0, 0)),
            matrix,
            matrix,
            pl.BlockSpec(occupied.shape, lambda u: (0, 0)),
        ]
        + [ANY] * len(after),
        out_specs=pl.BlockSpec((1, BLOCKS), lambda u: (0, 0)),
        compiler_params=params(),
        cost_estimate=cost(2.5 * units),
        interpret=INTERPRET,
        name="curvature",
    )(weight, flat, vectors, adjoint, occupied, *after)


def vector_kernel(eigvecs_ref, turn_ref, back_ref, wide_ref):
    n = eigvecs_ref.shape[2]
    wide_ref[...] = eigvecs_ref[0].astype(f32)
    real, imag = (wide_ref[pl.ds(part, n, stride=2), :].astype(bf16) for part in range(2))
    turn_ref[0, :n, :n] = real
    turn_ref[0, :n, n:] = imag
    turn_ref[0, n:, :n] = -imag
    turn_ref[0, n:, n:] = real
    group = n // OWNERS
    for part in range(2):
        packed = jnp.concatenate(
            [wide_ref[pl.ds(2 * r + part, OWNERS, stride=2 * group), :] for r in range(group)], axis=0
        )
        turned = packed.T
        if part == 0:
            back_ref[0, :n, :n] = turned.astype(bf16)
            back_ref[0, n:, n:] = turned.astype(bf16)
        else:
            back_ref[0, :n, n:] = turned.astype(bf16)
            back_ref[0, n:, :n] = (-turned).astype(bf16)


def vector_matrices(eigvecs):
    slots, width = eigvecs.shape[0], eigvecs.shape[1]
    shape = jax.ShapeDtypeStruct((slots, 2 * width, 2 * width), bf16)
    square = pl.BlockSpec((1, 2 * width, 2 * width), lambda i: (i, 0, 0))
    return pl.pallas_call(
        vector_kernel,
        grid=(slots,),
        out_shape=(shape, shape),
        in_specs=[pl.BlockSpec((1, 2 * width, width), lambda i: (i, 0, 0))],
        out_specs=(square, square),
        scratch_shapes=[pltpu.VMEM((2 * width, width), f32)],
        compiler_params=params(),
        cost_estimate=cost(2),
        interpret=INTERPRET,
        name="vector_matrices",
    )(eigvecs.reshape(slots, 2 * width, width))


def body(base_k, counts, block_order, lattice, real_space, eigvecs, occupied):
    plane, core = lax.axis_index("row_0"), lax.axis_index("row_1")
    row = plane * 2 + core
    plane_ref = plane.reshape(1).astype(jnp.int32)
    core_ref = core.reshape(1).astype(jnp.int32)
    depth, _, slab, _, width = real_space.shape

    own_base = lax.dynamic_slice_in_dim(base_k, row, 1, 0)
    own_count = lax.dynamic_slice_in_dim(counts, row, 1, 0).astype(f32)[:, None]
    mine = jnp.concatenate([own_base, own_count, block_order.astype(f32)[:, None]], axis=1)
    mine = jnp.pad(mine, ((0, 0), (0, BLOCKS - 5)))
    line = lax.all_to_all(jnp.broadcast_to(mine[None], (8, 1, BLOCKS)), ROW, 0, 0, tiled=True)

    own, send = split_rows(real_space.reshape(depth, 6 * slab, width), core_ref)
    swap = [(0, 1), (1, 0)]
    other = lax.ppermute(send, "row_1", swap)
    own_coords = jnp.pad(lattice.T.astype(f32), ((0, 5), (0, 0)))
    coords = jnp.concatenate([own_coords, lax.ppermute(own_coords, "row_1", swap)], axis=1)

    lines = jnp.broadcast_to(line.reshape(1, 8, BLOCKS), (16, 8, BLOCKS))
    table = lax.all_to_all(lines, KA, 0, 0, tiled=True).reshape(BLOCKS, BLOCKS)
    turning, back = vector_matrices(eigvecs)
    points, slots, weights = find_points(table, plane_ref)
    position = (lax.axis_index(KA) * 8 + row).astype(jnp.int32)
    weight = lax.dynamic_slice(weights, (jnp.int32(0), position), (SUB, 1)).reshape(SUB)

    own = own.reshape(3, 2 * depth, -1)
    other = other.reshape(3, 2 * depth, -1)
    half = OWNERS // 2
    opposite = (half, half, OWNERS, OWNERS)
    others = (OWNERS, OWNERS, OWNERS)

    def rest(chunk, after):
        low = 3 * OWNERS * (1 + chunk)
        return fourier(points, low, low + 3 * OWNERS, others, coords, own, other, 6, after)

    near0, far0, near13, far13, other = fourier(
        points, 0, 3 * OWNERS, opposite, coords, own, other, 6, narrowing=True
    )
    hop0 = first_hop(near0, far0)
    hop13 = first_hop(near13, far13)
    right0, left0, keep0 = rest(0, ())
    right0, left0 = add_arrived(*hop0, (right0, left0))
    ring0 = second_hop(right0, left0)
    right1, left1, keep1 = rest(1, (right0,))
    right3, left3, keep3 = rest(2, (keep1,))
    right1, left1, right3, left3 = add_arrived(*hop13, (right1, left1, right3, left3))
    ring1 = second_hop(right1, left1)
    ring3 = second_hop(right3, left3)

    def further(_):
        low = 12 * OWNERS
        near, far, right, left, keep = fourier(
            points, low, low + 4 * OWNERS, (half, half) + others, coords, own, other, 8
        )
        right, left = second_hop(*add_arrived(*first_hop(near, far), (right, left)))
        return keep + right + left

    extra = lax.cond(slots[0, 0] > 2 * OWNERS, further, lambda _: jnp.zeros(keep0.shape, f32), 0)

    placed1, sum0 = place_slots((1,), plane_ref, slots, [], (keep0, *ring0), True, (right3,))
    unit1 = to_owners(placed1)
    (placed23,) = place_slots((2, 3), plane_ref, slots, [sum0, extra], (keep1, *ring1), False)
    unit23 = to_owners(placed23)
    curve1 = curvature(1, 1, weight, unit1, turning, back, occupied, (placed23,))
    unit0 = to_owners(keep3 + ring3[0] + ring3[1])
    curve23 = curvature(2, 2, weight, unit23, turning, back, occupied, (curve1,))
    curve0 = curvature(0, 1, weight, unit0, turning, back, occupied, (curve23,))
    return (curve1 + curve23 + curve0)[0, :SUB]


def solution(mesh):
    finer = Mesh(mesh.devices.reshape(4, 4, 4, 2), ("ka_0", "ka_1", "row_0", "row_1"))
    placed = (
        P(KA, None),
        P(KA),
        P(KA_ROW),
        P(ROW, None),
        P(ROW, None, KA, None, None),
        P(KA_ROW, None, None, None),
        P(KA_ROW, None),
    )
    return jax.shard_map(body, mesh=finer, in_specs=placed, out_specs=P(KA_ROW), check_vma=False)
```

```python
import math

import jax
import jax.numpy as jnp
from jax import lax
from jax.experimental import pallas as pl
from jax.experimental.pallas import tpu as pltpu
from jax.sharding import Mesh
from jax.sharding import PartitionSpec as P

SUB = 4
KA = ("ka_0", "ka_1")
KA_ROW = ("ka_0", "ka_1", "row_0", "row_1")
ROW = ("row_0", "row_1")
PLANE = ("ka_0", "ka_1", "row_1")
INTERPRET = False

broadening = 1.0
refine_step = (0.05, 0.03, 0.02)

f32 = jnp.float32
bf16 = jnp.bfloat16
VMEM = pl.BlockSpec(memory_space=pltpu.VMEM)
SMEM = pl.BlockSpec(memory_space=pltpu.SMEM)
NX = 4
OWNERS = 32
BLOCKS = 128


def params(mebibytes):
    return pltpu.CompilerParams(vmem_limit_bytes=mebibytes << 20)


ANY = pl.BlockSpec(memory_space=pl.ANY)


def cost(microseconds):
    return pl.CostEstimate(flops=int(microseconds * 2.5e8), bytes_accessed=0, transcendentals=0)


def iota(shape, dim):
    return lax.broadcasted_iota(jnp.int32, shape, dim)


def place_of(position):
    plane = (position % 8) // 2
    owner = (position // 8) * 2 + position % 2
    return plane, owner


def index_kernel(place_ref, table_ref, points_ref, slots_ref, weight_ref):
    my_plane = place_ref[0]
    table = table_ref[...]
    turned = table.T
    square = (BLOCKS, BLOCKS)
    order_down = table[:, 4:5].astype(jnp.int32)
    order_along = turned[4:5, :].astype(jnp.int32)
    here_down = order_down == iota(square, 1)
    here_along = iota(square, 0) == order_along

    def along(column):
        return jnp.sum(jnp.where(here_along, table[:, column : column + 1], 0.0), axis=0, keepdims=True)

    base = [along(axis) for axis in range(3)]
    count = along(3)
    count_down = jnp.sum(jnp.where(here_down, turned[3:4, :], 0.0), axis=1, keepdims=True)

    plane_down, owner_down = place_of(iota(square, 0))
    plane_along, owner_along = place_of(iota(square, 1))
    mates = plane_down == plane_along
    ahead = mates & (owner_down < owner_along)
    plane_row, owner_row = place_of(iota((1, BLOCKS), 1))
    away = (plane_row - my_plane + NX) % NX
    seat = jnp.where(away == 1, 0, jnp.where(away == 3, 1, 2))

    def row_of(chunk, within):
        opposite = OWNERS * chunk + within
        apart = 3 * OWNERS * (1 + chunk) + seat * OWNERS + within
        spare = 12 * OWNERS + jnp.where(away == 2, 0, 1 + seat) * OWNERS + within
        return jnp.where(chunk == 3, spare, jnp.where(away == 2, opposite, apart))

    rows = 4 * OWNERS * NX
    entry = iota((rows, BLOCKS), 0)
    lane = iota((rows, BLOCKS), 1)
    gathered = [jnp.zeros((rows, BLOCKS), f32) for _ in range(3)]
    before = jnp.zeros((1, BLOCKS), f32)
    slots_ref[...] = jnp.zeros((8, BLOCKS), jnp.int32)
    weight_ref[...] = jnp.zeros((8, BLOCKS), f32)
    for s in range(SUB):
        fraction = (s + 0.5) / count - 0.5
        points = [base[axis] + fraction * refine_step[axis] for axis in range(3)]
        alive = count > s
        weight_ref[s : s + 1, :] = jnp.where(alive, 1.0 / count, 0.0)
        if s == 0:
            chunk, within = jnp.full((1, BLOCKS), 2, jnp.int32), owner_row
        else:
            live_down = count_down > s
            rank = before + jnp.sum(jnp.where(ahead & live_down, 1.0, 0.0), axis=0, keepdims=True)
            before = before + jnp.sum(jnp.where(mates & live_down, 1.0, 0.0), axis=0, keepdims=True)
            rank = jnp.where(alive, rank, 0.0).astype(jnp.int32)
            slots_ref[s : s + 1, :] = rank
            chunk, within = rank // OWNERS, rank % OWNERS
            chunk = jnp.where(chunk == 2, 3, chunk)
        match = entry == jnp.where(alive, row_of(chunk, within), -1)
        for axis in range(3):
            gathered[axis] = gathered[axis] + jnp.where(match, points[axis], 0.0)
    most = jnp.max(before, axis=1, keepdims=True)
    slots_ref[0:1, :] = jnp.broadcast_to(most, (1, BLOCKS)).astype(jnp.int32)
    points = jnp.zeros((rows, BLOCKS), f32)
    for axis in range(3):
        points = jnp.where(lane == axis, jnp.sum(gathered[axis], axis=1, keepdims=True), points)
    points_ref[...] = points


def find_points(table, plane):
    rows = OWNERS * NX
    return pl.pallas_call(
        index_kernel,
        out_shape=(
            jax.ShapeDtypeStruct((4 * rows, BLOCKS), f32),
            jax.ShapeDtypeStruct((8, BLOCKS), jnp.int32),
            jax.ShapeDtypeStruct((8, BLOCKS), f32),
        ),
        in_specs=[SMEM, VMEM],
        out_specs=(VMEM, VMEM, VMEM),
        compiler_params=params(8),
        cost_estimate=cost(2),
        interpret=INTERPRET,
        name="find_points",
    )(plane, table)


def split_kernel(dtype, core_ref, space_ref, out_ref, wide_ref):
    core = core_ref[0] if dtype == bf16 else 1 - core_ref[0]
    depth, rows, width = space_ref.shape
    half = rows // 12
    pitch = wide_ref.shape[0] // depth
    for first in range(0, depth, 8):
        wide = space_ref[first : first + 8].astype(f32)
        for r in range(8):
            wide_ref[(first + r) * pitch : (first + r) * pitch + rows, :] = wide[r]
    for matrix in range(3):
        for part in range(2):
            for r in range(half):
                at = matrix * (rows // 3) + 2 * (half * core + r) + part
                lanes = slice(r * width, (r + 1) * width)
                out_ref[matrix, part, :, lanes] = wide_ref[pl.ds(at, depth, stride=pitch), :].astype(dtype)


def split_rows(space, core, dtype, microseconds):
    depth, rows, width = space.shape
    block = min(depth, 128)
    lanes = rows // 12 * width
    return pl.pallas_call(
        lambda *refs: split_kernel(dtype, *refs),
        grid=(depth // block,),
        out_shape=jax.ShapeDtypeStruct((3, 2, depth, lanes), dtype),
        in_specs=[SMEM, pl.BlockSpec((block, rows, width), lambda i: (i, 0, 0))],
        out_specs=pl.BlockSpec((3, 2, block, lanes), lambda i: (0, 0, i, 0)),
        scratch_shapes=[pltpu.VMEM((block * (rows + 8), width), f32)],
        compiler_params=params(16),
        cost_estimate=cost(microseconds),
        interpret=INTERPRET,
        name="split_rows",
    )(core, space)


def turn(points, coords):
    turns = points[:, 0:1] * coords[0:1, :] + points[:, 1:2] * coords[1:2, :] + points[:, 2:3] * coords[2:3, :]
    rest = turns - jnp.floor(turns + 0.5)
    quarter = jnp.floor(4.0 * rest + 0.5)
    angle = (rest - 0.25 * quarter) * (2.0 * math.pi)
    square = angle * angle
    sine = angle * (1.0 + square * (-1.0 / 6 + square * (1.0 / 120 + square * (-1.0 / 5040 + square * (1.0 / 362880)))))
    cosine = 1.0 + square * (-0.5 + square * (1.0 / 24 + square * (-1.0 / 720 + square * (1.0 / 40320 - square / 3628800))))
    odd = jnp.abs(quarter) == 1.0
    first = jnp.where(odd, sine, cosine)
    second = jnp.where(odd, cosine, sine)
    cos_sign = jnp.where((quarter == 1.0) | (jnp.abs(quarter) == 2.0), -1.0, 1.0)
    sin_sign = jnp.where((quarter == -1.0) | (jnp.abs(quarter) == 2.0), -1.0, 1.0)
    return first * cos_sign, second * sin_sign


def fourier_kernel(low, high, narrowing, waits, points_ref, coords_ref, own_ref, other_ref, *refs):
    out_refs, phase_ref = refs[waits:-1], refs[-1]
    step = pl.program_id(0)
    count = high - low
    depth = coords_ref.shape[1] // 2
    tile = 16

    @pl.when(step == 0)
    def _():
        def rows_of(i, carry):
            first = pl.multiple_of(i * tile, tile)
            points = points_ref[pl.ds(low + first, tile), :]
            for source in range(2):
                coords = coords_ref[:, source * depth : (source + 1) * depth]
                cosine, sine = turn(points, coords)
                at_real = slice(source * 2 * depth, source * 2 * depth + depth)
                at_imag = slice(source * 2 * depth + depth, source * 2 * depth + 2 * depth)
                pairs = [(cosine, sine)]
                for axis in range(2):
                    coord = coords[axis : axis + 1, :]
                    pairs.append((-coord * sine, coord * cosine))
                for kind, (real, imag) in enumerate(pairs):
                    real_rows = pl.ds(2 * kind * count + first, tile)
                    imag_rows = pl.ds((2 * kind + 1) * count + first, tile)
                    phase_ref[real_rows, at_real] = real.astype(bf16)
                    phase_ref[real_rows, at_imag] = (-imag).astype(bf16)
                    phase_ref[imag_rows, at_real] = imag.astype(bf16)
                    phase_ref[imag_rows, at_imag] = real.astype(bf16)
            return carry

        lax.fori_loop(0, count // tile, rows_of, 0)

    if narrowing:
        other_value = other_ref[0].astype(bf16)
        out_refs[-1][0] = other_value
    else:
        other_value = other_ref[0]

    def store(product, kinds, first_kind, first_row):
        width = product.shape[1] // 2
        for kind in range(kinds):
            for half in range(2):
                block = product[kind * count : (kind + 1) * count, half * width : (half + 1) * width]
                at = (first_kind + kind) * 4 + first_row + half
                start = 0
                for ref in out_refs[: len(out_refs) - narrowing]:
                    size = ref.shape[0] // 40
                    ref[pl.ds(at, size, stride=40), :] = block[start : start + size]
                    start += size

    def product(kinds):
        rows = slice(0, kinds * count)
        return jnp.dot(phase_ref[rows, : 2 * depth], own_ref[0], preferred_element_type=f32) + jnp.dot(
            phase_ref[rows, 2 * depth :], other_value, preferred_element_type=f32
        )

    @pl.when(step < 2)
    def _():
        store(product(6), 6, 0, 2 * step)

    @pl.when(step >= 2)
    def _():
        store(product(2), 2, 6 + 2 * (step // 2 - 1), 2 * (step % 2))


def fourier(points, low, high, sizes, coords, own, other, microseconds, after=(), narrowing=False):
    depth2 = own.shape[1]
    width = own.shape[2] // 4
    spec = pl.BlockSpec((1, depth2, 2 * width), lambda j: (j // 2, 0, j % 2))
    shapes = [jax.ShapeDtypeStruct((size * 40, width), f32) for size in sizes]
    specs = [pl.BlockSpec(shape.shape, lambda j: (0, 0)) for shape in shapes]
    if narrowing:
        shapes.append(jax.ShapeDtypeStruct(own.shape, bf16))
        specs.append(spec)
    outs = pl.pallas_call(
        lambda *refs: fourier_kernel(low, high, int(narrowing), len(after), *refs),
        grid=(6,),
        out_shape=tuple(shapes),
        in_specs=[
            pl.BlockSpec(points.shape, lambda j: (0, 0)),
            pl.BlockSpec(coords.shape, lambda j: (0, 0)),
            spec,
            spec,
        ]
        + [ANY] * len(after),
        out_specs=tuple(specs),
        scratch_shapes=[pltpu.VMEM((6 * (high - low), 2 * depth2), bf16)],
        compiler_params=params(20),
        cost_estimate=cost(microseconds),
        interpret=INTERPRET,
        name="fourier",
    )(points, coords, own, other, *after)
    return tuple(out.reshape(-1, 40, width) for out in outs[: len(sizes)]) + tuple(outs[len(sizes) :])


def to_right(value):
    return lax.ppermute(value, "row_0", [(i, (i + 1) % NX) for i in range(NX)])


def to_left(value):
    return lax.ppermute(value, "row_0", [(i, (i - 1) % NX) for i in range(NX)])


def first_hop(near, far):
    near = to_right(near)
    far = to_left(far)
    return near, far


def add_kernel(chunks, waits, near_ref, far_ref, *refs):
    ins, outs = refs[: 2 * chunks], refs[2 * chunks + waits :]
    size = near_ref.shape[0] // chunks
    for c in range(chunks):
        rows = slice(c * size, (c + 1) * size)
        outs[2 * c][...] = ins[2 * c][...] + near_ref[rows]
        outs[2 * c + 1][...] = ins[2 * c + 1][...] + far_ref[rows]


def add_arrived(near, far, sides, after=()):
    chunks = len(sides) // 2
    count, rows, width = near.shape
    size = count // chunks
    whole = pl.BlockSpec(near.shape, lambda i: (0, 0, 0))
    lower = pl.BlockSpec((size, rows, width), lambda i: (0, 0, 0))
    upper = pl.BlockSpec((size, rows, width), lambda i: (1, 0, 0))
    return pl.pallas_call(
        lambda *refs: add_kernel(chunks, len(after), *refs),
        grid=(1,),
        out_shape=tuple(jax.ShapeDtypeStruct(side.shape, f32) for side in sides),
        in_specs=[whole, whole] + [lower, upper] * chunks + [ANY] * len(after),
        out_specs=(lower, upper) * chunks,
        input_output_aliases={2 + i: i for i in range(2 * chunks)},
        compiler_params=params(8),
        cost_estimate=cost(1.5 * chunks),
        interpret=INTERPRET,
        name="add_arrived",
    )(near, far, *sides, *after)


def second_hop(right, left):
    right = to_right(right)
    left = to_left(left)
    return right, left


def place_kernel(units, tables, waits, place_ref, slots_ref, *refs):
    ins = refs[: tables + 3]
    outs = refs[tables + 3 + waits :]
    out_ref, table_ref = outs[0], outs[1]
    plane = place_ref[0]
    size = ins[0].shape[0]
    for i in range(tables):
        table_ref[i * size : (i + 1) * size] = ins[i][...]
    keep, right, left = ins[tables:]
    if tables == 2:
        table_ref[2 * size : 3 * size] = ins[1][...]
    at = min(tables, 1) * size
    table_ref[at : at + size] = keep[...] + right[...] + left[...]

    def body(owner, carry):
        position = (owner // 2) * 8 + 2 * plane + owner % 2
        for u, s in enumerate(units):
            out_ref[owner, u] = table_ref[slots_ref[s, position]]
        return carry

    lax.fori_loop(0, OWNERS, body, 0)


def place_slots(units, plane, slots, tables, parts, keep_table, after=()):
    size, rows, width = parts[0].shape
    count = len(tables) + 1
    table = jax.ShapeDtypeStruct((count * size, rows, width), f32)
    out = jax.ShapeDtypeStruct((OWNERS, len(units), rows, width), f32)
    return pl.pallas_call(
        lambda *refs: place_kernel(units, len(tables), len(after), *refs),
        out_shape=(out, table) if keep_table else (out,),
        in_specs=[SMEM, SMEM] + [VMEM] * (len(tables) + 3) + [ANY] * len(after),
        out_specs=(VMEM, VMEM) if keep_table else (VMEM,),
        scratch_shapes=[] if keep_table else [pltpu.VMEM(table.shape, f32)],
        compiler_params=params(14),
        cost_estimate=cost(3),
        interpret=INTERPRET,
        name="place_slots",
    )(plane, slots, *tables, *parts, *after)


def to_owners(value):
    return lax.all_to_all(value, PLANE, split_axis=0, concat_axis=0, tiled=True)


def two_terms(value):
    high = value.astype(bf16)
    return high, (value - high.astype(f32)).astype(bf16)


def curvature_kernel(first, units, adding, weight_ref, field_ref, turn_ref, back_ref, occupied_ref, *refs):
    out_ref = refs[-1]
    previous = refs[0][...] if adding else 0.0
    unit = pl.program_id(0)
    sources = field_ref.shape[0] // (units * 40)
    n = field_ref.shape[1]
    stride = units * 40

    def plane_of(kind):
        return jnp.concatenate(
            [field_ref[pl.ds(unit * 40 + kind * 4 + r, sources, stride=stride), :] for r in range(4)], axis=0
        )

    matrices = jnp.concatenate(
        [jnp.concatenate([plane_of(2 * c), plane_of(2 * c + 1)], axis=1) for c in range(5)], axis=0
    )
    high, low = two_terms(matrices)
    vectors = turn_ref[0]
    rotated = jnp.dot(high, vectors, preferred_element_type=f32) + jnp.dot(low, vectors, preferred_element_type=f32)
    stacked = jnp.concatenate(
        [
            jnp.concatenate([rotated[c * n : (c + 1) * n, :n] for c in range(5)], axis=1),
            jnp.concatenate([rotated[c * n : (c + 1) * n, n:] for c in range(5)], axis=1),
        ],
        axis=0,
    )
    back = back_ref[0]
    high, low = two_terms(stacked)
    bar = jnp.dot(back, high, preferred_element_type=f32) + jnp.dot(back, low, preferred_element_type=f32)
    bar_real, bar_imag = bar[:n], bar[n:]
    diagonal = jnp.where(iota((n, n), 0) == iota((n, n), 1), bar_real[:, :n], 0.0)
    spacing = jnp.sum(diagonal, axis=0, keepdims=True) - jnp.sum(diagonal, axis=1, keepdims=True)
    smoothed = spacing / (spacing * spacing + broadening)

    def pick(value, c):
        return value[:, (c + 1) * n : (c + 2) * n]

    xcov_real = pick(bar_real, 2) + smoothed * pick(bar_real, 0)
    xcov_imag = pick(bar_imag, 2) + smoothed * pick(bar_imag, 0)
    ycov_real = pick(bar_real, 3) + smoothed * pick(bar_real, 1)
    ycov_imag = pick(bar_imag, 3) + smoothed * pick(bar_imag, 1)
    s = first + unit
    filled = occupied_ref[pl.ds(s, 1), :].astype(f32)
    filled_down = jnp.broadcast_to(filled, (n, n)).T
    pairing = filled_down * (1.0 - filled)
    product = pairing * (xcov_real * ycov_imag.T + xcov_imag * ycov_real.T)
    berry = jnp.sum(jnp.sum(product, axis=0, keepdims=True), axis=1, keepdims=True) * (-2.0 / n)
    weight = weight_ref[s]
    lane = iota((1, BLOCKS), 1)
    result = jnp.where((lane == s) & (weight > 0.0), weight * berry, 0.0)
    before = jnp.where(unit == 0, previous, out_ref[...])
    out_ref[...] = result + before


def curvature(first, units, weight, arrived, vectors, adjoint, occupied, previous=(), after=()):
    width = arrived.shape[-1]
    flat = arrived.reshape(-1, width)
    matrix = pl.BlockSpec((1, 2 * width, 2 * width), lambda u: (first + u, 0, 0))
    return pl.pallas_call(
        lambda *refs: curvature_kernel(first, units, len(previous), *refs),
        grid=(units,),
        out_shape=jax.ShapeDtypeStruct((1, BLOCKS), f32),
        in_specs=[
            SMEM,
            pl.BlockSpec(flat.shape, lambda u: (0, 0)),
            matrix,
            matrix,
            pl.BlockSpec(occupied.shape, lambda u: (0, 0)),
        ]
        + [pl.BlockSpec((1, BLOCKS), lambda u: (0, 0))] * len(previous)
        + [ANY] * len(after),
        out_specs=pl.BlockSpec((1, BLOCKS), lambda u: (0, 0)),
        compiler_params=params(12),
        cost_estimate=cost(2.5 * units),
        interpret=INTERPRET,
        name="curvature",
    )(weight, flat, vectors, adjoint, occupied, *previous, *after)


def vector_kernel(eigvecs_ref, turn_ref, back_ref, wide_ref):
    n = eigvecs_ref.shape[2]
    wide_ref[...] = eigvecs_ref[0].astype(f32)
    real, imag = (wide_ref[pl.ds(part, n, stride=2), :].astype(bf16) for part in range(2))
    turn_ref[0, :n, :n] = real
    turn_ref[0, :n, n:] = imag
    turn_ref[0, n:, :n] = -imag
    turn_ref[0, n:, n:] = real
    group = n // OWNERS
    for part in range(2):
        packed = jnp.concatenate(
            [wide_ref[pl.ds(2 * r + part, OWNERS, stride=2 * group), :] for r in range(group)], axis=0
        )
        turned = packed.T
        if part == 0:
            back_ref[0, :n, :n] = turned.astype(bf16)
            back_ref[0, n:, n:] = turned.astype(bf16)
        else:
            back_ref[0, :n, n:] = turned.astype(bf16)
            back_ref[0, n:, :n] = (-turned).astype(bf16)


def vector_matrices(eigvecs):
    slots, width = eigvecs.shape[0], eigvecs.shape[1]
    shape = jax.ShapeDtypeStruct((slots, 2 * width, 2 * width), bf16)
    square = pl.BlockSpec((1, 2 * width, 2 * width), lambda i: (i, 0, 0))
    return pl.pallas_call(
        vector_kernel,
        grid=(slots,),
        out_shape=(shape, shape),
        in_specs=[pl.BlockSpec((1, 2 * width, width), lambda i: (i, 0, 0))],
        out_specs=(square, square),
        scratch_shapes=[pltpu.VMEM((2 * width, width), f32)],
        compiler_params=params(4),
        cost_estimate=cost(2),
        interpret=INTERPRET,
        name="vector_matrices",
    )(eigvecs.reshape(slots, 2 * width, width))


def body(base_k, counts, block_order, lattice, real_space, eigvecs, occupied):
    plane, core = lax.axis_index("row_0"), lax.axis_index("row_1")
    row = plane * 2 + core
    plane_ref = plane.reshape(1).astype(jnp.int32)
    core_ref = core.reshape(1).astype(jnp.int32)
    depth, _, slab, _, width = real_space.shape

    own_base = lax.dynamic_slice_in_dim(base_k, row, 1, 0)
    own_count = lax.dynamic_slice_in_dim(counts, row, 1, 0).astype(f32)[:, None]
    mine = jnp.concatenate([own_base, own_count, block_order.astype(f32)[:, None]], axis=1)
    mine = jnp.pad(mine, ((0, 0), (0, BLOCKS - 5)))
    space = real_space.reshape(depth, 6 * slab, width)
    swap = [(0, 1), (1, 0)]
    send = split_rows(space, core_ref, f32, 5)
    other = lax.ppermute(send, "row_1", swap)
    own_coords = jnp.pad(lattice.T.astype(f32), ((0, 5), (0, 0)))
    coords = jnp.concatenate([own_coords, lax.ppermute(own_coords, "row_1", swap)], axis=1)

    table = lax.all_to_all(jnp.broadcast_to(mine[None], (BLOCKS, 1, BLOCKS)), KA_ROW, 0, 0, tiled=True)
    table = table.reshape(BLOCKS, BLOCKS)
    own = split_rows(space, core_ref, bf16, 4)
    turning, back = vector_matrices(eigvecs)
    points, slots, weights = find_points(table, plane_ref)
    position = (lax.axis_index(KA) * 8 + row).astype(jnp.int32)
    weight = lax.dynamic_slice(weights, (jnp.int32(0), position), (SUB, 1)).reshape(SUB)

    own = own.reshape(3, 2 * depth, -1)
    other = other.reshape(3, 2 * depth, -1)
    half = OWNERS // 2
    others = (OWNERS, OWNERS, OWNERS)

    def sums(low, sizes, microseconds, after=(), narrowing=False):
        return fourier(points, low, low + sum(sizes), sizes, coords, own, other, microseconds, after, narrowing)

    def rest(chunk, after):
        return sums(3 * OWNERS * (1 + chunk), others, 5, after)

    near0, far0, other = sums(0, (half, half), 5, (), True)
    hop0 = first_hop(near0, far0)
    near1, far1, near3, far3 = sums(OWNERS, (half,) * 4, 4, (near0,))
    hop1 = first_hop(near1, far1)
    right0, left0, keep0 = rest(0, (near1,))
    right0, left0 = add_arrived(*hop0, (right0, left0))
    ring0 = second_hop(right0, left0)
    right1, left1, keep1 = rest(1, (right0,))
    right1, left1 = add_arrived(*hop1, (right1, left1))
    ring1 = second_hop(right1, left1)
    hop3 = first_hop(near3, far3)
    right3, left3, keep3 = rest(2, (right1,))

    def further(_):
        low = 12 * OWNERS
        near, far, right, left, keep = sums(low, (half, half) + others, 8)
        right, left = second_hop(*add_arrived(*first_hop(near, far), (right, left)))
        return keep + right + left

    extra = lax.cond(slots[0, 0] > 2 * OWNERS, further, lambda _: jnp.zeros(keep0.shape, f32), 0)

    placed1, sum0 = place_slots((1,), plane_ref, slots, [], (keep0, *ring0), True, (keep3,))
    unit1 = to_owners(placed1)
    (placed23,) = place_slots((2, 3), plane_ref, slots, [sum0, extra], (keep1, *ring1), False)
    unit23 = to_owners(placed23)
    right3, left3 = add_arrived(*hop3, (right3, left3), (placed23,))
    ring3 = second_hop(right3, left3)
    curve1 = curvature(1, 1, weight, unit1, turning, back, occupied, (), (right3,))
    unit0 = to_owners(keep3 + ring3[0] + ring3[1])
    curve23 = curvature(2, 2, weight, unit23, turning, back, occupied, (curve1,))
    return curvature(0, 1, weight, unit0, turning, back, occupied, (curve23,)).reshape(BLOCKS)[:SUB]


def solution(mesh):
    finer = Mesh(mesh.devices.reshape(4, 4, 4, 2), ("ka_0", "ka_1", "row_0", "row_1"))
    placed = (
        P(KA, None),
        P(KA),
        P(KA_ROW),
        P(ROW, None),
        P(ROW, None, KA, None, None),
        P(KA_ROW, None, None, None),
        P(KA_ROW, None),
    )
    return jax.shard_map(body, mesh=finer, in_specs=placed, out_specs=P(KA_ROW), check_vma=False)
```

```python
import math

import jax
import jax.numpy as jnp
from jax import lax
from jax.experimental import pallas as pl
from jax.experimental.pallas import tpu as pltpu
from jax.sharding import Mesh
from jax.sharding import PartitionSpec as P

SUB = 4
KA = ("ka_0", "ka_1")
KA_ROW = ("ka_0", "ka_1", "row_0", "row_1")
ROW = ("row_0", "row_1")
PLANE = ("ka_0", "ka_1", "row_1")
INTERPRET = False

broadening = 1.0
refine_step = (0.05, 0.03, 0.02)

f32 = jnp.float32
bf16 = jnp.bfloat16
VMEM = pl.BlockSpec(memory_space=pltpu.VMEM)
SMEM = pl.BlockSpec(memory_space=pltpu.SMEM)
NX = 4
OWNERS = 32
SECOND = 28
SPARE = 40
BLOCKS = 128


def params(mebibytes):
    return pltpu.CompilerParams(vmem_limit_bytes=mebibytes << 20)


ANY = pl.BlockSpec(memory_space=pl.ANY)
HBM = pl.BlockSpec(memory_space=pltpu.HBM)


def cost(microseconds):
    return pl.CostEstimate(flops=int(microseconds * 2.5e8), bytes_accessed=0, transcendentals=0)


def iota(shape, dim):
    return lax.broadcasted_iota(jnp.int32, shape, dim)


def place_of(position):
    plane = (position % 8) // 2
    owner = (position // 8) * 2 + position % 2
    return plane, owner


def index_kernel(place_ref, table_ref, points_ref, slots_ref, weight_ref):
    my_plane = place_ref[0]
    table = table_ref[...]
    turned = table.T
    square = (BLOCKS, BLOCKS)
    order_down = table[:, 4:5].astype(jnp.int32)
    order_along = turned[4:5, :].astype(jnp.int32)
    here_down = order_down == iota(square, 1)
    here_along = iota(square, 0) == order_along

    def along(column):
        return jnp.sum(jnp.where(here_along, table[:, column : column + 1], 0.0), axis=0, keepdims=True)

    base = [along(axis) for axis in range(3)]
    count = along(3)
    count_down = jnp.sum(jnp.where(here_down, turned[3:4, :], 0.0), axis=1, keepdims=True)

    plane_down, owner_down = place_of(iota(square, 0))
    plane_along, owner_along = place_of(iota(square, 1))
    mates = plane_down == plane_along
    ahead = mates & (owner_down < owner_along)
    plane_row, owner_row = place_of(iota((1, BLOCKS), 1))
    away = (plane_row - my_plane + NX) % NX
    seat = jnp.where(away == 1, 0, jnp.where(away == 3, 1, 2))

    def row_of(chunk, within):
        opposite = OWNERS * chunk + within
        apart = 3 * OWNERS * (1 + chunk) + seat * OWNERS + within
        spare = 12 * OWNERS + jnp.where(away == 2, 0, 1 + seat) * SPARE + within
        return jnp.where(chunk == 3, spare, jnp.where(away == 2, opposite, apart))

    rows = 12 * OWNERS + NX * SPARE
    entry = iota((rows, BLOCKS), 0)
    lane = iota((rows, BLOCKS), 1)
    gathered = [jnp.zeros((rows, BLOCKS), f32) for _ in range(3)]
    before = jnp.zeros((1, BLOCKS), f32)
    slots_ref[...] = jnp.zeros((8, BLOCKS), jnp.int32)
    weight_ref[...] = jnp.zeros((8, BLOCKS), f32)
    for s in range(SUB):
        fraction = (s + 0.5) / count - 0.5
        points = [base[axis] + fraction * refine_step[axis] for axis in range(3)]
        alive = count > s
        weight_ref[s : s + 1, :] = jnp.where(alive, 1.0 / count, 0.0)
        if s == 0:
            chunk, within = jnp.full((1, BLOCKS), 2, jnp.int32), owner_row
        else:
            live_down = count_down > s
            rank = before + jnp.sum(jnp.where(ahead & live_down, 1.0, 0.0), axis=0, keepdims=True)
            before = before + jnp.sum(jnp.where(mates & live_down, 1.0, 0.0), axis=0, keepdims=True)
            rank = jnp.where(alive, rank, 0.0).astype(jnp.int32)
            slots_ref[s : s + 1, :] = rank
            chunk = jnp.where(rank < OWNERS, 0, jnp.where(rank < OWNERS + SECOND, 1, 3))
            within = rank - jnp.where(chunk == 0, 0, jnp.where(chunk == 1, OWNERS, OWNERS + SECOND))
        match = entry == jnp.where(alive, row_of(chunk, within), -1)
        for axis in range(3):
            gathered[axis] = gathered[axis] + jnp.where(match, points[axis], 0.0)
    most = jnp.max(before, axis=1, keepdims=True)
    slots_ref[0:1, :] = jnp.broadcast_to(most, (1, BLOCKS)).astype(jnp.int32)
    points = jnp.zeros((rows, BLOCKS), f32)
    for axis in range(3):
        points = jnp.where(lane == axis, jnp.sum(gathered[axis], axis=1, keepdims=True), points)
    points_ref[...] = points


def find_points(table, plane):
    rows = 12 * OWNERS + NX * SPARE
    return pl.pallas_call(
        index_kernel,
        out_shape=(
            jax.ShapeDtypeStruct((rows, BLOCKS), f32),
            jax.ShapeDtypeStruct((8, BLOCKS), jnp.int32),
            jax.ShapeDtypeStruct((8, BLOCKS), f32),
        ),
        in_specs=[SMEM, VMEM],
        out_specs=(VMEM, VMEM, VMEM),
        compiler_params=params(8),
        cost_estimate=cost(2),
        interpret=INTERPRET,
        name="find_points",
    )(plane, table)


def pieces_of(depth):
    return [(matrix, slice(half * depth // 2, (half + 1) * depth // 2)) for matrix in range(3) for half in range(2)]


def coming_rows(core, space_ref, in_buffer, sems):
    _, depth, rows, _ = in_buffer.shape
    copies = []
    for k, (matrix, at) in enumerate(pieces_of(depth)):
        first = pl.multiple_of(rows * (2 * matrix + core), rows)
        copies.append(
            pltpu.make_async_copy(space_ref.at[at, pl.ds(first, rows), :], in_buffer.at[matrix, at], sems.at[k])
        )
    return copies


def turn_rows(in_buffer, wide_ref, matrix, at, store):
    _, _, rows, width = in_buffer.shape
    size = at.stop - at.start
    for first in range(0, size, 8):
        wide = in_buffer[matrix, at.start + first : at.start + first + 8].astype(f32)
        for r in range(8):
            wide_ref[(first + r) * rows : (first + r + 1) * rows, :] = wide[r]
    for part in range(2):
        for r in range(rows // 2):
            store(part, slice(r * width, (r + 1) * width), wide_ref[pl.ds(2 * r + part, size, stride=rows), :])


def send_kernel(core_ref, space_ref, out_ref, token_ref, in_buffer, out_buffer, wide_ref, in_sems, out_sems):
    token_ref[...] = jnp.zeros(token_ref.shape, f32)
    depth = in_buffer.shape[1]
    coming = coming_rows(core_ref[0], space_ref, in_buffer, in_sems)
    places = pieces_of(depth)
    going = [
        pltpu.make_async_copy(out_buffer.at[matrix, :, at], out_ref.at[matrix, :, at], out_sems.at[k])
        for k, (matrix, at) in enumerate(places)
    ]
    for copy in coming:
        copy.start()
    for k, (matrix, at) in enumerate(places):
        coming[k].wait()

        def store(part, lanes, value):
            out_buffer[matrix, part, at, lanes] = value

        turn_rows(in_buffer, wide_ref, matrix, at, store)
        going[k].start()
    for copy in going:
        copy.wait()


def send_rows(space, core):
    depth, rows, width = space.shape
    half = rows // 6
    shape = (3, 2, depth, half // 2 * width)
    return pl.pallas_call(
        send_kernel,
        out_shape=(jax.ShapeDtypeStruct(shape, f32), jax.ShapeDtypeStruct((8, BLOCKS), f32)),
        in_specs=[SMEM, HBM],
        out_specs=(HBM, VMEM),
        scratch_shapes=[
            pltpu.VMEM((3, depth, half, width), bf16),
            pltpu.VMEM(shape, f32),
            pltpu.VMEM((depth // 2 * half, width), f32),
            pltpu.SemaphoreType.DMA((6,)),
            pltpu.SemaphoreType.DMA((6,)),
        ],
        compiler_params=params(58),
        cost_estimate=cost(5),
        interpret=INTERPRET,
        name="send_rows",
    )(core, space)


def join_kernel(core_ref, space_ref, other_ref, out_ref, in_buffer, other_buffer, wide_ref, in_sems, other_sems):
    depth = in_buffer.shape[1]
    coming = coming_rows(core_ref[0], space_ref, in_buffer, in_sems)
    places = pieces_of(depth)
    others = [
        pltpu.make_async_copy(other_ref.at[matrix, :, at], other_buffer.at[matrix, :, at], other_sems.at[k])
        for k, (matrix, at) in enumerate(places)
    ]
    for k in range(6):
        coming[k].start()
        others[k].start()
    for k, (matrix, at) in enumerate(places):
        coming[k].wait()

        def store(part, lanes, value):
            rows = slice(part * depth + at.start, part * depth + at.stop)
            out_ref[matrix, rows, lanes] = value.astype(bf16)

        turn_rows(in_buffer, wide_ref, matrix, at, store)
        others[k].wait()
        for part in range(2):
            rows = slice((2 + part) * depth + at.start, (2 + part) * depth + at.stop)
            out_ref[matrix, rows, :] = other_buffer[matrix, part, at, :].astype(bf16)


def join_rows(space, core, other):
    depth, rows, width = space.shape
    half = rows // 6
    lanes = half // 2 * width
    return pl.pallas_call(
        join_kernel,
        out_shape=jax.ShapeDtypeStruct((3, 4 * depth, lanes), bf16),
        in_specs=[SMEM, HBM, HBM],
        out_specs=VMEM,
        scratch_shapes=[
            pltpu.VMEM((3, depth, half, width), bf16),
            pltpu.VMEM((3, 2, depth, lanes), f32),
            pltpu.VMEM((depth // 2 * half, width), f32),
            pltpu.SemaphoreType.DMA((6,)),
            pltpu.SemaphoreType.DMA((6,)),
        ],
        compiler_params=params(54),
        cost_estimate=cost(5),
        interpret=INTERPRET,
        name="join_rows",
    )(core, space, other)


def pack_kernel(row_ref, base_ref, counts_ref, order_ref, *refs):
    out_ref = refs[-1]
    row = row_ref[0]
    lane = iota((1, 1, BLOCKS), 2)
    value = jnp.zeros((1, 1, BLOCKS), f32)
    for axis in range(3):
        value = jnp.where(lane == axis, base_ref[row, axis], value)
    value = jnp.where(lane == 3, counts_ref[row].astype(f32), value)
    value = jnp.where(lane == 4, order_ref[0].astype(f32), value)
    out_ref[...] = jnp.broadcast_to(value, out_ref.shape)


def pack(row, base_k, counts, block_order, after):
    return pl.pallas_call(
        pack_kernel,
        out_shape=jax.ShapeDtypeStruct((BLOCKS, 1, BLOCKS), f32),
        in_specs=[SMEM] * 4 + [ANY] * len(after),
        out_specs=VMEM,
        compiler_params=params(4),
        cost_estimate=cost(1),
        interpret=INTERPRET,
        name="pack",
    )(row, base_k, counts, block_order, *after)


def turn(points, coords):
    turns = points[:, 0:1] * coords[0:1, :] + points[:, 1:2] * coords[1:2, :] + points[:, 2:3] * coords[2:3, :]
    rest = turns - jnp.floor(turns + 0.5)
    quarter = jnp.floor(4.0 * rest + 0.5)
    angle = (rest - 0.25 * quarter) * (2.0 * math.pi)
    square = angle * angle
    sine = angle * (1.0 + square * (-1.0 / 6 + square * (1.0 / 120 + square * (-1.0 / 5040 + square * (1.0 / 362880)))))
    cosine = 1.0 + square * (-0.5 + square * (1.0 / 24 + square * (-1.0 / 720 + square * (1.0 / 40320 - square / 3628800))))
    odd = jnp.abs(quarter) == 1.0
    first = jnp.where(odd, sine, cosine)
    second = jnp.where(odd, cosine, sine)
    cos_sign = jnp.where((quarter == 1.0) | (jnp.abs(quarter) == 2.0), -1.0, 1.0)
    sin_sign = jnp.where((quarter == -1.0) | (jnp.abs(quarter) == 2.0), -1.0, 1.0)
    return first * cos_sign, second * sin_sign


def store_phases(low, count, points_ref, coords_ref, phase_ref):
    depth = coords_ref.shape[1] // 2
    tile = 16

    def rows_of(i, carry):
        first = pl.multiple_of(i * tile, tile)
        points = points_ref[pl.ds(low + first, tile), :]
        for source in range(2):
            coords = coords_ref[:, source * depth : (source + 1) * depth]
            cosine, sine = turn(points, coords)
            at_real = slice(source * 2 * depth, source * 2 * depth + depth)
            at_imag = slice(source * 2 * depth + depth, source * 2 * depth + 2 * depth)
            pairs = [(cosine, sine)]
            for axis in range(2):
                coord = coords[axis : axis + 1, :]
                pairs.append((-coord * sine, coord * cosine))
            for kind, (real, imag) in enumerate(pairs):
                real_rows = pl.ds(2 * kind * count + first, tile)
                imag_rows = pl.ds((2 * kind + 1) * count + first, tile)
                phase_ref[real_rows, at_real] = real.astype(bf16)
                phase_ref[real_rows, at_imag] = (-imag).astype(bf16)
                phase_ref[imag_rows, at_real] = imag.astype(bf16)
                phase_ref[imag_rows, at_imag] = real.astype(bf16)
        return carry

    lax.fori_loop(0, count // tile, rows_of, 0)


def store_sums(phase_ref, matrices, count, kinds, first_kind, first_row, out_refs, pitches):
    product = jnp.dot(phase_ref[: kinds * count, :], matrices, preferred_element_type=f32)
    width = product.shape[1] // 2
    for kind in range(kinds):
        for half in range(2):
            block = product[kind * count : (kind + 1) * count, half * width : (half + 1) * width]
            at = (first_kind + kind) * 4 + first_row + half
            start = 0
            for ref, pitch in zip(out_refs, pitches):
                size = ref.shape[0] // 40
                ref[pl.ds(at, size, stride=40), :] = block[start : start + size]
                start += pitch


PLACES = tuple((matrix, part) for matrix in range(3) for part in range(2))


def fourier_kernel(low, pitches, waits, streamed, points_ref, coords_ref, matrices_ref, *refs):
    refs = refs[waits:]
    outs = len(pitches)
    out_refs, token_ref, phase_ref = refs[:outs], refs[outs], refs[outs + 1]
    token_ref[...] = jnp.zeros(token_ref.shape, f32)
    count = sum(pitches)
    lanes = matrices_ref.shape[2] // 2
    copies = []
    if streamed:
        buffer_ref, sems = refs[outs + 2 :]
        for k, (matrix, part) in enumerate(PLACES):
            source = matrices_ref.at[matrix, :, pl.ds(part * lanes, lanes)]
            copies.append(pltpu.make_async_copy(source, buffer_ref.at[k], sems.at[k]))
        for copy in copies:
            copy.start()
    store_phases(low, count, points_ref, coords_ref, phase_ref)
    for k, (matrix, part) in enumerate(PLACES):
        kinds, first_kind = (6, 0) if matrix == 0 else (2, 4 + 2 * matrix)
        if streamed:
            copies[k].wait()
            block = buffer_ref[k]
        else:
            block = matrices_ref[matrix, :, part * lanes : (part + 1) * lanes]
        store_sums(phase_ref, block, count, kinds, first_kind, 2 * part, out_refs, pitches)


def fourier(points, low, sizes, pitches, coords, matrices, microseconds, after=(), streamed=False):
    depth4 = matrices.shape[1]
    width = matrices.shape[2] // 4
    shapes = tuple(jax.ShapeDtypeStruct((size * 40, width), f32) for size in sizes)
    scratch = [pltpu.VMEM((6 * sum(pitches), depth4), bf16)]
    if streamed:
        scratch += [pltpu.VMEM((6, depth4, 2 * width), bf16), pltpu.SemaphoreType.DMA((6,))]
    outs = pl.pallas_call(
        lambda *refs: fourier_kernel(low, pitches, len(after), streamed, *refs),
        out_shape=shapes + (jax.ShapeDtypeStruct((8, BLOCKS), f32),),
        in_specs=[VMEM, VMEM, HBM if streamed else VMEM] + [ANY] * len(after),
        out_specs=(VMEM,) * (len(shapes) + 1),
        scratch_shapes=scratch,
        compiler_params=params(18),
        cost_estimate=cost(microseconds),
        interpret=INTERPRET,
        name="fourier",
    )(points, coords, matrices, *after)
    return tuple(out.reshape(-1, 40, width) for out in outs[:-1]) + (outs[-1],)


def to_right(value):
    return lax.ppermute(value, "row_0", [(i, (i + 1) % NX) for i in range(NX)])


def to_left(value):
    return lax.ppermute(value, "row_0", [(i, (i - 1) % NX) for i in range(NX)])


def first_hop(near, far):
    near = to_right(near)
    far = to_left(far)
    return near, far


def add_kernel(waits, near_ref, far_ref, right_ref, left_ref, *refs):
    right_out, left_out, token_ref = refs[waits:]
    half = near_ref.shape[0]
    right_out[:half] = right_ref[:half] + near_ref[...]
    right_out[half:] = right_ref[half:]
    left_out[:half] = left_ref[:half]
    left_out[half:] = left_ref[half:] + far_ref[...]
    token_ref[...] = jnp.zeros(token_ref.shape, f32)


def add_arrived(near, far, right, left, after=()):
    shape = jax.ShapeDtypeStruct(right.shape, f32)
    return pl.pallas_call(
        lambda *refs: add_kernel(len(after), *refs),
        out_shape=(shape, shape, jax.ShapeDtypeStruct((8, BLOCKS), f32)),
        in_specs=[VMEM] * 4 + [ANY] * len(after),
        out_specs=(VMEM,) * 3,
        input_output_aliases={2: 0, 3: 1},
        compiler_params=params(6),
        cost_estimate=cost(1.5),
        interpret=INTERPRET,
        name="add_arrived",
    )(near, far, right, left, *after)


def second_hop(right, left):
    right = to_right(right)
    left = to_left(left)
    return right, left


def place_kernel(place_ref, slots_ref, *refs):
    keep0, right0, left0, keep1, right1, left1, extra = refs[:7]
    out_ref, token_ref, table_ref = refs[-3:]
    token_ref[...] = jnp.zeros(token_ref.shape, f32)
    plane = place_ref[0]
    first, second = keep0.shape[0], keep0.shape[0] + keep1.shape[0]
    table_ref[:first] = keep0[...] + right0[...] + left0[...]
    table_ref[first:second] = keep1[...] + right1[...] + left1[...]
    table_ref[second:] = extra[...]

    def body(owner, carry):
        position = (owner // 2) * 8 + 2 * plane + owner % 2
        for s in range(1, SUB):
            out_ref[owner, s - 1] = table_ref[slots_ref[s, position]]
        return carry

    lax.fori_loop(0, OWNERS, body, 0)


def place_slots(plane, slots, parts0, parts1, extra, after):
    _, rows, width = extra.shape
    size = OWNERS + SECOND + SPARE
    return pl.pallas_call(
        place_kernel,
        out_shape=(
            jax.ShapeDtypeStruct((OWNERS, SUB - 1, rows, width), f32),
            jax.ShapeDtypeStruct((8, BLOCKS), f32),
        ),
        in_specs=[SMEM, SMEM] + [VMEM] * 7 + [ANY] * len(after),
        out_specs=(VMEM, VMEM),
        scratch_shapes=[pltpu.VMEM((size, rows, width), f32)],
        compiler_params=params(12),
        cost_estimate=cost(4),
        interpret=INTERPRET,
        name="place_slots",
    )(plane, slots, *parts0, *parts1, extra, *after)


def total_kernel(keep_ref, right_ref, left_ref, out_ref):
    out_ref[...] = keep_ref[...] + right_ref[...] + left_ref[...]


def total(keep, right, left):
    return pl.pallas_call(
        total_kernel,
        out_shape=jax.ShapeDtypeStruct(keep.shape, f32),
        in_specs=[VMEM] * 3,
        out_specs=VMEM,
        compiler_params=params(8),
        cost_estimate=cost(1.5),
        interpret=INTERPRET,
        name="total",
    )(keep, right, left)


def to_owners(value):
    return lax.all_to_all(value, PLANE, split_axis=0, concat_axis=0, tiled=True)


def two_terms(value):
    high = value.astype(bf16)
    return high, (value - high.astype(f32)).astype(bf16)


def curvature_kernel(first, units, adding, weight_ref, field_ref, turn_ref, back_ref, occupied_ref, *refs):
    out_ref = refs[-1]
    previous = refs[0][...] if adding else 0.0
    unit = pl.program_id(0)
    sources = field_ref.shape[0] // (units * 40)
    n = field_ref.shape[1]
    stride = units * 40

    def plane_of(kind):
        return jnp.concatenate(
            [field_ref[pl.ds(unit * 40 + kind * 4 + r, sources, stride=stride), :] for r in range(4)], axis=0
        )

    matrices = jnp.concatenate(
        [jnp.concatenate([plane_of(2 * c), plane_of(2 * c + 1)], axis=1) for c in range(5)], axis=0
    )
    high, low = two_terms(matrices)
    vectors = turn_ref[0]
    rotated = jnp.dot(high, vectors, preferred_element_type=f32) + jnp.dot(low, vectors, preferred_element_type=f32)
    stacked = jnp.concatenate(
        [
            jnp.concatenate([rotated[c * n : (c + 1) * n, :n] for c in range(5)], axis=1),
            jnp.concatenate([rotated[c * n : (c + 1) * n, n:] for c in range(5)], axis=1),
        ],
        axis=0,
    )
    back = back_ref[0]
    high, low = two_terms(stacked)
    bar = jnp.dot(back, high, preferred_element_type=f32) + jnp.dot(back, low, preferred_element_type=f32)
    bar_real, bar_imag = bar[:n], bar[n:]
    diagonal = jnp.where(iota((n, n), 0) == iota((n, n), 1), bar_real[:, :n], 0.0)
    spacing = jnp.sum(diagonal, axis=0, keepdims=True) - jnp.sum(diagonal, axis=1, keepdims=True)
    smoothed = spacing / (spacing * spacing + broadening)

    def pick(value, c):
        return value[:, (c + 1) * n : (c + 2) * n]

    xcov_real = pick(bar_real, 2) + smoothed * pick(bar_real, 0)
    xcov_imag = pick(bar_imag, 2) + smoothed * pick(bar_imag, 0)
    ycov_real = pick(bar_real, 3) + smoothed * pick(bar_real, 1)
    ycov_imag = pick(bar_imag, 3) + smoothed * pick(bar_imag, 1)
    s = first + unit
    filled = occupied_ref[pl.ds(s, 1), :].astype(f32)
    filled_down = jnp.broadcast_to(filled, (n, n)).T
    pairing = filled_down * (1.0 - filled)
    product = pairing * (xcov_real * ycov_imag.T + xcov_imag * ycov_real.T)
    berry = jnp.sum(jnp.sum(product, axis=0, keepdims=True), axis=1, keepdims=True) * (-2.0 / n)
    weight = weight_ref[s]
    lane = iota((1, SUB), 1)
    result = jnp.where((lane == s) & (weight > 0.0), weight * berry, 0.0)
    before = jnp.where(unit == 0, previous, out_ref[...])
    out_ref[...] = result + before


def curvature(first, units, weight, arrived, vectors, adjoint, occupied, previous=(), after=()):
    width = arrived.shape[-1]
    flat = arrived.reshape(-1, width)
    matrix = pl.BlockSpec((1, 2 * width, 2 * width), lambda u: (first + u, 0, 0))
    return pl.pallas_call(
        lambda *refs: curvature_kernel(first, units, len(previous), *refs),
        grid=(units,),
        out_shape=jax.ShapeDtypeStruct((1, SUB), f32),
        in_specs=[
            SMEM,
            pl.BlockSpec(flat.shape, lambda u: (0, 0)),
            matrix,
            matrix,
            pl.BlockSpec(occupied.shape, lambda u: (0, 0)),
        ]
        + [pl.BlockSpec((1, SUB), lambda u: (0, 0))] * len(previous)
        + [ANY] * len(after),
        out_specs=pl.BlockSpec((1, SUB), lambda u: (0, 0)),
        compiler_params=params(58),
        cost_estimate=cost(2.5 * units),
        interpret=INTERPRET,
        name="curvature",
    )(weight, flat, vectors, adjoint, occupied, *previous, *after)


def vector_kernel(eigvecs_ref, *refs):
    turn_ref, back_ref, wide_ref = refs[-3:]
    n = eigvecs_ref.shape[2]
    wide_ref[...] = eigvecs_ref[0].astype(f32)
    real, imag = (wide_ref[pl.ds(part, n, stride=2), :].astype(bf16) for part in range(2))
    turn_ref[0, :n, :n] = real
    turn_ref[0, :n, n:] = imag
    turn_ref[0, n:, :n] = -imag
    turn_ref[0, n:, n:] = real
    group = n // OWNERS
    for part in range(2):
        packed = jnp.concatenate(
            [wide_ref[pl.ds(2 * r + part, OWNERS, stride=2 * group), :] for r in range(group)], axis=0
        )
        turned = packed.T
        if part == 0:
            back_ref[0, :n, :n] = turned.astype(bf16)
            back_ref[0, n:, n:] = turned.astype(bf16)
        else:
            back_ref[0, :n, n:] = turned.astype(bf16)
            back_ref[0, n:, :n] = (-turned).astype(bf16)


def vector_matrices(eigvecs, after):
    slots, width = eigvecs.shape[0], eigvecs.shape[1]
    shape = jax.ShapeDtypeStruct((slots, 2 * width, 2 * width), bf16)
    square = pl.BlockSpec((1, 2 * width, 2 * width), lambda i: (i, 0, 0))
    return pl.pallas_call(
        vector_kernel,
        grid=(slots,),
        out_shape=(shape, shape),
        in_specs=[pl.BlockSpec((1, 2 * width, width), lambda i: (i, 0, 0))] + [ANY] * len(after),
        out_specs=(square, square),
        scratch_shapes=[pltpu.VMEM((2 * width, width), f32)],
        compiler_params=params(4),
        cost_estimate=cost(2),
        interpret=INTERPRET,
        name="vector_matrices",
    )(eigvecs.reshape(slots, 2 * width, width), *after)


def body(base_k, counts, block_order, lattice, real_space, eigvecs, occupied):
    plane, core = lax.axis_index("row_0"), lax.axis_index("row_1")
    row = plane * 2 + core
    plane_ref = plane.reshape(1).astype(jnp.int32)
    core_ref = core.reshape(1).astype(jnp.int32)
    depth, _, slab, _, width = real_space.shape

    space = real_space.reshape(depth, 6 * slab, width)
    swap = [(0, 1), (1, 0)]
    send, token = send_rows(space, 1 - core_ref)
    mine = pack(row.reshape(1).astype(jnp.int32), base_k, counts, block_order, (token,))
    other = lax.ppermute(send, "row_1", swap)
    own_coords = jnp.pad(lattice.T.astype(f32), ((0, 5), (0, 0)))
    coords = jnp.concatenate([own_coords, lax.ppermute(own_coords, "row_1", swap)], axis=1)

    table = lax.all_to_all(mine, KA_ROW, 0, 0, tiled=True)
    table = table.reshape(BLOCKS, BLOCKS)
    matrices = join_rows(space, core_ref, other)
    points, slots, weights = find_points(table, plane_ref)
    position = (lax.axis_index(KA) * 8 + row).astype(jnp.int32)
    weight = lax.dynamic_slice(weights, (jnp.int32(0), position), (SUB, 1)).reshape(SUB)

    half = OWNERS // 2

    def sums(low, sizes, pitches, microseconds, after=(), streamed=False):
        return fourier(points, low, sizes, pitches, coords, matrices, microseconds, after, streamed)

    def rest(chunk, size, after):
        return sums(3 * OWNERS * (1 + chunk), (size,) * 3, (OWNERS,) * 3, 5, after)

    near0, far0, token = sums(0, (half, half), (half, half), 4, (), True)
    hop0 = first_hop(near0, far0)
    near1, far1, near3, far3, token = sums(
        OWNERS, (half, SECOND - half, half, half), (half,) * 4, 4, (token,)
    )
    hop1 = first_hop(near1, far1)
    right0, left0, keep0, token = rest(0, OWNERS, (token,))
    right0, left0, token = add_arrived(*hop0, right0, left0)
    ring0 = second_hop(right0, left0)
    right1, left1, keep1, token = rest(1, SECOND, (token,))
    right1, left1, token = add_arrived(*hop1, right1, left1)
    ring1 = second_hop(right1, left1)
    hop3 = first_hop(near3, far3)
    right3, left3, keep3, token = rest(2, OWNERS, (token,))

    def further(_):
        parts = (24, 16, SPARE, SPARE, SPARE)
        near, far, right, left, keep, _ = sums(12 * OWNERS, parts, parts, 8)
        right, left, _ = add_arrived(*first_hop(near, far), right, left)
        right, left = second_hop(right, left)
        return keep + right + left

    empty = (SPARE,) + keep0.shape[1:]
    extra = lax.cond(slots[0, 0] > OWNERS + SECOND, further, lambda _: jnp.zeros(empty, f32), 0)

    placed, token = place_slots(plane_ref, slots, (keep0, *ring0), (keep1, *ring1), extra, (token,))
    unit123 = to_owners(placed)
    right3, left3, token = add_arrived(*hop3, right3, left3, (token,))
    ring3 = second_hop(right3, left3)
    turning, back = vector_matrices(eigvecs, (token,))
    unit0 = to_owners(total(keep3, *ring3))
    curve = curvature(1, 3, weight, unit123, turning, back, occupied)
    return curvature(0, 1, weight, unit0, turning, back, occupied, (curve,)).reshape(SUB)


def solution(mesh):
    finer = Mesh(mesh.devices.reshape(4, 4, 4, 2), ("ka_0", "ka_1", "row_0", "row_1"))
    placed = (
        P(KA, None),
        P(KA),
        P(KA_ROW),
        P(ROW, None),
        P(ROW, None, KA, None, None),
        P(KA_ROW, None, None, None),
        P(KA_ROW, None),
    )
    return jax.shard_map(body, mesh=finer, in_specs=placed, out_specs=P(KA_ROW), check_vma=False)
```

```python
import math

import jax
import jax.numpy as jnp
from jax import lax
from jax.experimental import pallas as pl
from jax.experimental.pallas import tpu as pltpu
from jax.sharding import Mesh
from jax.sharding import PartitionSpec as P

SUB = 4
KA = ("ka_0", "ka_1")
KA_ROW = ("ka_0", "ka_1", "row_0", "row_1")
ROW = ("row_0", "row_1")
PLANE = ("ka_0", "ka_1", "row_1")
INTERPRET = False

broadening = 1.0
refine_step = (0.05, 0.03, 0.02)

f32 = jnp.float32
bf16 = jnp.bfloat16
VMEM = pl.BlockSpec(memory_space=pltpu.VMEM)
SMEM = pl.BlockSpec(memory_space=pltpu.SMEM)
NX = 4
OWNERS = 32
SECOND = 32
SPARE = 32
BLOCKS = 128


def params(mebibytes):
    return pltpu.CompilerParams(vmem_limit_bytes=mebibytes << 20)


ANY = pl.BlockSpec(memory_space=pl.ANY)
HBM = pl.BlockSpec(memory_space=pltpu.HBM)


def cost(microseconds):
    return pl.CostEstimate(flops=int(microseconds * 2.5e8), bytes_accessed=0, transcendentals=0)


def iota(shape, dim):
    return lax.broadcasted_iota(jnp.int32, shape, dim)


def place_of(position):
    plane = (position % 8) // 2
    owner = (position // 8) * 2 + position % 2
    return plane, owner


def index_kernel(place_ref, table_ref, points_ref, slots_ref, weight_ref):
    my_plane = place_ref[0]
    table = table_ref[...]
    turned = table.T
    square = (BLOCKS, BLOCKS)
    order_down = table[:, 4:5].astype(jnp.int32)
    order_along = turned[4:5, :].astype(jnp.int32)
    here_down = order_down == iota(square, 1)
    here_along = iota(square, 0) == order_along

    def along(column):
        return jnp.sum(jnp.where(here_along, table[:, column : column + 1], 0.0), axis=0, keepdims=True)

    base = [along(axis) for axis in range(3)]
    count = along(3)
    count_down = jnp.sum(jnp.where(here_down, turned[3:4, :], 0.0), axis=1, keepdims=True)

    plane_down, owner_down = place_of(iota(square, 0))
    plane_along, owner_along = place_of(iota(square, 1))
    mates = plane_down == plane_along
    ahead = mates & (owner_down < owner_along)
    plane_row, owner_row = place_of(iota((1, BLOCKS), 1))
    away = (plane_row - my_plane + NX) % NX
    seat = jnp.where(away == 1, 0, jnp.where(away == 3, 1, 2))

    def row_of(chunk, within):
        opposite = OWNERS * chunk + within
        apart = 3 * OWNERS * (1 + chunk) + seat * OWNERS + within
        spare = 12 * OWNERS + jnp.where(away == 2, 0, 1 + seat) * SPARE + within
        return jnp.where(chunk == 3, spare, jnp.where(away == 2, opposite, apart))

    rows = 12 * OWNERS + NX * SPARE
    entry = iota((rows, BLOCKS), 0)
    lane = iota((rows, BLOCKS), 1)
    gathered = [jnp.zeros((rows, BLOCKS), f32) for _ in range(3)]
    before = jnp.zeros((1, BLOCKS), f32)
    slots_ref[...] = jnp.zeros((8, BLOCKS), jnp.int32)
    weight_ref[...] = jnp.zeros((8, BLOCKS), f32)
    for s in range(SUB):
        fraction = (s + 0.5) / count - 0.5
        points = [base[axis] + fraction * refine_step[axis] for axis in range(3)]
        alive = count > s
        weight_ref[s : s + 1, :] = jnp.where(alive, 1.0 / count, 0.0)
        if s == 0:
            chunk, within = jnp.full((1, BLOCKS), 2, jnp.int32), owner_row
        else:
            live_down = count_down > s
            rank = before + jnp.sum(jnp.where(ahead & live_down, 1.0, 0.0), axis=0, keepdims=True)
            before = before + jnp.sum(jnp.where(mates & live_down, 1.0, 0.0), axis=0, keepdims=True)
            rank = jnp.where(alive, rank, 0.0).astype(jnp.int32)
            slots_ref[s : s + 1, :] = rank
            chunk = jnp.where(rank < OWNERS, 0, jnp.where(rank < OWNERS + SECOND, 1, 3))
            within = rank - jnp.where(chunk == 0, 0, jnp.where(chunk == 1, OWNERS, OWNERS + SECOND))
        match = entry == jnp.where(alive, row_of(chunk, within), -1)
        for axis in range(3):
            gathered[axis] = gathered[axis] + jnp.where(match, points[axis], 0.0)
    most = jnp.max(before, axis=1, keepdims=True)
    slots_ref[0:1, :] = jnp.broadcast_to(most, (1, BLOCKS)).astype(jnp.int32)
    points = jnp.zeros((rows, BLOCKS), f32)
    for axis in range(3):
        points = jnp.where(lane == axis, jnp.sum(gathered[axis], axis=1, keepdims=True), points)
    points_ref[...] = points


def find_points(table, plane):
    rows = 12 * OWNERS + NX * SPARE
    return pl.pallas_call(
        index_kernel,
        out_shape=(
            jax.ShapeDtypeStruct((rows, BLOCKS), f32),
            jax.ShapeDtypeStruct((8, BLOCKS), jnp.int32),
            jax.ShapeDtypeStruct((8, BLOCKS), f32),
        ),
        in_specs=[SMEM, VMEM],
        out_specs=(VMEM, VMEM, VMEM),
        compiler_params=params(8),
        cost_estimate=cost(2),
        interpret=INTERPRET,
        name="find_points",
    )(plane, table)


def pieces_of(depth):
    return [(matrix, slice(half * depth // 2, (half + 1) * depth // 2)) for matrix in range(3) for half in range(2)]


def coming_rows(core, space_ref, in_buffer, sems):
    _, depth, rows, _ = in_buffer.shape
    copies = []
    for k, (matrix, at) in enumerate(pieces_of(depth)):
        first = pl.multiple_of(rows * (2 * matrix + core), rows)
        copies.append(
            pltpu.make_async_copy(space_ref.at[at, pl.ds(first, rows), :], in_buffer.at[matrix, at], sems.at[k])
        )
    return copies


def turn_rows(in_buffer, wide_ref, matrix, at, store):
    _, _, rows, width = in_buffer.shape
    size = at.stop - at.start
    for first in range(0, size, 8):
        wide = in_buffer[matrix, at.start + first : at.start + first + 8].astype(f32)
        for r in range(8):
            wide_ref[(first + r) * rows : (first + r + 1) * rows, :] = wide[r]
    for part in range(2):
        for r in range(rows // 2):
            store(part, slice(r * width, (r + 1) * width), wide_ref[pl.ds(2 * r + part, size, stride=rows), :])


def send_kernel(core_ref, space_ref, out_ref, token_ref, in_buffer, out_buffer, wide_ref, in_sems, out_sems):
    token_ref[...] = jnp.zeros(token_ref.shape, f32)
    depth = in_buffer.shape[1]
    coming = coming_rows(core_ref[0], space_ref, in_buffer, in_sems)
    places = pieces_of(depth)
    going = [
        pltpu.make_async_copy(out_buffer.at[matrix, :, at], out_ref.at[matrix, :, at], out_sems.at[k])
        for k, (matrix, at) in enumerate(places)
    ]
    for copy in coming:
        copy.start()
    for k, (matrix, at) in enumerate(places):
        coming[k].wait()

        def store(part, lanes, value):
            out_buffer[matrix, part, at, lanes] = value

        turn_rows(in_buffer, wide_ref, matrix, at, store)
        going[k].start()
    for copy in going:
        copy.wait()


def send_rows(space, core):
    depth, rows, width = space.shape
    half = rows // 6
    shape = (3, 2, depth, half // 2 * width)
    return pl.pallas_call(
        send_kernel,
        out_shape=(jax.ShapeDtypeStruct(shape, f32), jax.ShapeDtypeStruct((8, BLOCKS), f32)),
        in_specs=[SMEM, HBM],
        out_specs=(HBM, VMEM),
        scratch_shapes=[
            pltpu.VMEM((3, depth, half, width), bf16),
            pltpu.VMEM(shape, f32),
            pltpu.VMEM((depth // 2 * half, width), f32),
            pltpu.SemaphoreType.DMA((6,)),
            pltpu.SemaphoreType.DMA((6,)),
        ],
        compiler_params=params(58),
        cost_estimate=cost(5),
        interpret=INTERPRET,
        name="send_rows",
    )(core, space)


def join_kernel(core_ref, space_ref, other_ref, out_ref, in_buffer, other_buffer, wide_ref, in_sems, other_sems):
    depth = in_buffer.shape[1]
    coming = coming_rows(core_ref[0], space_ref, in_buffer, in_sems)
    places = pieces_of(depth)
    others = [
        pltpu.make_async_copy(other_ref.at[matrix, :, at], other_buffer.at[matrix, :, at], other_sems.at[k])
        for k, (matrix, at) in enumerate(places)
    ]
    for k in range(6):
        coming[k].start()
        others[k].start()
    for k, (matrix, at) in enumerate(places):
        coming[k].wait()

        def store(part, lanes, value):
            rows = slice(part * depth + at.start, part * depth + at.stop)
            out_ref[matrix, rows, lanes] = value.astype(bf16)

        turn_rows(in_buffer, wide_ref, matrix, at, store)
        others[k].wait()
        for part in range(2):
            rows = slice((2 + part) * depth + at.start, (2 + part) * depth + at.stop)
            out_ref[matrix, rows, :] = other_buffer[matrix, part, at, :].astype(bf16)


def join_rows(space, core, other):
    depth, rows, width = space.shape
    half = rows // 6
    lanes = half // 2 * width
    return pl.pallas_call(
        join_kernel,
        out_shape=jax.ShapeDtypeStruct((3, 4 * depth, lanes), bf16),
        in_specs=[SMEM, HBM, HBM],
        out_specs=VMEM,
        scratch_shapes=[
            pltpu.VMEM((3, depth, half, width), bf16),
            pltpu.VMEM((3, 2, depth, lanes), f32),
            pltpu.VMEM((depth // 2 * half, width), f32),
            pltpu.SemaphoreType.DMA((6,)),
            pltpu.SemaphoreType.DMA((6,)),
        ],
        compiler_params=params(54),
        cost_estimate=cost(5),
        interpret=INTERPRET,
        name="join_rows",
    )(core, space, other)


def pack_kernel(row_ref, base_ref, counts_ref, order_ref, *refs):
    out_ref = refs[-1]
    row = row_ref[0]
    lane = iota((1, 1, BLOCKS), 2)
    value = jnp.zeros((1, 1, BLOCKS), f32)
    for axis in range(3):
        value = jnp.where(lane == axis, base_ref[row, axis], value)
    value = jnp.where(lane == 3, counts_ref[row].astype(f32), value)
    value = jnp.where(lane == 4, order_ref[0].astype(f32), value)
    out_ref[...] = jnp.broadcast_to(value, out_ref.shape)


def pack(row, base_k, counts, block_order, after):
    return pl.pallas_call(
        pack_kernel,
        out_shape=jax.ShapeDtypeStruct((BLOCKS, 1, BLOCKS), f32),
        in_specs=[SMEM] * 4 + [ANY] * len(after),
        out_specs=VMEM,
        compiler_params=params(4),
        cost_estimate=cost(1),
        interpret=INTERPRET,
        name="pack",
    )(row, base_k, counts, block_order, *after)


def turn(points, coords):
    turns = points[:, 0:1] * coords[0:1, :] + points[:, 1:2] * coords[1:2, :] + points[:, 2:3] * coords[2:3, :]
    rest = turns - jnp.floor(turns + 0.5)
    quarter = jnp.floor(4.0 * rest + 0.5)
    angle = (rest - 0.25 * quarter) * (2.0 * math.pi)
    square = angle * angle
    sine = angle * (1.0 + square * (-1.0 / 6 + square * (1.0 / 120 + square * (-1.0 / 5040 + square * (1.0 / 362880)))))
    cosine = 1.0 + square * (-0.5 + square * (1.0 / 24 + square * (-1.0 / 720 + square * (1.0 / 40320 - square / 3628800))))
    odd = jnp.abs(quarter) == 1.0
    first = jnp.where(odd, sine, cosine)
    second = jnp.where(odd, cosine, sine)
    cos_sign = jnp.where((quarter == 1.0) | (jnp.abs(quarter) == 2.0), -1.0, 1.0)
    sin_sign = jnp.where((quarter == -1.0) | (jnp.abs(quarter) == 2.0), -1.0, 1.0)
    return first * cos_sign, second * sin_sign


def store_phases(low, count, points_ref, coords_ref, phase_ref):
    depth = coords_ref.shape[1] // 2
    tile = 16

    def rows_of(i, carry):
        first = pl.multiple_of(i * tile, tile)
        points = points_ref[pl.ds(low + first, tile), :]
        for source in range(2):
            coords = coords_ref[:, source * depth : (source + 1) * depth]
            cosine, sine = turn(points, coords)
            at_real = slice(source * 2 * depth, source * 2 * depth + depth)
            at_imag = slice(source * 2 * depth + depth, source * 2 * depth + 2 * depth)
            pairs = [(cosine, sine)]
            for axis in range(2):
                coord = coords[axis : axis + 1, :]
                pairs.append((-coord * sine, coord * cosine))
            for kind, (real, imag) in enumerate(pairs):
                real_rows = pl.ds(2 * kind * count + first, tile)
                imag_rows = pl.ds((2 * kind + 1) * count + first, tile)
                phase_ref[real_rows, at_real] = real.astype(bf16)
                phase_ref[real_rows, at_imag] = (-imag).astype(bf16)
                phase_ref[imag_rows, at_real] = imag.astype(bf16)
                phase_ref[imag_rows, at_imag] = real.astype(bf16)
        return carry

    lax.fori_loop(0, count // tile, rows_of, 0)


def store_sums(phase_ref, matrices, count, kinds, first_kind, first_row, out_refs, pitches):
    product = jnp.dot(phase_ref[: kinds * count, :], matrices, preferred_element_type=f32)
    width = product.shape[1] // 2
    for kind in range(kinds):
        for half in range(2):
            block = product[kind * count : (kind + 1) * count, half * width : (half + 1) * width]
            at = (first_kind + kind) * 4 + first_row + half
            start = 0
            for ref, pitch in zip(out_refs, pitches):
                size = ref.shape[0] // 40
                ref[pl.ds(at, size, stride=40), :] = block[start : start + size]
                start += pitch


PLACES = tuple((matrix, part) for matrix in range(3) for part in range(2))


def fourier_kernel(low, pitches, waits, streamed, points_ref, coords_ref, matrices_ref, *refs):
    refs = refs[waits:]
    outs = len(pitches)
    out_refs, token_ref, phase_ref = refs[:outs], refs[outs], refs[outs + 1]
    token_ref[...] = jnp.zeros(token_ref.shape, f32)
    count = sum(pitches)
    lanes = matrices_ref.shape[2] // 2
    copies = []
    if streamed:
        buffer_ref, sems = refs[outs + 2 :]
        for k, (matrix, part) in enumerate(PLACES):
            source = matrices_ref.at[matrix, :, pl.ds(part * lanes, lanes)]
            copies.append(pltpu.make_async_copy(source, buffer_ref.at[k], sems.at[k]))
        for copy in copies:
            copy.start()
    store_phases(low, count, points_ref, coords_ref, phase_ref)
    for k, (matrix, part) in enumerate(PLACES):
        kinds, first_kind = (6, 0) if matrix == 0 else (2, 4 + 2 * matrix)
        if streamed:
            copies[k].wait()
            block = buffer_ref[k]
        else:
            block = matrices_ref[matrix, :, part * lanes : (part + 1) * lanes]
        store_sums(phase_ref, block, count, kinds, first_kind, 2 * part, out_refs, pitches)


def fourier(points, low, sizes, pitches, coords, matrices, microseconds, after=(), streamed=False):
    depth4 = matrices.shape[1]
    width = matrices.shape[2] // 4
    shapes = tuple(jax.ShapeDtypeStruct((size * 40, width), f32) for size in sizes)
    scratch = [pltpu.VMEM((6 * sum(pitches), depth4), bf16)]
    if streamed:
        scratch += [pltpu.VMEM((6, depth4, 2 * width), bf16), pltpu.SemaphoreType.DMA((6,))]
    outs = pl.pallas_call(
        lambda *refs: fourier_kernel(low, pitches, len(after), streamed, *refs),
        out_shape=shapes + (jax.ShapeDtypeStruct((8, BLOCKS), f32),),
        in_specs=[VMEM, VMEM, HBM if streamed else VMEM] + [ANY] * len(after),
        out_specs=(VMEM,) * (len(shapes) + 1),
        scratch_shapes=scratch,
        compiler_params=params(18),
        cost_estimate=cost(microseconds),
        interpret=INTERPRET,
        name="fourier",
    )(points, coords, matrices, *after)
    return tuple(out.reshape(-1, 40, width) for out in outs[:-1]) + (outs[-1],)


def to_right(value):
    return lax.ppermute(value, "row_0", [(i, (i + 1) % NX) for i in range(NX)])


def to_left(value):
    return lax.ppermute(value, "row_0", [(i, (i - 1) % NX) for i in range(NX)])


def first_hop(near, far):
    near = to_right(near)
    far = to_left(far)
    return near, far


def add_kernel(waits, near_ref, far_ref, right_ref, left_ref, *refs):
    right_out, left_out, token_ref = refs[waits:]
    half = near_ref.shape[0]
    right_out[:half] = right_ref[:half] + near_ref[...]
    right_out[half:] = right_ref[half:]
    left_out[:half] = left_ref[:half]
    left_out[half:] = left_ref[half:] + far_ref[...]
    token_ref[...] = jnp.zeros(token_ref.shape, f32)


def add_arrived(near, far, right, left, after=()):
    shape = jax.ShapeDtypeStruct(right.shape, f32)
    return pl.pallas_call(
        lambda *refs: add_kernel(len(after), *refs),
        out_shape=(shape, shape, jax.ShapeDtypeStruct((8, BLOCKS), f32)),
        in_specs=[VMEM] * 4 + [ANY] * len(after),
        out_specs=(VMEM,) * 3,
        input_output_aliases={2: 0, 3: 1},
        compiler_params=params(6),
        cost_estimate=cost(1.5),
        interpret=INTERPRET,
        name="add_arrived",
    )(near, far, right, left, *after)


def second_hop(right, left):
    right = to_right(right)
    left = to_left(left)
    return right, left


def place_kernel(place_ref, slots_ref, *refs):
    keep0, right0, left0, keep1, right1, left1, extra = refs[:7]
    out_ref, token_ref, table_ref = refs[-3:]
    token_ref[...] = jnp.zeros(token_ref.shape, f32)
    plane = place_ref[0]
    first, second = keep0.shape[0], keep0.shape[0] + keep1.shape[0]
    table_ref[:first] = keep0[...] + right0[...] + left0[...]
    table_ref[first:second] = keep1[...] + right1[...] + left1[...]
    table_ref[second:] = extra[...]

    def body(owner, carry):
        position = (owner // 2) * 8 + 2 * plane + owner % 2
        for s in range(1, SUB):
            out_ref[owner, s - 1] = table_ref[slots_ref[s, position]]
        return carry

    lax.fori_loop(0, OWNERS, body, 0)


def place_slots(plane, slots, parts0, parts1, extra, after):
    _, rows, width = extra.shape
    size = OWNERS + SECOND + SPARE
    return pl.pallas_call(
        place_kernel,
        out_shape=(
            jax.ShapeDtypeStruct((OWNERS, SUB - 1, rows, width), f32),
            jax.ShapeDtypeStruct((8, BLOCKS), f32),
        ),
        in_specs=[SMEM, SMEM] + [VMEM] * 7 + [ANY] * len(after),
        out_specs=(VMEM, VMEM),
        scratch_shapes=[pltpu.VMEM((size, rows, width), f32)],
        compiler_params=params(12),
        cost_estimate=cost(4),
        interpret=INTERPRET,
        name="place_slots",
    )(plane, slots, *parts0, *parts1, extra, *after)


def total_kernel(keep_ref, right_ref, left_ref, out_ref):
    out_ref[...] = keep_ref[...] + right_ref[...] + left_ref[...]


def total(keep, right, left):
    return pl.pallas_call(
        total_kernel,
        out_shape=jax.ShapeDtypeStruct(keep.shape, f32),
        in_specs=[VMEM] * 3,
        out_specs=VMEM,
        compiler_params=params(8),
        cost_estimate=cost(1.5),
        interpret=INTERPRET,
        name="total",
    )(keep, right, left)


def to_owners(value):
    return lax.all_to_all(value, PLANE, split_axis=0, concat_axis=0, tiled=True)


def two_terms(value):
    high = value.astype(bf16)
    return high, (value - high.astype(f32)).astype(bf16)


def curvature_kernel(first, units, adding, weight_ref, field_ref, turn_ref, back_ref, occupied_ref, *refs):
    out_ref = refs[-1]
    previous = refs[0][...] if adding else 0.0
    unit = pl.program_id(0)
    sources = field_ref.shape[0] // (units * 40)
    n = field_ref.shape[1]
    stride = units * 40

    def plane_of(kind):
        return jnp.concatenate(
            [field_ref[pl.ds(unit * 40 + kind * 4 + r, sources, stride=stride), :] for r in range(4)], axis=0
        )

    matrices = jnp.concatenate(
        [jnp.concatenate([plane_of(2 * c), plane_of(2 * c + 1)], axis=1) for c in range(5)], axis=0
    )
    high, low = two_terms(matrices)
    vectors = turn_ref[0]
    rotated = jnp.dot(high, vectors, preferred_element_type=f32) + jnp.dot(low, vectors, preferred_element_type=f32)
    stacked = jnp.concatenate(
        [
            jnp.concatenate([rotated[c * n : (c + 1) * n, :n] for c in range(5)], axis=1),
            jnp.concatenate([rotated[c * n : (c + 1) * n, n:] for c in range(5)], axis=1),
        ],
        axis=0,
    )
    back = back_ref[0]
    high, low = two_terms(stacked)
    bar = jnp.dot(back, high, preferred_element_type=f32) + jnp.dot(back, low, preferred_element_type=f32)
    bar_real, bar_imag = bar[:n], bar[n:]
    diagonal = jnp.where(iota((n, n), 0) == iota((n, n), 1), bar_real[:, :n], 0.0)
    spacing = jnp.sum(diagonal, axis=0, keepdims=True) - jnp.sum(diagonal, axis=1, keepdims=True)
    smoothed = spacing / (spacing * spacing + broadening)

    def pick(value, c):
        return value[:, (c + 1) * n : (c + 2) * n]

    xcov_real = pick(bar_real, 2) + smoothed * pick(bar_real, 0)
    xcov_imag = pick(bar_imag, 2) + smoothed * pick(bar_imag, 0)
    ycov_real = pick(bar_real, 3) + smoothed * pick(bar_real, 1)
    ycov_imag = pick(bar_imag, 3) + smoothed * pick(bar_imag, 1)
    s = first + unit
    filled = occupied_ref[pl.ds(s, 1), :].astype(f32)
    filled_down = jnp.broadcast_to(filled, (n, n)).T
    pairing = filled_down * (1.0 - filled)
    product = pairing * (xcov_real * ycov_imag.T + xcov_imag * ycov_real.T)
    berry = jnp.sum(jnp.sum(product, axis=0, keepdims=True), axis=1, keepdims=True) * (-2.0 / n)
    weight = weight_ref[s]
    lane = iota((1, SUB), 1)
    result = jnp.where((lane == s) & (weight > 0.0), weight * berry, 0.0)
    before = jnp.where(unit == 0, previous, out_ref[...])
    out_ref[...] = result + before


def curvature(first, units, weight, arrived, vectors, adjoint, occupied, previous=(), after=()):
    width = arrived.shape[-1]
    flat = arrived.reshape(-1, width)
    matrix = pl.BlockSpec((1, 2 * width, 2 * width), lambda u: (first + u, 0, 0))
    return pl.pallas_call(
        lambda *refs: curvature_kernel(first, units, len(previous), *refs),
        grid=(units,),
        out_shape=jax.ShapeDtypeStruct((1, SUB), f32),
        in_specs=[
            SMEM,
            pl.BlockSpec(flat.shape, lambda u: (0, 0)),
            matrix,
            matrix,
            pl.BlockSpec(occupied.shape, lambda u: (0, 0)),
        ]
        + [pl.BlockSpec((1, SUB), lambda u: (0, 0))] * len(previous)
        + [ANY] * len(after),
        out_specs=pl.BlockSpec((1, SUB), lambda u: (0, 0)),
        compiler_params=params(58),
        cost_estimate=cost(2.5 * units),
        interpret=INTERPRET,
        name="curvature",
    )(weight, flat, vectors, adjoint, occupied, *previous, *after)


def vector_kernel(eigvecs_ref, *refs):
    turn_ref, back_ref, wide_ref = refs[-3:]
    n = eigvecs_ref.shape[2]
    wide_ref[...] = eigvecs_ref[0].astype(f32)
    real, imag = (wide_ref[pl.ds(part, n, stride=2), :].astype(bf16) for part in range(2))
    turn_ref[0, :n, :n] = real
    turn_ref[0, :n, n:] = imag
    turn_ref[0, n:, :n] = -imag
    turn_ref[0, n:, n:] = real
    group = n // OWNERS
    for part in range(2):
        packed = jnp.concatenate(
            [wide_ref[pl.ds(2 * r + part, OWNERS, stride=2 * group), :] for r in range(group)], axis=0
        )
        turned = packed.T
        if part == 0:
            back_ref[0, :n, :n] = turned.astype(bf16)
            back_ref[0, n:, n:] = turned.astype(bf16)
        else:
            back_ref[0, :n, n:] = turned.astype(bf16)
            back_ref[0, n:, :n] = (-turned).astype(bf16)


def vector_matrices(eigvecs, after):
    slots, width = eigvecs.shape[0], eigvecs.shape[1]
    shape = jax.ShapeDtypeStruct((slots, 2 * width, 2 * width), bf16)
    square = pl.BlockSpec((1, 2 * width, 2 * width), lambda i: (i, 0, 0))
    return pl.pallas_call(
        vector_kernel,
        grid=(slots,),
        out_shape=(shape, shape),
        in_specs=[pl.BlockSpec((1, 2 * width, width), lambda i: (i, 0, 0))] + [ANY] * len(after),
        out_specs=(square, square),
        scratch_shapes=[pltpu.VMEM((2 * width, width), f32)],
        compiler_params=params(4),
        cost_estimate=cost(2),
        interpret=INTERPRET,
        name="vector_matrices",
    )(eigvecs.reshape(slots, 2 * width, width), *after)


def body(base_k, counts, block_order, lattice, real_space, eigvecs, occupied):
    plane, core = lax.axis_index("row_0"), lax.axis_index("row_1")
    row = plane * 2 + core
    plane_ref = plane.reshape(1).astype(jnp.int32)
    core_ref = core.reshape(1).astype(jnp.int32)
    depth, _, slab, _, width = real_space.shape

    space = real_space.reshape(depth, 6 * slab, width)
    swap = [(0, 1), (1, 0)]
    send, token = send_rows(space, 1 - core_ref)
    mine = pack(row.reshape(1).astype(jnp.int32), base_k, counts, block_order, (token,))
    other = lax.ppermute(send, "row_1", swap)
    own_coords = jnp.pad(lattice.T.astype(f32), ((0, 5), (0, 0)))
    coords = jnp.concatenate([own_coords, lax.ppermute(own_coords, "row_1", swap)], axis=1)

    table = lax.all_to_all(mine, KA_ROW, 0, 0, tiled=True)
    table = table.reshape(BLOCKS, BLOCKS)
    matrices = join_rows(space, core_ref, other)
    points, slots, weights = find_points(table, plane_ref)
    position = (lax.axis_index(KA) * 8 + row).astype(jnp.int32)
    weight = lax.dynamic_slice(weights, (jnp.int32(0), position), (SUB, 1)).reshape(SUB)

    half = OWNERS // 2

    def sums(low, sizes, pitches, microseconds, after=(), streamed=False):
        return fourier(points, low, sizes, pitches, coords, matrices, microseconds, after, streamed)

    def rest(chunk, size, after):
        return sums(3 * OWNERS * (1 + chunk), (size,) * 3, (OWNERS,) * 3, 5, after)

    near0, far0, token = sums(0, (half, half), (half, half), 4, (), True)
    hop0 = first_hop(near0, far0)
    near1, far1, near3, far3, token = sums(
        OWNERS, (half, SECOND - half, half, half), (half,) * 4, 4, (token,)
    )
    hop1 = first_hop(near1, far1)
    right0, left0, keep0, token = rest(0, OWNERS, (token,))
    right0, left0, token = add_arrived(*hop0, right0, left0)
    ring0 = second_hop(right0, left0)
    right1, left1, keep1, token = rest(1, SECOND, (token,))
    right1, left1, token = add_arrived(*hop1, right1, left1)
    ring1 = second_hop(right1, left1)
    hop3 = first_hop(near3, far3)
    right3, left3, keep3, token = rest(2, OWNERS, (token,))

    def further(_):
        parts = (half, half, SPARE, SPARE, SPARE)
        near, far, right, left, keep, _ = sums(12 * OWNERS, parts, parts, 8)
        right, left, _ = add_arrived(*first_hop(near, far), right, left)
        right, left = second_hop(right, left)
        return keep + right + left

    empty = (SPARE,) + keep0.shape[1:]
    extra = lax.cond(slots[0, 0] > OWNERS + SECOND, further, lambda _: jnp.zeros(empty, f32), 0)

    placed, token = place_slots(plane_ref, slots, (keep0, *ring0), (keep1, *ring1), extra, (token,))
    unit123 = to_owners(placed)
    right3, left3, token = add_arrived(*hop3, right3, left3, (token,))
    ring3 = second_hop(right3, left3)
    turning, back = vector_matrices(eigvecs, (token,))
    unit0 = to_owners(total(keep3, *ring3))
    curve = curvature(1, 3, weight, unit123, turning, back, occupied)
    return curvature(0, 1, weight, unit0, turning, back, occupied, (curve,)).reshape(SUB)


def solution(mesh):
    finer = Mesh(mesh.devices.reshape(4, 4, 4, 2), ("ka_0", "ka_1", "row_0", "row_1"))
    placed = (
        P(KA, None),
        P(KA),
        P(KA_ROW),
        P(ROW, None),
        P(ROW, None, KA, None, None),
        P(KA_ROW, None, None, None),
        P(KA_ROW, None),
    )
    return jax.shard_map(body, mesh=finer, in_specs=placed, out_specs=P(KA_ROW), check_vma=False)
```

```python
import math

import jax
import jax.numpy as jnp
from jax import lax
from jax.experimental import pallas as pl
from jax.experimental.pallas import tpu as pltpu
from jax.sharding import Mesh
from jax.sharding import PartitionSpec as P

SUB = 4
KA = ("ka_0", "ka_1")
KA_ROW = ("ka_0", "ka_1", "row_0", "row_1")
ROW = ("row_0", "row_1")
PLANE = ("ka_0", "ka_1", "row_1")
INTERPRET = False

broadening = 1.0
refine_step = (0.05, 0.03, 0.02)

f32 = jnp.float32
bf16 = jnp.bfloat16
VMEM = pl.BlockSpec(memory_space=pltpu.VMEM)
SMEM = pl.BlockSpec(memory_space=pltpu.SMEM)
NX = 4
OWNERS = 32
SECOND = 32
SPARE = 32
BLOCKS = 128


def params(mebibytes):
    return pltpu.CompilerParams(vmem_limit_bytes=mebibytes << 20)


ANY = pl.BlockSpec(memory_space=pl.ANY)
HBM = pl.BlockSpec(memory_space=pltpu.HBM)


def cost(microseconds):
    return pl.CostEstimate(flops=int(microseconds * 2.5e8), bytes_accessed=0, transcendentals=0)


def iota(shape, dim):
    return lax.broadcasted_iota(jnp.int32, shape, dim)


def place_of(position):
    plane = (position % 8) // 2
    owner = (position // 8) * 2 + position % 2
    return plane, owner


def index_kernel(place_ref, table_ref, points_ref, slots_ref, weight_ref):
    my_plane = place_ref[0]
    table = table_ref[...]
    turned = table.T
    square = (BLOCKS, BLOCKS)
    order_down = table[:, 4:5].astype(jnp.int32)
    order_along = turned[4:5, :].astype(jnp.int32)
    here_down = order_down == iota(square, 1)
    here_along = iota(square, 0) == order_along

    def along(column):
        return jnp.sum(jnp.where(here_along, table[:, column : column + 1], 0.0), axis=0, keepdims=True)

    base = [along(axis) for axis in range(3)]
    count = along(3)
    count_down = jnp.sum(jnp.where(here_down, turned[3:4, :], 0.0), axis=1, keepdims=True)

    plane_down, owner_down = place_of(iota(square, 0))
    plane_along, owner_along = place_of(iota(square, 1))
    mates = plane_down == plane_along
    ahead = mates & (owner_down < owner_along)
    plane_row, owner_row = place_of(iota((1, BLOCKS), 1))
    away = (plane_row - my_plane + NX) % NX
    seat = jnp.where(away == 1, 0, jnp.where(away == 3, 1, 2))

    def row_of(chunk, within):
        opposite = OWNERS * chunk + within
        apart = 3 * OWNERS * (1 + chunk) + seat * OWNERS + within
        spare = 12 * OWNERS + jnp.where(away == 2, 0, 1 + seat) * SPARE + within
        return jnp.where(chunk == 3, spare, jnp.where(away == 2, opposite, apart))

    rows = 12 * OWNERS + NX * SPARE
    entry = iota((rows, BLOCKS), 0)
    lane = iota((rows, BLOCKS), 1)
    gathered = [jnp.zeros((rows, BLOCKS), f32) for _ in range(3)]
    before = jnp.zeros((1, BLOCKS), f32)
    slots_ref[...] = jnp.zeros((8, BLOCKS), jnp.int32)
    weight_ref[...] = jnp.zeros((8, BLOCKS), f32)
    for s in range(SUB):
        fraction = (s + 0.5) / count - 0.5
        points = [base[axis] + fraction * refine_step[axis] for axis in range(3)]
        alive = count > s
        weight_ref[s : s + 1, :] = jnp.where(alive, 1.0 / count, 0.0)
        if s == 0:
            chunk, within = jnp.full((1, BLOCKS), 2, jnp.int32), owner_row
        else:
            live_down = count_down > s
            rank = before + jnp.sum(jnp.where(ahead & live_down, 1.0, 0.0), axis=0, keepdims=True)
            before = before + jnp.sum(jnp.where(mates & live_down, 1.0, 0.0), axis=0, keepdims=True)
            rank = jnp.where(alive, rank, 0.0).astype(jnp.int32)
            slots_ref[s : s + 1, :] = rank
            chunk = jnp.where(rank < OWNERS, 0, jnp.where(rank < OWNERS + SECOND, 1, 3))
            within = rank - jnp.where(chunk == 0, 0, jnp.where(chunk == 1, OWNERS, OWNERS + SECOND))
        match = entry == jnp.where(alive, row_of(chunk, within), -1)
        for axis in range(3):
            gathered[axis] = gathered[axis] + jnp.where(match, points[axis], 0.0)
    most = jnp.max(before, axis=1, keepdims=True)
    slots_ref[0:1, :] = jnp.broadcast_to(most, (1, BLOCKS)).astype(jnp.int32)
    points = jnp.zeros((rows, BLOCKS), f32)
    for axis in range(3):
        points = jnp.where(lane == axis, jnp.sum(gathered[axis], axis=1, keepdims=True), points)
    points_ref[...] = points


def pieces_of(depth):
    return [(matrix, slice(half * depth // 2, (half + 1) * depth // 2)) for matrix in range(3) for half in range(2)]


def coming_rows(core, space_ref, in_buffer, sems):
    _, depth, rows, _ = in_buffer.shape
    copies = []
    for k, (matrix, at) in enumerate(pieces_of(depth)):
        first = pl.multiple_of(rows * (2 * matrix + core), rows)
        copies.append(
            pltpu.make_async_copy(space_ref.at[at, pl.ds(first, rows), :], in_buffer.at[matrix, at], sems.at[k])
        )
    return copies


def turn_rows(in_buffer, wide_ref, matrix, at, store):
    _, _, rows, width = in_buffer.shape
    size = at.stop - at.start
    for first in range(0, size, 8):
        wide = in_buffer[matrix, at.start + first : at.start + first + 8].astype(f32)
        for r in range(8):
            wide_ref[(first + r) * rows : (first + r + 1) * rows, :] = wide[r]
    for part in range(2):
        for r in range(rows // 2):
            store(part, slice(r * width, (r + 1) * width), wide_ref[pl.ds(2 * r + part, size, stride=rows), :])


def send_kernel(
    core_ref, row_ref, base_ref, counts_ref, order_ref, space_ref, out_ref, told_ref, *scratch
):
    in_buffer, out_buffer, wide_ref, in_sems, out_sems = scratch
    depth = in_buffer.shape[1]
    coming = coming_rows(core_ref[0], space_ref, in_buffer, in_sems)
    places = pieces_of(depth)
    going = [
        pltpu.make_async_copy(out_buffer.at[matrix, :, at], out_ref.at[matrix, :, at], out_sems.at[k])
        for k, (matrix, at) in enumerate(places)
    ]
    for copy in coming:
        copy.start()
    lane = iota((1, BLOCKS), 1)
    told = jnp.where(lane == 4, order_ref[...].astype(f32), 0.0)
    own = iota((1, 8), 1) == row_ref[0]
    told = jnp.where(lane == 3, jnp.sum(jnp.where(own, counts_ref[...].astype(f32), 0.0), axis=1, keepdims=True), told)
    for axis in range(3):
        part = jnp.where(own, base_ref[axis : axis + 1, :], 0.0)
        told = jnp.where(lane == axis, jnp.sum(part, axis=1, keepdims=True), told)
    told_ref[...] = jnp.broadcast_to(told.reshape(1, 1, BLOCKS), told_ref.shape)
    for k, (matrix, at) in enumerate(places):
        coming[k].wait()

        def store(part, lanes, value):
            out_buffer[matrix, part, at, lanes] = value

        turn_rows(in_buffer, wide_ref, matrix, at, store)
        going[k].start()
    for copy in going:
        copy.wait()


def send_rows(space, core, row, base_k, counts, block_order):
    depth, rows, width = space.shape
    half = rows // 6
    shape = (3, 2, depth, half // 2 * width)
    return pl.pallas_call(
        send_kernel,
        out_shape=(jax.ShapeDtypeStruct(shape, f32), jax.ShapeDtypeStruct((BLOCKS, 1, BLOCKS), f32)),
        in_specs=[SMEM, SMEM, VMEM, VMEM, VMEM, HBM],
        out_specs=(HBM, VMEM),
        scratch_shapes=[
            pltpu.VMEM((3, depth, half, width), bf16),
            pltpu.VMEM(shape, f32),
            pltpu.VMEM((depth // 2 * half, width), f32),
            pltpu.SemaphoreType.DMA((6,)),
            pltpu.SemaphoreType.DMA((6,)),
        ],
        compiler_params=params(58),
        cost_estimate=cost(5),
        interpret=INTERPRET,
        name="send_rows",
    )(core, row, base_k.T, counts.reshape(1, 8), block_order.reshape(1, 1), space)


def join_kernel(core_ref, space_ref, other_ref, out_ref, in_buffer, other_buffer, wide_ref, in_sems, other_sems):
    depth = in_buffer.shape[1]
    coming = coming_rows(core_ref[0], space_ref, in_buffer, in_sems)
    places = pieces_of(depth)
    others = [
        pltpu.make_async_copy(other_ref.at[matrix, :, at], other_buffer.at[matrix, :, at], other_sems.at[k])
        for k, (matrix, at) in enumerate(places)
    ]
    for k in range(6):
        coming[k].start()
        others[k].start()
    for k, (matrix, at) in enumerate(places):
        coming[k].wait()

        def store(part, lanes, value):
            rows = slice(part * depth + at.start, part * depth + at.stop)
            out_ref[matrix, rows, lanes] = value.astype(bf16)

        turn_rows(in_buffer, wide_ref, matrix, at, store)
        others[k].wait()
        for part in range(2):
            rows = slice((2 + part) * depth + at.start, (2 + part) * depth + at.stop)
            out_ref[matrix, rows, :] = other_buffer[matrix, part, at, :].astype(bf16)


def join_rows(space, core, other):
    depth, rows, width = space.shape
    half = rows // 6
    lanes = half // 2 * width
    return pl.pallas_call(
        join_kernel,
        out_shape=jax.ShapeDtypeStruct((3, 4 * depth, lanes), bf16),
        in_specs=[SMEM, HBM, HBM],
        out_specs=VMEM,
        scratch_shapes=[
            pltpu.VMEM((3, depth, half, width), bf16),
            pltpu.VMEM((3, 2, depth, lanes), f32),
            pltpu.VMEM((depth // 2 * half, width), f32),
            pltpu.SemaphoreType.DMA((6,)),
            pltpu.SemaphoreType.DMA((6,)),
        ],
        compiler_params=params(54),
        cost_estimate=cost(5),
        interpret=INTERPRET,
        name="join_rows",
    )(core, space, other)


def turn(points, coords):
    turns = points[:, 0:1] * coords[0:1, :] + points[:, 1:2] * coords[1:2, :] + points[:, 2:3] * coords[2:3, :]
    rest = turns - jnp.floor(turns + 0.5)
    quarter = jnp.floor(4.0 * rest + 0.5)
    angle = (rest - 0.25 * quarter) * (2.0 * math.pi)
    square = angle * angle
    sine = angle * (1.0 + square * (-1.0 / 6 + square * (1.0 / 120 + square * (-1.0 / 5040 + square * (1.0 / 362880)))))
    cosine = 1.0 + square * (-0.5 + square * (1.0 / 24 + square * (-1.0 / 720 + square * (1.0 / 40320 - square / 3628800))))
    odd = jnp.abs(quarter) == 1.0
    first = jnp.where(odd, sine, cosine)
    second = jnp.where(odd, cosine, sine)
    cos_sign = jnp.where((quarter == 1.0) | (jnp.abs(quarter) == 2.0), -1.0, 1.0)
    sin_sign = jnp.where((quarter == -1.0) | (jnp.abs(quarter) == 2.0), -1.0, 1.0)
    return first * cos_sign, second * sin_sign


def store_phases(low, count, points_ref, coords_ref, phase_ref):
    depth = coords_ref.shape[1] // 2
    tile = 16

    def rows_of(i, carry):
        first = pl.multiple_of(i * tile, tile)
        points = points_ref[pl.ds(low + first, tile), :]
        for source in range(2):
            coords = coords_ref[:, source * depth : (source + 1) * depth]
            cosine, sine = turn(points, coords)
            at_real = slice(source * 2 * depth, source * 2 * depth + depth)
            at_imag = slice(source * 2 * depth + depth, source * 2 * depth + 2 * depth)
            pairs = [(cosine, sine)]
            for axis in range(2):
                coord = coords[axis : axis + 1, :]
                pairs.append((-coord * sine, coord * cosine))
            for kind, (real, imag) in enumerate(pairs):
                real_rows = pl.ds(2 * kind * count + first, tile)
                imag_rows = pl.ds((2 * kind + 1) * count + first, tile)
                phase_ref[real_rows, at_real] = real.astype(bf16)
                phase_ref[real_rows, at_imag] = (-imag).astype(bf16)
                phase_ref[imag_rows, at_real] = imag.astype(bf16)
                phase_ref[imag_rows, at_imag] = real.astype(bf16)
        return carry

    lax.fori_loop(0, count // tile, rows_of, 0)


def store_sums(phase_ref, matrices, count, kinds, first_kind, first_row, out_refs, pitches):
    product = jnp.dot(phase_ref[: kinds * count, :], matrices, preferred_element_type=f32)
    width = product.shape[1] // 2
    for kind in range(kinds):
        for half in range(2):
            block = product[kind * count : (kind + 1) * count, half * width : (half + 1) * width]
            at = (first_kind + kind) * 4 + first_row + half
            start = 0
            for ref, pitch in zip(out_refs, pitches):
                size = ref.shape[0] // 40
                ref[pl.ds(at, size, stride=40), :] = block[start : start + size]
                start += pitch


PLACES = tuple((matrix, part) for matrix in range(3) for part in range(2))


def fourier_kernel(low, pitches, waits, points_ref, coords_ref, matrices_ref, *refs):
    refs = refs[waits:]
    outs = len(pitches)
    out_refs, token_ref, phase_ref = refs[:outs], refs[outs], refs[outs + 1]
    token_ref[...] = jnp.zeros(token_ref.shape, f32)
    count = sum(pitches)
    lanes = matrices_ref.shape[2] // 2
    store_phases(low, count, points_ref, coords_ref, phase_ref)
    for matrix, part in PLACES:
        kinds, first_kind = (6, 0) if matrix == 0 else (2, 4 + 2 * matrix)
        block = matrices_ref[matrix, :, part * lanes : (part + 1) * lanes]
        store_sums(phase_ref, block, count, kinds, first_kind, 2 * part, out_refs, pitches)


def fourier(points, low, sizes, pitches, coords, matrices, microseconds, after=()):
    depth4 = matrices.shape[1]
    width = matrices.shape[2] // 4
    shapes = tuple(jax.ShapeDtypeStruct((size * 40, width), f32) for size in sizes)
    outs = pl.pallas_call(
        lambda *refs: fourier_kernel(low, pitches, len(after), *refs),
        out_shape=shapes + (jax.ShapeDtypeStruct((8, BLOCKS), f32),),
        in_specs=[VMEM, VMEM, VMEM] + [ANY] * len(after),
        out_specs=(VMEM,) * (len(shapes) + 1),
        scratch_shapes=[pltpu.VMEM((6 * sum(pitches), depth4), bf16)],
        compiler_params=params(18),
        cost_estimate=cost(microseconds),
        interpret=INTERPRET,
        name="fourier",
    )(points, coords, matrices, *after)
    return tuple(out.reshape(-1, 40, width) for out in outs[:-1]) + (outs[-1],)


def first_kernel(place_ref, table_ref, coords_ref, matrices_ref, *refs):
    near_ref, far_ref, points_ref, slots_ref, weight_ref, token_ref, phase_ref, buffer_ref, sems = refs
    token_ref[...] = jnp.zeros(token_ref.shape, f32)
    lanes = matrices_ref.shape[2] // 2
    copies = []
    for k, (matrix, part) in enumerate(PLACES):
        source = matrices_ref.at[matrix, :, pl.ds(part * lanes, lanes)]
        copies.append(pltpu.make_async_copy(source, buffer_ref.at[k], sems.at[k]))
    for copy in copies:
        copy.start()
    index_kernel(place_ref, table_ref, points_ref, slots_ref, weight_ref)
    store_phases(0, OWNERS, points_ref, coords_ref, phase_ref)
    for k, (matrix, part) in enumerate(PLACES):
        kinds, first_kind = (6, 0) if matrix == 0 else (2, 4 + 2 * matrix)
        copies[k].wait()
        store_sums(
            phase_ref, buffer_ref[k], OWNERS, kinds, first_kind, 2 * part, (near_ref, far_ref), (OWNERS // 2,) * 2
        )


def first_fourier(table, plane, coords, matrices):
    depth4 = matrices.shape[1]
    width = matrices.shape[2] // 4
    side = jax.ShapeDtypeStruct((OWNERS // 2 * 40, width), f32)
    near, far, points, slots, weights, token = pl.pallas_call(
        first_kernel,
        out_shape=(
            side,
            side,
            jax.ShapeDtypeStruct((12 * OWNERS + NX * SPARE, BLOCKS), f32),
            jax.ShapeDtypeStruct((8, BLOCKS), jnp.int32),
            jax.ShapeDtypeStruct((8, BLOCKS), f32),
            jax.ShapeDtypeStruct((8, BLOCKS), f32),
        ),
        in_specs=[SMEM, VMEM, VMEM, HBM],
        out_specs=(VMEM,) * 6,
        scratch_shapes=[
            pltpu.VMEM((6 * OWNERS, depth4), bf16),
            pltpu.VMEM((6, depth4, 2 * width), bf16),
            pltpu.SemaphoreType.DMA((6,)),
        ],
        compiler_params=params(18),
        cost_estimate=cost(5),
        interpret=INTERPRET,
        name="first_fourier",
    )(plane, table, coords, matrices)
    return near.reshape(-1, 40, width), far.reshape(-1, 40, width), points, slots, weights, token


def to_right(value):
    return lax.ppermute(value, "row_0", [(i, (i + 1) % NX) for i in range(NX)])


def to_left(value):
    return lax.ppermute(value, "row_0", [(i, (i - 1) % NX) for i in range(NX)])


def first_hop(near, far):
    near = to_right(near)
    far = to_left(far)
    return near, far


def add_kernel(waits, near_ref, far_ref, right_ref, left_ref, *refs):
    right_out, left_out, token_ref = refs[waits:]
    half = near_ref.shape[0]
    right_out[:half] = right_ref[:half] + near_ref[...]
    right_out[half:] = right_ref[half:]
    left_out[:half] = left_ref[:half]
    left_out[half:] = left_ref[half:] + far_ref[...]
    token_ref[...] = jnp.zeros(token_ref.shape, f32)


def add_arrived(near, far, right, left, after=()):
    shape = jax.ShapeDtypeStruct(right.shape, f32)
    return pl.pallas_call(
        lambda *refs: add_kernel(len(after), *refs),
        out_shape=(shape, shape, jax.ShapeDtypeStruct((8, BLOCKS), f32)),
        in_specs=[VMEM] * 4 + [ANY] * len(after),
        out_specs=(VMEM,) * 3,
        input_output_aliases={2: 0, 3: 1},
        compiler_params=params(6),
        cost_estimate=cost(1.5),
        interpret=INTERPRET,
        name="add_arrived",
    )(near, far, right, left, *after)


def second_hop(right, left):
    right = to_right(right)
    left = to_left(left)
    return right, left


def place_kernel(place_ref, slots_ref, *refs):
    keep0, right0, left0, keep1, right1, left1, extra = refs[:7]
    out_ref, token_ref, table_ref = refs[-3:]
    token_ref[...] = jnp.zeros(token_ref.shape, f32)
    plane = place_ref[0]
    first, second = keep0.shape[0], keep0.shape[0] + keep1.shape[0]
    table_ref[:first] = keep0[...] + right0[...] + left0[...]
    table_ref[first:second] = keep1[...] + right1[...] + left1[...]
    table_ref[second:] = extra[...]

    def body(owner, carry):
        position = (owner // 2) * 8 + 2 * plane + owner % 2
        for s in range(1, SUB):
            out_ref[owner, s - 1] = table_ref[slots_ref[s, position]]
        return carry

    lax.fori_loop(0, OWNERS, body, 0)


def place_slots(plane, slots, parts0, parts1, extra, after):
    _, rows, width = extra.shape
    size = OWNERS + SECOND + SPARE
    return pl.pallas_call(
        place_kernel,
        out_shape=(
            jax.ShapeDtypeStruct((OWNERS, SUB - 1, rows, width), f32),
            jax.ShapeDtypeStruct((8, BLOCKS), f32),
        ),
        in_specs=[SMEM, SMEM] + [VMEM] * 7 + [ANY] * len(after),
        out_specs=(VMEM, VMEM),
        scratch_shapes=[pltpu.VMEM((size, rows, width), f32)],
        compiler_params=params(12),
        cost_estimate=cost(4),
        interpret=INTERPRET,
        name="place_slots",
    )(plane, slots, *parts0, *parts1, extra, *after)


def total_kernel(keep_ref, right_ref, left_ref, out_ref):
    out_ref[...] = keep_ref[...] + right_ref[...] + left_ref[...]


def total(keep, right, left):
    return pl.pallas_call(
        total_kernel,
        out_shape=jax.ShapeDtypeStruct(keep.shape, f32),
        in_specs=[VMEM] * 3,
        out_specs=VMEM,
        compiler_params=params(8),
        cost_estimate=cost(1.5),
        interpret=INTERPRET,
        name="total",
    )(keep, right, left)


def to_owners(value):
    return lax.all_to_all(value, PLANE, split_axis=0, concat_axis=0, tiled=True)


def two_terms(value):
    high = value.astype(bf16)
    return high, (value - high.astype(f32)).astype(bf16)


def curvature_kernel(first, units, adding, weight_ref, field_ref, turn_ref, back_ref, occupied_ref, *refs):
    out_ref = refs[-1]
    previous = refs[0][...] if adding else 0.0
    unit = pl.program_id(0)
    sources = field_ref.shape[0] // (units * 40)
    n = field_ref.shape[1]
    stride = units * 40

    def plane_of(kind):
        return jnp.concatenate(
            [field_ref[pl.ds(unit * 40 + kind * 4 + r, sources, stride=stride), :] for r in range(4)], axis=0
        )

    matrices = jnp.concatenate(
        [jnp.concatenate([plane_of(2 * c), plane_of(2 * c + 1)], axis=1) for c in range(5)], axis=0
    )
    high, low = two_terms(matrices)
    vectors = turn_ref[0]
    rotated = jnp.dot(high, vectors, preferred_element_type=f32) + jnp.dot(low, vectors, preferred_element_type=f32)
    stacked = jnp.concatenate(
        [
            jnp.concatenate([rotated[c * n : (c + 1) * n, :n] for c in range(5)], axis=1),
            jnp.concatenate([rotated[c * n : (c + 1) * n, n:] for c in range(5)], axis=1),
        ],
        axis=0,
    )
    back = back_ref[0]
    high, low = two_terms(stacked)
    bar = jnp.dot(back, high, preferred_element_type=f32) + jnp.dot(back, low, preferred_element_type=f32)
    bar_real, bar_imag = bar[:n], bar[n:]
    diagonal = jnp.where(iota((n, n), 0) == iota((n, n), 1), bar_real[:, :n], 0.0)
    spacing = jnp.sum(diagonal, axis=0, keepdims=True) - jnp.sum(diagonal, axis=1, keepdims=True)
    smoothed = spacing / (spacing * spacing + broadening)

    def pick(value, c):
        return value[:, (c + 1) * n : (c + 2) * n]

    xcov_real = pick(bar_real, 2) + smoothed * pick(bar_real, 0)
    xcov_imag = pick(bar_imag, 2) + smoothed * pick(bar_imag, 0)
    ycov_real = pick(bar_real, 3) + smoothed * pick(bar_real, 1)
    ycov_imag = pick(bar_imag, 3) + smoothed * pick(bar_imag, 1)
    s = first + unit
    filled = occupied_ref[pl.ds(s, 1), :].astype(f32)
    filled_down = jnp.broadcast_to(filled, (n, n)).T
    pairing = filled_down * (1.0 - filled)
    product = pairing * (xcov_real * ycov_imag.T + xcov_imag * ycov_real.T)
    berry = jnp.sum(jnp.sum(product, axis=0, keepdims=True), axis=1, keepdims=True) * (-2.0 / n)
    weight = weight_ref[s]
    lane = iota((1, SUB), 1)
    result = jnp.where((lane == s) & (weight > 0.0), weight * berry, 0.0)
    before = jnp.where(unit == 0, previous, out_ref[...])
    out_ref[...] = result + before


def curvature(first, units, weight, arrived, vectors, adjoint, occupied, previous=(), after=()):
    width = arrived.shape[-1]
    flat = arrived.reshape(-1, width)
    matrix = pl.BlockSpec((1, 2 * width, 2 * width), lambda u: (first + u, 0, 0))
    return pl.pallas_call(
        lambda *refs: curvature_kernel(first, units, len(previous), *refs),
        grid=(units,),
        out_shape=jax.ShapeDtypeStruct((1, SUB), f32),
        in_specs=[
            SMEM,
            pl.BlockSpec(flat.shape, lambda u: (0, 0)),
            matrix,
            matrix,
            pl.BlockSpec(occupied.shape, lambda u: (0, 0)),
        ]
        + [pl.BlockSpec((1, SUB), lambda u: (0, 0))] * len(previous)
        + [ANY] * len(after),
        out_specs=pl.BlockSpec((1, SUB), lambda u: (0, 0)),
        compiler_params=params(58),
        cost_estimate=cost(2.5 * units),
        interpret=INTERPRET,
        name="curvature",
    )(weight, flat, vectors, adjoint, occupied, *previous, *after)


def vector_kernel(eigvecs_ref, *refs):
    turn_ref, back_ref, wide_ref = refs[-3:]
    n = eigvecs_ref.shape[2]
    wide_ref[...] = eigvecs_ref[0].astype(f32)
    real, imag = (wide_ref[pl.ds(part, n, stride=2), :].astype(bf16) for part in range(2))
    turn_ref[0, :n, :n] = real
    turn_ref[0, :n, n:] = imag
    turn_ref[0, n:, :n] = -imag
    turn_ref[0, n:, n:] = real
    group = n // OWNERS
    for part in range(2):
        packed = jnp.concatenate(
            [wide_ref[pl.ds(2 * r + part, OWNERS, stride=2 * group), :] for r in range(group)], axis=0
        )
        turned = packed.T
        if part == 0:
            back_ref[0, :n, :n] = turned.astype(bf16)
            back_ref[0, n:, n:] = turned.astype(bf16)
        else:
            back_ref[0, :n, n:] = turned.astype(bf16)
            back_ref[0, n:, :n] = (-turned).astype(bf16)


def vector_matrices(eigvecs, after):
    slots, width = eigvecs.shape[0], eigvecs.shape[1]
    shape = jax.ShapeDtypeStruct((slots, 2 * width, 2 * width), bf16)
    square = pl.BlockSpec((1, 2 * width, 2 * width), lambda i: (i, 0, 0))
    return pl.pallas_call(
        vector_kernel,
        grid=(slots,),
        out_shape=(shape, shape),
        in_specs=[pl.BlockSpec((1, 2 * width, width), lambda i: (i, 0, 0))] + [ANY] * len(after),
        out_specs=(square, square),
        scratch_shapes=[pltpu.VMEM((2 * width, width), f32)],
        compiler_params=params(4),
        cost_estimate=cost(2),
        interpret=INTERPRET,
        name="vector_matrices",
    )(eigvecs.reshape(slots, 2 * width, width), *after)


def body(base_k, counts, block_order, lattice, real_space, eigvecs, occupied):
    plane, core = lax.axis_index("row_0"), lax.axis_index("row_1")
    row = plane * 2 + core
    plane_ref = plane.reshape(1).astype(jnp.int32)
    core_ref = core.reshape(1).astype(jnp.int32)
    depth, _, slab, _, width = real_space.shape

    space = real_space.reshape(depth, 6 * slab, width)
    swap = [(0, 1), (1, 0)]
    row_ref = row.reshape(1).astype(jnp.int32)
    send, mine = send_rows(space, 1 - core_ref, row_ref, base_k, counts, block_order)
    other = lax.ppermute(send, "row_1", swap)
    own_coords = jnp.pad(lattice.T.astype(f32), ((0, 5), (0, 0)))
    coords = jnp.concatenate([own_coords, lax.ppermute(own_coords, "row_1", swap)], axis=1)

    table = lax.all_to_all(mine, KA_ROW, 0, 0, tiled=True)
    table = table.reshape(BLOCKS, BLOCKS)
    matrices = join_rows(space, core_ref, other)
    near0, far0, points, slots, weights, token = first_fourier(table, plane_ref, coords, matrices)
    position = (lax.axis_index(KA) * 8 + row).astype(jnp.int32)
    weight = lax.dynamic_slice(weights, (jnp.int32(0), position), (SUB, 1)).reshape(SUB)

    half = OWNERS // 2

    def sums(low, sizes, pitches, microseconds, after=()):
        return fourier(points, low, sizes, pitches, coords, matrices, microseconds, after)

    def rest(chunk, size, after):
        return sums(3 * OWNERS * (1 + chunk), (size,) * 3, (OWNERS,) * 3, 5, after)

    hop0 = first_hop(near0, far0)
    near1, far1, near3, far3, token = sums(
        OWNERS, (half, SECOND - half, half, half), (half,) * 4, 4, (token,)
    )
    hop1 = first_hop(near1, far1)
    right0, left0, keep0, token = rest(0, OWNERS, (token,))
    right0, left0, token = add_arrived(*hop0, right0, left0)
    ring0 = second_hop(right0, left0)
    right1, left1, keep1, token = rest(1, SECOND, (token,))
    right1, left1, token = add_arrived(*hop1, right1, left1)
    ring1 = second_hop(right1, left1)
    hop3 = first_hop(near3, far3)
    right3, left3, keep3, token = rest(2, OWNERS, (token,))

    def further(_):
        parts = (half, half, SPARE, SPARE, SPARE)
        near, far, right, left, keep, _ = sums(12 * OWNERS, parts, parts, 8)
        right, left, _ = add_arrived(*first_hop(near, far), right, left)
        right, left = second_hop(right, left)
        return keep + right + left

    empty = (SPARE,) + keep0.shape[1:]
    extra = lax.cond(slots[0, 0] > OWNERS + SECOND, further, lambda _: jnp.zeros(empty, f32), 0)

    placed, token = place_slots(plane_ref, slots, (keep0, *ring0), (keep1, *ring1), extra, (token,))
    unit123 = to_owners(placed)
    right3, left3, token = add_arrived(*hop3, right3, left3, (token,))
    ring3 = second_hop(right3, left3)
    turning, back = vector_matrices(eigvecs, (token,))
    unit0 = to_owners(total(keep3, *ring3))
    curve = curvature(1, 3, weight, unit123, turning, back, occupied)
    return curvature(0, 1, weight, unit0, turning, back, occupied, (curve,)).reshape(SUB)


def solution(mesh):
    finer = Mesh(mesh.devices.reshape(4, 4, 4, 2), ("ka_0", "ka_1", "row_0", "row_1"))
    placed = (
        P(KA, None),
        P(KA),
        P(KA_ROW),
        P(ROW, None),
        P(ROW, None, KA, None, None),
        P(KA_ROW, None, None, None),
        P(KA_ROW, None),
    )
    return jax.shard_map(body, mesh=finer, in_specs=placed, out_specs=P(KA_ROW), check_vma=False)
```

```python
import math

import jax
import jax.numpy as jnp
from jax import lax
from jax.experimental import pallas as pl
from jax.experimental.pallas import tpu as pltpu
from jax.sharding import Mesh
from jax.sharding import PartitionSpec as P

SUB = 4
KA = ("ka_0", "ka_1")
KA_ROW = ("ka_0", "ka_1", "row_0", "row_1")
ROW = ("row_0", "row_1")
PLANE = ("ka_0", "ka_1", "row_1")
INTERPRET = False

broadening = 1.0
refine_step = (0.05, 0.03, 0.02)

f32 = jnp.float32
bf16 = jnp.bfloat16
VMEM = pl.BlockSpec(memory_space=pltpu.VMEM)
SMEM = pl.BlockSpec(memory_space=pltpu.SMEM)
NX = 4
OWNERS = 32
SECOND = 32
SPARE = 32
BLOCKS = 128


def params(mebibytes):
    return pltpu.CompilerParams(vmem_limit_bytes=mebibytes << 20)


ANY = pl.BlockSpec(memory_space=pl.ANY)
HBM = pl.BlockSpec(memory_space=pltpu.HBM)


def cost(microseconds):
    return pl.CostEstimate(flops=int(microseconds * 2.5e8), bytes_accessed=0, transcendentals=0)


def iota(shape, dim):
    return lax.broadcasted_iota(jnp.int32, shape, dim)


def place_of(position):
    plane = (position % 8) // 2
    owner = (position // 8) * 2 + position % 2
    return plane, owner


def index_kernel(place_ref, table_ref, points_ref, slots_ref, weight_ref):
    my_plane = place_ref[0]
    table = table_ref[...]
    turned = table.T
    square = (BLOCKS, BLOCKS)
    order_down = table[:, 4:5].astype(jnp.int32)
    order_along = turned[4:5, :].astype(jnp.int32)
    here_down = order_down == iota(square, 1)
    here_along = iota(square, 0) == order_along

    def along(column):
        return jnp.sum(jnp.where(here_along, table[:, column : column + 1], 0.0), axis=0, keepdims=True)

    base = [along(axis) for axis in range(3)]
    count = along(3)
    count_down = jnp.sum(jnp.where(here_down, turned[3:4, :], 0.0), axis=1, keepdims=True)

    plane_down, owner_down = place_of(iota(square, 0))
    plane_along, owner_along = place_of(iota(square, 1))
    mates = plane_down == plane_along
    ahead = mates & (owner_down < owner_along)
    plane_row, owner_row = place_of(iota((1, BLOCKS), 1))
    away = (plane_row - my_plane + NX) % NX
    seat = jnp.where(away == 1, 0, jnp.where(away == 3, 1, 2))

    def row_of(chunk, within):
        opposite = OWNERS * chunk + within
        apart = 3 * OWNERS * (1 + chunk) + seat * OWNERS + within
        spare = 12 * OWNERS + jnp.where(away == 2, 0, 1 + seat) * SPARE + within
        return jnp.where(chunk == 3, spare, jnp.where(away == 2, opposite, apart))

    rows = 12 * OWNERS + NX * SPARE
    entry = iota((rows, BLOCKS), 0)
    lane = iota((rows, BLOCKS), 1)
    gathered = [jnp.zeros((rows, BLOCKS), f32) for _ in range(3)]
    before = jnp.zeros((1, BLOCKS), f32)
    slots_ref[...] = jnp.zeros((8, BLOCKS), jnp.int32)
    weight_ref[...] = jnp.zeros((8, BLOCKS), f32)
    for s in range(SUB):
        fraction = (s + 0.5) / count - 0.5
        points = [base[axis] + fraction * refine_step[axis] for axis in range(3)]
        alive = count > s
        weight_ref[s : s + 1, :] = jnp.where(alive, 1.0 / count, 0.0)
        if s == 0:
            chunk, within = jnp.full((1, BLOCKS), 2, jnp.int32), owner_row
        else:
            live_down = count_down > s
            rank = before + jnp.sum(jnp.where(ahead & live_down, 1.0, 0.0), axis=0, keepdims=True)
            before = before + jnp.sum(jnp.where(mates & live_down, 1.0, 0.0), axis=0, keepdims=True)
            rank = jnp.where(alive, rank, 0.0).astype(jnp.int32)
            slots_ref[s : s + 1, :] = rank
            chunk = jnp.where(rank < OWNERS, 0, jnp.where(rank < OWNERS + SECOND, 1, 3))
            within = rank - jnp.where(chunk == 0, 0, jnp.where(chunk == 1, OWNERS, OWNERS + SECOND))
        match = entry == jnp.where(alive, row_of(chunk, within), -1)
        for axis in range(3):
            gathered[axis] = gathered[axis] + jnp.where(match, points[axis], 0.0)
    most = jnp.max(before, axis=1, keepdims=True)
    slots_ref[0:1, :] = jnp.broadcast_to(most, (1, BLOCKS)).astype(jnp.int32)
    points = jnp.zeros((rows, BLOCKS), f32)
    for axis in range(3):
        points = jnp.where(lane == axis, jnp.sum(gathered[axis], axis=1, keepdims=True), points)
    points_ref[...] = points


def pieces_of(depth):
    return [(matrix, slice(half * depth // 2, (half + 1) * depth // 2)) for matrix in range(3) for half in range(2)]


def coming_rows(core, space_ref, in_buffer, sems):
    _, depth, rows, _ = in_buffer.shape
    copies = []
    for k, (matrix, at) in enumerate(pieces_of(depth)):
        first = pl.multiple_of(rows * (2 * matrix + core), rows)
        copies.append(
            pltpu.make_async_copy(space_ref.at[at, pl.ds(first, rows), :], in_buffer.at[matrix, at], sems.at[k])
        )
    return copies


def turn_rows(in_buffer, wide_ref, matrix, at, store):
    _, _, rows, width = in_buffer.shape
    size = at.stop - at.start
    for first in range(0, size, 8):
        wide = in_buffer[matrix, at.start + first : at.start + first + 8].astype(f32)
        for r in range(8):
            wide_ref[(first + r) * rows : (first + r + 1) * rows, :] = wide[r]
    for part in range(2):
        for r in range(rows // 2):
            store(part, slice(r * width, (r + 1) * width), wide_ref[pl.ds(2 * r + part, size, stride=rows), :])


def send_kernel(
    core_ref, row_ref, base_ref, counts_ref, order_ref, space_ref, out_ref, told_ref, *scratch
):
    in_buffer, out_buffer, wide_ref, in_sems, out_sems = scratch
    depth = in_buffer.shape[1]
    coming = coming_rows(core_ref[0], space_ref, in_buffer, in_sems)
    places = pieces_of(depth)
    going = [
        pltpu.make_async_copy(out_buffer.at[matrix, :, at], out_ref.at[matrix, :, at], out_sems.at[k])
        for k, (matrix, at) in enumerate(places)
    ]
    for copy in coming:
        copy.start()
    lane = iota((1, BLOCKS), 1)
    told = jnp.where(lane == 4, order_ref[...].astype(f32), 0.0)
    own = iota((1, 8), 1) == row_ref[0]
    told = jnp.where(lane == 3, jnp.sum(jnp.where(own, counts_ref[...].astype(f32), 0.0), axis=1, keepdims=True), told)
    for axis in range(3):
        part = jnp.where(own, base_ref[axis : axis + 1, :], 0.0)
        told = jnp.where(lane == axis, jnp.sum(part, axis=1, keepdims=True), told)
    told_ref[...] = jnp.broadcast_to(told.reshape(1, 1, BLOCKS), told_ref.shape)
    for k, (matrix, at) in enumerate(places):
        coming[k].wait()

        def store(part, lanes, value):
            out_buffer[matrix, part, at, lanes] = value

        turn_rows(in_buffer, wide_ref, matrix, at, store)
        going[k].start()
    for copy in going:
        copy.wait()


def send_rows(space, core, row, base_k, counts, block_order):
    depth, rows, width = space.shape
    half = rows // 6
    shape = (3, 2, depth, half // 2 * width)
    return pl.pallas_call(
        send_kernel,
        out_shape=(jax.ShapeDtypeStruct(shape, f32), jax.ShapeDtypeStruct((BLOCKS, 1, BLOCKS), f32)),
        in_specs=[SMEM, SMEM, VMEM, VMEM, VMEM, HBM],
        out_specs=(HBM, VMEM),
        scratch_shapes=[
            pltpu.VMEM((3, depth, half, width), bf16),
            pltpu.VMEM(shape, f32),
            pltpu.VMEM((depth // 2 * half, width), f32),
            pltpu.SemaphoreType.DMA((6,)),
            pltpu.SemaphoreType.DMA((6,)),
        ],
        compiler_params=params(58),
        cost_estimate=cost(5),
        interpret=INTERPRET,
        name="send_rows",
    )(core, row, base_k.T, counts.reshape(1, 8), block_order.reshape(1, 1), space)


def join_kernel(core_ref, space_ref, other_ref, out_ref, in_buffer, other_buffer, wide_ref, in_sems, other_sems):
    depth = in_buffer.shape[1]
    coming = coming_rows(core_ref[0], space_ref, in_buffer, in_sems)
    places = pieces_of(depth)
    others = [
        pltpu.make_async_copy(other_ref.at[matrix, :, at], other_buffer.at[matrix, :, at], other_sems.at[k])
        for k, (matrix, at) in enumerate(places)
    ]
    for k in range(6):
        coming[k].start()
        others[k].start()
    for k, (matrix, at) in enumerate(places):
        coming[k].wait()

        def store(part, lanes, value):
            rows = slice(part * depth + at.start, part * depth + at.stop)
            out_ref[matrix, rows, lanes] = value.astype(bf16)

        turn_rows(in_buffer, wide_ref, matrix, at, store)
        others[k].wait()
        for part in range(2):
            rows = slice((2 + part) * depth + at.start, (2 + part) * depth + at.stop)
            out_ref[matrix, rows, :] = other_buffer[matrix, part, at, :].astype(bf16)


def join_rows(space, core, other):
    depth, rows, width = space.shape
    half = rows // 6
    lanes = half // 2 * width
    return pl.pallas_call(
        join_kernel,
        out_shape=jax.ShapeDtypeStruct((3, 4 * depth, lanes), bf16),
        in_specs=[SMEM, HBM, HBM],
        out_specs=VMEM,
        scratch_shapes=[
            pltpu.VMEM((3, depth, half, width), bf16),
            pltpu.VMEM((3, 2, depth, lanes), f32),
            pltpu.VMEM((depth // 2 * half, width), f32),
            pltpu.SemaphoreType.DMA((6,)),
            pltpu.SemaphoreType.DMA((6,)),
        ],
        compiler_params=params(54),
        cost_estimate=cost(5),
        interpret=INTERPRET,
        name="join_rows",
    )(core, space, other)


def turn(points, coords):
    turns = points[:, 0:1] * coords[0:1, :] + points[:, 1:2] * coords[1:2, :] + points[:, 2:3] * coords[2:3, :]
    rest = turns - jnp.floor(turns + 0.5)
    quarter = jnp.floor(4.0 * rest + 0.5)
    angle = (rest - 0.25 * quarter) * (2.0 * math.pi)
    square = angle * angle
    sine = angle * (1.0 + square * (-1.0 / 6 + square * (1.0 / 120 + square * (-1.0 / 5040 + square * (1.0 / 362880)))))
    cosine = 1.0 + square * (-0.5 + square * (1.0 / 24 + square * (-1.0 / 720 + square * (1.0 / 40320 - square / 3628800))))
    odd = jnp.abs(quarter) == 1.0
    first = jnp.where(odd, sine, cosine)
    second = jnp.where(odd, cosine, sine)
    cos_sign = jnp.where((quarter == 1.0) | (jnp.abs(quarter) == 2.0), -1.0, 1.0)
    sin_sign = jnp.where((quarter == -1.0) | (jnp.abs(quarter) == 2.0), -1.0, 1.0)
    return first * cos_sign, second * sin_sign


def store_phases(low, count, points_ref, coords_ref, phase_ref):
    depth = coords_ref.shape[1] // 2
    tile = 16

    def rows_of(i, carry):
        first = pl.multiple_of(i * tile, tile)
        points = points_ref[pl.ds(low + first, tile), :]
        for source in range(2):
            coords = coords_ref[:, source * depth : (source + 1) * depth]
            cosine, sine = turn(points, coords)
            at_real = slice(source * 2 * depth, source * 2 * depth + depth)
            at_imag = slice(source * 2 * depth + depth, source * 2 * depth + 2 * depth)
            pairs = [(cosine, sine)]
            for axis in range(2):
                coord = coords[axis : axis + 1, :]
                pairs.append((-coord * sine, coord * cosine))
            for kind, (real, imag) in enumerate(pairs):
                real_rows = pl.ds(2 * kind * count + first, tile)
                imag_rows = pl.ds((2 * kind + 1) * count + first, tile)
                phase_ref[real_rows, at_real] = real.astype(bf16)
                phase_ref[real_rows, at_imag] = (-imag).astype(bf16)
                phase_ref[imag_rows, at_real] = imag.astype(bf16)
                phase_ref[imag_rows, at_imag] = real.astype(bf16)
        return carry

    lax.fori_loop(0, count // tile, rows_of, 0)


def store_sums(phase_ref, matrices, count, kinds, first_kind, first_row, out_refs, pitches):
    product = jnp.dot(phase_ref[: kinds * count, :], matrices, preferred_element_type=f32)
    width = product.shape[1] // 2
    for kind in range(kinds):
        for half in range(2):
            block = product[kind * count : (kind + 1) * count, half * width : (half + 1) * width]
            at = (first_kind + kind) * 4 + first_row + half
            start = 0
            for ref, pitch in zip(out_refs, pitches):
                size = ref.shape[0] // 40
                ref[pl.ds(at, size, stride=40), :] = block[start : start + size]
                start += pitch


PLACES = tuple((matrix, part) for matrix in range(3) for part in range(2))


def fourier_kernel(low, pitches, waits, points_ref, coords_ref, matrices_ref, *refs):
    refs = refs[waits:]
    outs = len(pitches)
    out_refs, token_ref, phase_ref = refs[:outs], refs[outs], refs[outs + 1]
    token_ref[...] = jnp.zeros(token_ref.shape, f32)
    count = sum(pitches)
    lanes = matrices_ref.shape[2] // 2
    store_phases(low, count, points_ref, coords_ref, phase_ref)
    for matrix, part in PLACES:
        kinds, first_kind = (6, 0) if matrix == 0 else (2, 4 + 2 * matrix)
        block = matrices_ref[matrix, :, part * lanes : (part + 1) * lanes]
        store_sums(phase_ref, block, count, kinds, first_kind, 2 * part, out_refs, pitches)


def fourier(points, low, sizes, pitches, coords, matrices, microseconds, after=()):
    depth4 = matrices.shape[1]
    width = matrices.shape[2] // 4
    shapes = tuple(jax.ShapeDtypeStruct((size * 40, width), f32) for size in sizes)
    outs = pl.pallas_call(
        lambda *refs: fourier_kernel(low, pitches, len(after), *refs),
        out_shape=shapes + (jax.ShapeDtypeStruct((8, BLOCKS), f32),),
        in_specs=[VMEM, VMEM, VMEM] + [ANY] * len(after),
        out_specs=(VMEM,) * (len(shapes) + 1),
        scratch_shapes=[pltpu.VMEM((6 * sum(pitches), depth4), bf16)],
        compiler_params=params(18),
        cost_estimate=cost(microseconds),
        interpret=INTERPRET,
        name="fourier",
    )(points, coords, matrices, *after)
    return tuple(out.reshape(-1, 40, width) for out in outs[:-1]) + (outs[-1],)


def first_kernel(place_ref, table_ref, coords_ref, matrices_ref, *refs):
    near_ref, far_ref, points_ref, slots_ref, weight_ref, token_ref, phase_ref, buffer_ref, sems = refs
    token_ref[...] = jnp.zeros(token_ref.shape, f32)
    lanes = matrices_ref.shape[2] // 2
    copies = []
    for k, (matrix, part) in enumerate(PLACES):
        source = matrices_ref.at[matrix, :, pl.ds(part * lanes, lanes)]
        copies.append(pltpu.make_async_copy(source, buffer_ref.at[k], sems.at[k]))
    for copy in copies:
        copy.start()
    index_kernel(place_ref, table_ref, points_ref, slots_ref, weight_ref)
    store_phases(0, OWNERS, points_ref, coords_ref, phase_ref)
    for k, (matrix, part) in enumerate(PLACES):
        kinds, first_kind = (6, 0) if matrix == 0 else (2, 4 + 2 * matrix)
        copies[k].wait()
        store_sums(
            phase_ref, buffer_ref[k], OWNERS, kinds, first_kind, 2 * part, (near_ref, far_ref), (OWNERS // 2,) * 2
        )


def first_fourier(table, plane, coords, matrices):
    depth4 = matrices.shape[1]
    width = matrices.shape[2] // 4
    side = jax.ShapeDtypeStruct((OWNERS // 2 * 40, width), f32)
    near, far, points, slots, weights, token = pl.pallas_call(
        first_kernel,
        out_shape=(
            side,
            side,
            jax.ShapeDtypeStruct((12 * OWNERS + NX * SPARE, BLOCKS), f32),
            jax.ShapeDtypeStruct((8, BLOCKS), jnp.int32),
            jax.ShapeDtypeStruct((8, BLOCKS), f32),
            jax.ShapeDtypeStruct((8, BLOCKS), f32),
        ),
        in_specs=[SMEM, VMEM, VMEM, HBM],
        out_specs=(VMEM,) * 6,
        scratch_shapes=[
            pltpu.VMEM((6 * OWNERS, depth4), bf16),
            pltpu.VMEM((6, depth4, 2 * width), bf16),
            pltpu.SemaphoreType.DMA((6,)),
        ],
        compiler_params=params(18),
        cost_estimate=cost(5),
        interpret=INTERPRET,
        name="first_fourier",
    )(plane, table, coords, matrices)
    return near.reshape(-1, 40, width), far.reshape(-1, 40, width), points, slots, weights, token


def to_right(value):
    return lax.ppermute(value, "row_0", [(i, (i + 1) % NX) for i in range(NX)])


def to_left(value):
    return lax.ppermute(value, "row_0", [(i, (i - 1) % NX) for i in range(NX)])


def first_hop(near, far):
    near = to_right(near)
    far = to_left(far)
    return near, far


def add_kernel(waits, near_ref, far_ref, right_ref, left_ref, *refs):
    right_out, left_out, token_ref = refs[waits:]
    half = near_ref.shape[0]
    right_out[:half] = right_ref[:half] + near_ref[...]
    right_out[half:] = right_ref[half:]
    left_out[:half] = left_ref[:half]
    left_out[half:] = left_ref[half:] + far_ref[...]
    token_ref[...] = jnp.zeros(token_ref.shape, f32)


def add_arrived(near, far, right, left, after=()):
    shape = jax.ShapeDtypeStruct(right.shape, f32)
    return pl.pallas_call(
        lambda *refs: add_kernel(len(after), *refs),
        out_shape=(shape, shape, jax.ShapeDtypeStruct((8, BLOCKS), f32)),
        in_specs=[VMEM] * 4 + [ANY] * len(after),
        out_specs=(VMEM,) * 3,
        input_output_aliases={2: 0, 3: 1},
        compiler_params=params(6),
        cost_estimate=cost(1.5),
        interpret=INTERPRET,
        name="add_arrived",
    )(near, far, right, left, *after)


def second_hop(right, left):
    right = to_right(right)
    left = to_left(left)
    return right, left


def place_kernel(place_ref, slots_ref, *refs):
    keep0, right0, left0, keep1, right1, left1, extra = refs[:7]
    out_ref, token_ref, table_ref = refs[-3:]
    token_ref[...] = jnp.zeros(token_ref.shape, f32)
    plane = place_ref[0]
    first, second = keep0.shape[0], keep0.shape[0] + keep1.shape[0]
    table_ref[:first] = keep0[...] + right0[...] + left0[...]
    table_ref[first:second] = keep1[...] + right1[...] + left1[...]
    table_ref[second:] = extra[...]

    def body(owner, carry):
        position = (owner // 2) * 8 + 2 * plane + owner % 2
        for s in range(1, SUB):
            out_ref[owner, s - 1] = table_ref[slots_ref[s, position]]
        return carry

    lax.fori_loop(0, OWNERS, body, 0)


def place_slots(plane, slots, parts0, parts1, extra, after):
    _, rows, width = extra.shape
    size = OWNERS + SECOND + SPARE
    return pl.pallas_call(
        place_kernel,
        out_shape=(
            jax.ShapeDtypeStruct((OWNERS, SUB - 1, rows, width), f32),
            jax.ShapeDtypeStruct((8, BLOCKS), f32),
        ),
        in_specs=[SMEM, SMEM] + [VMEM] * 7 + [ANY] * len(after),
        out_specs=(VMEM, VMEM),
        scratch_shapes=[pltpu.VMEM((size, rows, width), f32)],
        compiler_params=params(12),
        cost_estimate=cost(4),
        interpret=INTERPRET,
        name="place_slots",
    )(plane, slots, *parts0, *parts1, extra, *after)


def total_kernel(keep_ref, right_ref, left_ref, out_ref):
    out_ref[...] = keep_ref[...] + right_ref[...] + left_ref[...]


def total(keep, right, left):
    return pl.pallas_call(
        total_kernel,
        out_shape=jax.ShapeDtypeStruct(keep.shape, f32),
        in_specs=[VMEM] * 3,
        out_specs=VMEM,
        compiler_params=params(8),
        cost_estimate=cost(1.5),
        interpret=INTERPRET,
        name="total",
    )(keep, right, left)


def to_owners(value):
    return lax.all_to_all(value, PLANE, split_axis=0, concat_axis=0, tiled=True)


def two_terms(value):
    high = value.astype(bf16)
    return high, (value - high.astype(f32)).astype(bf16)


def curvature_kernel(first, units, adding, weight_ref, field_ref, turn_ref, back_ref, occupied_ref, *refs):
    out_ref = refs[-1]
    previous = refs[0][...] if adding else 0.0
    unit = pl.program_id(0)
    sources = field_ref.shape[0] // (units * 40)
    n = field_ref.shape[1]
    stride = units * 40

    def plane_of(kind):
        return jnp.concatenate(
            [field_ref[pl.ds(unit * 40 + kind * 4 + r, sources, stride=stride), :] for r in range(4)], axis=0
        )

    matrices = jnp.concatenate(
        [jnp.concatenate([plane_of(2 * c), plane_of(2 * c + 1)], axis=1) for c in range(5)], axis=0
    )
    high, low = two_terms(matrices)
    vectors = turn_ref[0]
    rotated = jnp.dot(high, vectors, preferred_element_type=f32) + jnp.dot(low, vectors, preferred_element_type=f32)
    stacked = jnp.concatenate(
        [
            jnp.concatenate([rotated[c * n : (c + 1) * n, :n] for c in range(5)], axis=1),
            jnp.concatenate([rotated[c * n : (c + 1) * n, n:] for c in range(5)], axis=1),
        ],
        axis=0,
    )
    back = back_ref[0]
    high, low = two_terms(stacked)
    bar = jnp.dot(back, high, preferred_element_type=f32) + jnp.dot(back, low, preferred_element_type=f32)
    bar_real, bar_imag = bar[:n], bar[n:]
    diagonal = jnp.where(iota((n, n), 0) == iota((n, n), 1), bar_real[:, :n], 0.0)
    spacing = jnp.sum(diagonal, axis=0, keepdims=True) - jnp.sum(diagonal, axis=1, keepdims=True)
    smoothed = spacing / (spacing * spacing + broadening)

    def pick(value, c):
        return value[:, (c + 1) * n : (c + 2) * n]

    xcov_real = pick(bar_real, 2) + smoothed * pick(bar_real, 0)
    xcov_imag = pick(bar_imag, 2) + smoothed * pick(bar_imag, 0)
    ycov_real = pick(bar_real, 3) + smoothed * pick(bar_real, 1)
    ycov_imag = pick(bar_imag, 3) + smoothed * pick(bar_imag, 1)
    s = first + unit
    filled = occupied_ref[pl.ds(s, 1), :].astype(f32)
    filled_down = jnp.broadcast_to(filled, (n, n)).T
    pairing = filled_down * (1.0 - filled)
    product = pairing * (xcov_real * ycov_imag.T + xcov_imag * ycov_real.T)
    berry = jnp.sum(jnp.sum(product, axis=0, keepdims=True), axis=1, keepdims=True) * (-2.0 / n)
    weight = weight_ref[s]
    lane = iota((1, SUB), 1)
    result = jnp.where((lane == s) & (weight > 0.0), weight * berry, 0.0)
    before = jnp.where(unit == 0, previous, out_ref[...])
    out_ref[...] = result + before


def curvature(first, units, weight, arrived, vectors, adjoint, occupied, previous=(), after=()):
    width = arrived.shape[-1]
    flat = arrived.reshape(-1, width)
    matrix = pl.BlockSpec((1, 2 * width, 2 * width), lambda u: (u, 0, 0))
    return pl.pallas_call(
        lambda *refs: curvature_kernel(first, units, len(previous), *refs),
        grid=(units,),
        out_shape=jax.ShapeDtypeStruct((1, SUB), f32),
        in_specs=[
            SMEM,
            VMEM,
            matrix,
            matrix,
            pl.BlockSpec(occupied.shape, lambda u: (0, 0)),
        ]
        + [pl.BlockSpec((1, SUB), lambda u: (0, 0))] * len(previous)
        + [ANY] * len(after),
        out_specs=pl.BlockSpec((1, SUB), lambda u: (0, 0)),
        compiler_params=params(58 if units > 1 else 12),
        cost_estimate=cost(2.5 * units),
        interpret=INTERPRET,
        name="curvature",
    )(weight, flat, vectors, adjoint, occupied, *previous, *after)


def vector_kernel(eigvecs_ref, *refs):
    turn_ref, back_ref, wide_ref = refs[-3:]
    n = eigvecs_ref.shape[2]
    wide_ref[...] = eigvecs_ref[0].astype(f32)
    real, imag = (wide_ref[pl.ds(part, n, stride=2), :].astype(bf16) for part in range(2))
    turn_ref[0, :n, :n] = real
    turn_ref[0, :n, n:] = imag
    turn_ref[0, n:, :n] = -imag
    turn_ref[0, n:, n:] = real
    group = n // OWNERS
    for part in range(2):
        packed = jnp.concatenate(
            [wide_ref[pl.ds(2 * r + part, OWNERS, stride=2 * group), :] for r in range(group)], axis=0
        )
        turned = packed.T
        if part == 0:
            back_ref[0, :n, :n] = turned.astype(bf16)
            back_ref[0, n:, n:] = turned.astype(bf16)
        else:
            back_ref[0, :n, n:] = turned.astype(bf16)
            back_ref[0, n:, :n] = (-turned).astype(bf16)


def vector_matrices(eigvecs, first, count, after):
    slots, width = eigvecs.shape[0], eigvecs.shape[1]
    shape = jax.ShapeDtypeStruct((count, 2 * width, 2 * width), bf16)
    square = pl.BlockSpec((1, 2 * width, 2 * width), lambda i: (i, 0, 0))
    return pl.pallas_call(
        vector_kernel,
        grid=(count,),
        out_shape=(shape, shape),
        in_specs=[pl.BlockSpec((1, 2 * width, width), lambda i: (first + i, 0, 0))] + [ANY] * len(after),
        out_specs=(square, square),
        scratch_shapes=[pltpu.VMEM((2 * width, width), f32)],
        compiler_params=params(4),
        cost_estimate=cost(2),
        interpret=INTERPRET,
        name="vector_matrices",
    )(eigvecs.reshape(slots, 2 * width, width), *after)


def body(base_k, counts, block_order, lattice, real_space, eigvecs, occupied):
    plane, core = lax.axis_index("row_0"), lax.axis_index("row_1")
    row = plane * 2 + core
    plane_ref = plane.reshape(1).astype(jnp.int32)
    core_ref = core.reshape(1).astype(jnp.int32)
    depth, _, slab, _, width = real_space.shape

    space = real_space.reshape(depth, 6 * slab, width)
    swap = [(0, 1), (1, 0)]
    row_ref = row.reshape(1).astype(jnp.int32)
    send, mine = send_rows(space, 1 - core_ref, row_ref, base_k, counts, block_order)
    other = lax.ppermute(send, "row_1", swap)
    own_coords = jnp.pad(lattice.T.astype(f32), ((0, 5), (0, 0)))
    coords = jnp.concatenate([own_coords, lax.ppermute(own_coords, "row_1", swap)], axis=1)

    table = lax.all_to_all(mine, KA_ROW, 0, 0, tiled=True)
    table = table.reshape(BLOCKS, BLOCKS)
    matrices = join_rows(space, core_ref, other)
    near0, far0, points, slots, weights, token = first_fourier(table, plane_ref, coords, matrices)
    position = (lax.axis_index(KA) * 8 + row).astype(jnp.int32)
    weight = lax.dynamic_slice(weights, (jnp.int32(0), position), (SUB, 1)).reshape(SUB)

    half = OWNERS // 2

    def sums(low, sizes, pitches, microseconds, after=()):
        return fourier(points, low, sizes, pitches, coords, matrices, microseconds, after)

    def rest(chunk, size, after):
        return sums(3 * OWNERS * (1 + chunk), (size,) * 3, (OWNERS,) * 3, 5, after)

    hop0 = first_hop(near0, far0)
    near1, far1, near3, far3, token = sums(
        OWNERS, (half, SECOND - half, half, half), (half,) * 4, 4, (token,)
    )
    hop1 = first_hop(near1, far1)
    right0, left0, keep0, token = rest(0, OWNERS, (token,))
    right0, left0, token = add_arrived(*hop0, right0, left0)
    ring0 = second_hop(right0, left0)
    right1, left1, keep1, token = rest(1, SECOND, (token,))
    right1, left1, token = add_arrived(*hop1, right1, left1)
    ring1 = second_hop(right1, left1)
    hop3 = first_hop(near3, far3)
    right3, left3, keep3, token = rest(2, OWNERS, (token,))

    def further(_):
        parts = (half, half, SPARE, SPARE, SPARE)
        near, far, right, left, keep, _ = sums(12 * OWNERS, parts, parts, 8)
        right, left, _ = add_arrived(*first_hop(near, far), right, left)
        right, left = second_hop(right, left)
        return keep + right + left

    empty = (SPARE,) + keep0.shape[1:]
    extra = lax.cond(slots[0, 0] > OWNERS + SECOND, further, lambda _: jnp.zeros(empty, f32), 0)

    placed, token = place_slots(plane_ref, slots, (keep0, *ring0), (keep1, *ring1), extra, (token,))
    unit123 = to_owners(placed)
    right3, left3, token = add_arrived(*hop3, right3, left3, (token,))
    ring3 = second_hop(right3, left3)
    turning0, back0 = vector_matrices(eigvecs, 0, 1, (token,))
    turning, back = vector_matrices(eigvecs, 1, SUB - 1, (token,))
    unit0 = to_owners(total(keep3, *ring3))
    curve = curvature(1, 3, weight, unit123, turning, back, occupied)
    return curvature(0, 1, weight, unit0, turning0, back0, occupied, (curve,)).reshape(SUB)


def solution(mesh):
    finer = Mesh(mesh.devices.reshape(4, 4, 4, 2), ("ka_0", "ka_1", "row_0", "row_1"))
    placed = (
        P(KA, None),
        P(KA),
        P(KA_ROW),
        P(ROW, None),
        P(ROW, None, KA, None, None),
        P(KA_ROW, None, None, None),
        P(KA_ROW, None),
    )
    return jax.shard_map(body, mesh=finer, in_specs=placed, out_specs=P(KA_ROW), check_vma=False)
```
